128 devices in a mesh: lat: 8 (over x, core), lon: 16 (over z, y).
Axes of the slice: x: 4, y: 4, z: 4, core: 2. Of those that a mesh axis runs over, the one named last changes fastest.
Arguments:
- tracers: bfloat16 [512, 2048, 32, 4], P('lat', 'lon'), may hold values from 0 to 2
- weights: bfloat16 [512, 16, 8, 128, 128], P('lat', 'lon'), may hold values from -1 to 1, as said below
- source_row: int32 [512, 16, 8], P('lat', 'lon'), may hold values from 0 to 511, as said below
- source_block: int32 [512, 16, 8], P('lat', 'lon'), may hold values from 0 to 15, as said below
- slot_count: int32 [512, 16], P('lat', 'lon'), may hold values from 1 to 8, as said below
Outputs:
- advected_fixed: float32 [512, 2048, 32, 4], P('lat', 'lon')
The draws below stay inside these ranges and needn't reach their ends.
Inputs may be any that keep to these rules, and one draw needn't show every extreme that they name: source_row differs from the target tile's own row by at most 4 and lies within the grid. source_block lies at cyclic distance at most 2 from the target tile's own index along the row, except for target tiles of the first and the last latitude row, where it may reach 3; the allowed distance grows from 1 at the equator towards the poles; in the two outermost rows slot 0 reaches exactly 3 sectors ahead on even tiles and 3 sectors behind on odd tiles. slot_count grows from 1 or 2 at the equator to 8 at the two outermost rows. weights are of either sign; for each target tile the weights of each target cell over the used slots and all source cells sum (before rounding to bfloat16) to one value of that tile between 0.9 and 1.05.
All inputs are finite; a program needn't handle non-finite values.
Results may differ from the reference program's by a relative error of at most 0.0003.
Values may be sent and summed in bfloat16 or wider, within the bound.
No kernel may reach another device: no remote copies, remote signals or barrier semaphores. Data moves between devices by JAX's collectives and lax.ppermute only.
A program may use at most 192 MiB of HBM per device.

```python
import math
import jax
import jax.numpy as jnp
from jax import lax

TILE = 128
LEV = 32
TRC = 4
KMAX = 8
RLAT = 4
REACH = 3
NLAT = 512
NBLK = 16
NLON = 2048


def source_lists(key):
    base = jax.random.fold_in(key, 4711)
    first_key, second_key, third_key = jax.random.split(base, 3)
    shape = (NLAT, NBLK, KMAX)
    rows_all = jnp.arange(NLAT, dtype=jnp.int32)[:, None, None]
    distance = jnp.abs(2 * rows_all - (NLAT - 1))
    span = max((NLAT - 1) * (NLAT - 1), 1)
    extra = jax.random.randint(first_key, (NLAT, NBLK, 1), 0, 2, dtype=jnp.int32)
    counts = jnp.minimum(KMAX, 1 + (KMAX - 1) * distance * distance // span + extra)[:, :, 0]
    allowed = 1 + (REACH - 1) * distance * distance // span
    offsets = jax.random.randint(second_key, shape, -REACH, REACH + 1, dtype=jnp.int32)
    offsets = jnp.clip(offsets, -allowed, allowed)
    slots = jnp.arange(KMAX, dtype=jnp.int32)[None, None, :]
    columns = jnp.arange(NBLK, dtype=jnp.int32)[None, :, None]
    outermost = (distance == NLAT - 1) & (slots == 0)
    polar_sign = 1 - 2 * (columns % 2)
    offsets = jnp.where(outermost, allowed * polar_sign, offsets)
    blocks = (columns + offsets) % NBLK
    row_shift = jax.random.randint(third_key, shape, -RLAT, RLAT + 1, dtype=jnp.int32)
    rows_out = jnp.clip(rows_all + row_shift, 0, NLAT - 1)
    return (rows_out.astype(jnp.int32), blocks.astype(jnp.int32), counts.astype(jnp.int32))


def draw_source_row(key, part):
    return source_lists(key)[0]


def draw_source_block(key, part):
    return source_lists(key)[1]


def draw_slot_count(key, part):
    return source_lists(key)[2]


def draw_weights(key, part):
    counts = source_lists(key)[2]
    base = jax.random.fold_in(key, 911)
    spread = float(TILE * KMAX) ** (-0.5)

    def one_row(packed):
        row_number, count_row = packed
        row_key = jax.random.fold_in(base, row_number)
        noise_key, target_key = jax.random.split(row_key)
        shape = (NBLK, KMAX, TILE, TILE)
        noise = jax.random.normal(noise_key, shape, jnp.float32) * spread
        target = jax.random.uniform(target_key, (NBLK,), jnp.float32, 0.9, 1.05)
        active = (jnp.arange(KMAX, dtype=jnp.int32)[None, :] < count_row[:, None]).astype(jnp.float32)
        used = count_row.astype(jnp.float32) * TILE
        mask = active[:, :, None, None]
        row_total = jnp.sum(noise * mask, axis=(1, 3))
        offset = (target[:, None] - row_total) / used[:, None]
        result = noise + mask * offset[:, None, :, None]
        return result.astype(jnp.bfloat16)
    return lax.map(one_row, (jnp.arange(NLAT, dtype=jnp.int32), counts))


def block_scale(rng, dims, shards, smallest, top_value):
    loudness = 1.0
    for position, parts in shards:
        steps = jax.random.uniform(jax.random.fold_in(jax.random.fold_in(rng, 6), position), (parts,), jnp.float32, smallest / len(shards), top_value / len(shards))
        loudness = loudness * jnp.repeat(jnp.exp(steps), dims[position] // parts).reshape((-1,) + (1,) * (len(dims) - 1 - position))
    return loudness


def setup_inputs(seed: int = 0) -> dict:
    arg_keys = jax.random.split(jax.random.key(seed), 6)
    return {
        "tracers": jnp.clip(2.0 * jax.random.uniform(arg_keys[0], (NLAT, NLON, LEV, TRC), jnp.float32) ** block_scale(arg_keys[0], (NLAT, NLON, LEV, TRC), ((0, 8), (1, 16)), -0.2, 0.2), 0.0, 2.0).astype(jnp.bfloat16),
        "weights": draw_weights(jax.random.fold_in(arg_keys[5], 71), 0),
        "source_row": draw_source_row(jax.random.fold_in(arg_keys[5], 71), 0),
        "source_block": draw_source_block(jax.random.fold_in(arg_keys[5], 71), 0),
        "slot_count": draw_slot_count(jax.random.fold_in(arg_keys[5], 71), 0),
    }


def latitude_area(total_rows, first_row, count_rows):
    rows_all = jnp.arange(count_rows, dtype=jnp.int32) + first_row
    angle = -0.5 * math.pi + (rows_all.astype(jnp.float32) + 0.5) * (math.pi / total_rows)
    return jnp.cos(angle)


def reference(tracers, weights, source_row, source_block, slot_count):
    channels = LEV * TRC
    blocks = tracers.reshape(NLAT, NBLK, TILE, channels)

    def one_row(packed):
        rows_here, blocks_here, counts_here, weights_here = packed
        sources = blocks[rows_here, blocks_here]
        active = jnp.arange(KMAX, dtype=jnp.int32)[None, :] < counts_here[:, None]
        sources = jnp.where(active[:, :, None, None], sources, jnp.zeros((), sources.dtype))
        return jnp.einsum("bkij,bkjc->bic", weights_here.astype(jnp.float32), sources.astype(jnp.float32))

    advected = lax.map(one_row, (source_row, source_block, slot_count, weights))
    advected = advected.reshape(NLAT, NLON, channels)
    field = tracers.reshape(NLAT, NLON, channels)
    area = latitude_area(NLAT, 0, NLAT)
    total_area = NLON * jnp.sum(area)
    mass_old = jnp.sum(area[:, None, None] * field, axis=(0, 1))
    mass_new = jnp.sum(area[:, None, None] * advected, axis=(0, 1))
    fixed = advected + (mass_old - mass_new) / total_area
    return fixed.reshape(NLAT, NLON, LEV, TRC)
```

```python
import math

import jax
import jax.numpy as jnp
from jax import lax
from jax.experimental import pallas as pl
from jax.experimental.pallas import tpu as pltpu
from jax.sharding import PartitionSpec as P

ROWS = 64
C = 128
KMAX = 8
R = 4
E = R + 1
MID = ROWS - 2 * E
PAD = ROWS + 2 * R
NLAT, NLON_DEV, NLAT_DEV = 512, 16, 8
TB = 4
FAR = 2 * PAD
NT = (((1,), (1,)), ((), ()))


def ring(by):
    return [(i, (i + by) % NLON_DEV) for i in range(NLON_DEV)]


UP = [(i, i + 1) for i in range(NLAT_DEV - 1)]
DOWN = [(i + 1, i) for i in range(NLAT_DEV - 1)]


def polar(by):
    return [
        (a * NLON_DEV + i, a * NLON_DEV + (i + by) % NLON_DEV)
        for a in (0, NLAT_DEV - 1)
        for i in range(NLON_DEV)
    ]


def near_kernel(idx_ref, w_ref, *refs):
    parts, (out_ref, src, sem) = refs[:-3], refs[-3:]
    step = pl.program_id(0)
    own, le, lm, re, rm, up, dn = parts

    def copies():
        todo = [(own, 0, ROWS, 0 * PAD + R)]
        for n, (e, m) in enumerate(((le, lm), (re, rm))):
            at = (n + 1) * PAD + R
            todo.append((e, 0, E, at))
            todo.append((m, 0, MID, at + E))
            todo.append((e, E, E, at + E + MID))
        for n in range(3):
            todo.append((up, n * R, R, n * PAD))
            todo.append((dn, n * R, R, n * PAD + R + ROWS))
        return [
            pltpu.make_async_copy(ref.at[pl.ds(a, n)], src.at[pl.ds(to, n)], sem.at[i])
            for i, (ref, a, n, to) in enumerate(todo)
        ]

    @pl.when(step == 0)
    def _():
        for copy in copies():
            copy.start()
        src[3 * PAD] = jnp.zeros((C, C), src.dtype)
        for copy in copies():
            copy.wait()

    for j in range(TB):
        t = step * TB + j
        lhs = jnp.concatenate([src[idx_ref[k, t]] for k in range(KMAX)], axis=1)
        rhs = jnp.concatenate([w_ref[j, k] for k in range(KMAX)], axis=1)
        out_ref[j] = lax.dot_general(lhs, rhs, NT, preferred_element_type=jnp.float32)


def near_call(idx, weights, parts):
    n_copies = 7 + 6
    return pl.pallas_call(
        near_kernel,
        grid_spec=pltpu.PrefetchScalarGridSpec(
            num_scalar_prefetch=1,
            grid=(ROWS // TB,),
            in_specs=[pl.BlockSpec((TB, KMAX, C, C), lambda s, i: (s, 0, 0, 0))]
            + [pl.BlockSpec(memory_space=pltpu.HBM)] * len(parts),
            out_specs=pl.BlockSpec((TB, C, C), lambda s, i: (s, 0, 0)),
            scratch_shapes=[
                pltpu.VMEM((3 * PAD + 1, C, C), jnp.bfloat16),
                pltpu.SemaphoreType.DMA((n_copies,)),
            ],
        ),
        out_shape=jax.ShapeDtypeStruct((ROWS, C, C), jnp.float32),
        compiler_params=pltpu.CompilerParams(
            dimension_semantics=("arbitrary",), vmem_limit_bytes=20 << 20
        ),
        cost_estimate=pl.CostEstimate(
            flops=2 * ROWS * KMAX * C**3, bytes_accessed=28 << 20, transcendentals=0
        ),
        name="near",
    )(idx, weights, *parts)


GROUP = 8


def far_kernel(lst_ref, num_ref, area_ref, w_hbm, le, lm, re, rm, up, dn, l3, r3, part_ref, out_ref, mass_ref, src, wbuf, sem, wsem):
    todo = []
    for n, (e, m) in enumerate(((le, lm), (re, rm))):
        at = n * PAD + R
        todo.append((e, 0, E, at))
        todo.append((m, 0, MID, at + E))
        todo.append((e, E, E, at + E + MID))
        todo.append((up, n * R, R, n * PAD))
        todo.append((dn, n * R, R, n * PAD + R + ROWS))
    todo.append((l3, 0, E, FAR))
    todo.append((r3, 0, E, FAR + E))
    copies = [
        pltpu.make_async_copy(ref.at[pl.ds(a, n)], src.at[pl.ds(to, n)], sem.at[i])
        for i, (ref, a, n, to) in enumerate(todo)
    ]
    for copy in copies:
        copy.start()
    groups = num_ref[0]

    def entry(g, j):
        v = lst_ref[g * GROUP + j]
        slot = lax.shift_right_logical(v, 9)
        return lax.shift_right_logical(slot, 3), slot & (KMAX - 1), v & 511

    def weight_copy(g, j):
        t, k, _ = entry(g, j)
        return pltpu.make_async_copy(w_hbm.at[t, k], wbuf.at[g * GROUP + j], wsem.at[g])

    def issue(g, carry):
        for j in range(GROUP):
            weight_copy(g, j).start()
        return carry

    lax.fori_loop(0, groups, issue, 0)
    out_ref[...] = part_ref[...]
    src[FAR + 2 * E] = jnp.zeros((C, C), src.dtype)
    for copy in copies:
        copy.wait()

    def work(g, carry):
        for j in range(GROUP):
            weight_copy(g, j).wait()
        got = []
        for j in range(GROUP):
            t, _, s = entry(g, j)
            got.append(
                (t, lax.dot_general(src[s], wbuf[g * GROUP + j], NT, preferred_element_type=jnp.float32))
            )
        for t, d in got:
            out_ref[t] = out_ref[t] + d
        return carry

    lax.fori_loop(0, groups, work, 0)

    def add_up(t, acc):
        return acc + area_ref[t] * out_ref[t]

    acc = lax.fori_loop(0, ROWS, add_up, jnp.zeros((C, C), jnp.float32), unroll=4)
    mass_ref[...] = lax.dot_general(
        jnp.ones((8, C), jnp.float32), acc, NT,
        precision=lax.Precision.HIGHEST, preferred_element_type=jnp.float32,
    )


def far_call(lst, num, area, weights, parts, partial):
    smem = pl.BlockSpec(memory_space=pltpu.SMEM)
    hbm = pl.BlockSpec(memory_space=pltpu.HBM)
    vmem = pl.BlockSpec(memory_space=pltpu.VMEM)
    return pl.pallas_call(
        far_kernel,
        in_specs=[smem, smem, smem, hbm] + [hbm] * len(parts) + [vmem],
        out_specs=[vmem, vmem],
        out_shape=[
            jax.ShapeDtypeStruct((ROWS, C, C), jnp.float32),
            jax.ShapeDtypeStruct((8, C), jnp.float32),
        ],
        scratch_shapes=[
            pltpu.VMEM((FAR + 2 * E + 1, C, C), jnp.bfloat16),
            pltpu.VMEM((ROWS * KMAX, C, C), jnp.bfloat16),
            pltpu.SemaphoreType.DMA((12,)),
            pltpu.SemaphoreType.DMA((ROWS * KMAX // GROUP,)),
        ],
        compiler_params=pltpu.CompilerParams(vmem_limit_bytes=40 << 20),
        cost_estimate=pl.CostEstimate(
            flops=2 * ROWS * KMAX * C**3 // 2, bytes_accessed=20 << 20, transcendentals=0
        ),
        name="far",
    )(lst, num, area, weights, *parts, partial)


def latitude_area(first_row, count_rows):
    rows_all = jnp.arange(count_rows, dtype=jnp.int32) + first_row
    angle = -0.5 * math.pi + (rows_all.astype(jnp.float32) + 0.5) * (math.pi / NLAT)
    return jnp.cos(angle)


def slots(source_row, source_block, slot_count, lat, lon):
    row = source_row[:, 0, :].T - (lat * ROWS - R)
    row = jnp.clip(row, 0, PAD - 1)
    rel = (source_block[:, 0, :].T - lon + 3) % NLON_DEV - 3
    active = jnp.arange(KMAX, dtype=jnp.int32)[:, None] < slot_count[:, 0][None, :]
    size = jnp.abs(rel)
    side = (rel > 0).astype(jnp.int32)
    is_near = active & (size <= 1)
    near = jnp.where(is_near, jnp.where(rel == 0, 0, side + 1) * PAD + row, 3 * PAD)
    polar_row = jnp.clip(jnp.where(lat == 0, row - R, row - R - (ROWS - E)), 0, E - 1)
    far = jnp.where(size >= 3, FAR + side * E + polar_row, side * PAD + row)
    is_far = active & (size >= 2)
    target = jnp.arange(ROWS, dtype=jnp.int32)[None, :]
    slot = target * KMAX + jnp.arange(KMAX, dtype=jnp.int32)[:, None]
    order = jnp.where(is_far, slot, ROWS * KMAX + slot)
    zero = FAR + 2 * E
    packed = (order * 512 + jnp.where(is_far, far, zero)).reshape(-1)
    packed = jnp.sort(packed) & (ROWS * KMAX * 512 - 1)
    groups = (jnp.sum(is_far.astype(jnp.int32)) + GROUP - 1) // GROUP
    return near.astype(jnp.int32), packed.astype(jnp.int32), groups.reshape(1)


def local(tracers, weights, source_row, source_block, slot_count):
    lat, lon = lax.axis_index("lat"), lax.axis_index("lon")
    q = tracers.transpose(0, 2, 3, 1).reshape(ROWS, C, C)
    qe = jnp.concatenate([q[:E], q[ROWS - E :]], axis=0)
    qm = q[E : ROWS - E]
    le, re = (lax.ppermute(qe, "lon", ring(1)), lax.ppermute(qe, "lon", ring(-1)))
    lm, rm = (lax.ppermute(qm, "lon", ring(1)), lax.ppermute(qm, "lon", ring(-1)))
    near_idx, far_list, far_groups = slots(source_row, source_block, slot_count, lat, lon)
    area = latitude_area(lat * ROWS, ROWS)
    total_area = C * NLON_DEV * jnp.sum(latitude_area(0, NLAT))
    mass_old = jnp.sum(area[:, None, None] * q.astype(jnp.float32), axis=(0, 2))

    up1 = lax.ppermute(jnp.concatenate([v[2 * E - R :] for v in (qe, le, re)], axis=0), "lat", UP)
    dn1 = lax.ppermute(jnp.concatenate([v[:R] for v in (qe, le, re)], axis=0), "lat", DOWN)
    lle, rre = (lax.ppermute(le, "lon", ring(1)), lax.ppermute(re, "lon", ring(-1)))
    llm, rrm = (lax.ppermute(lm, "lon", ring(1)), lax.ppermute(rm, "lon", ring(-1)))
    up2 = lax.ppermute(jnp.concatenate([v[2 * E - R :] for v in (lle, rre)], axis=0), "lat", UP)
    dn2 = lax.ppermute(jnp.concatenate([v[:R] for v in (lle, rre)], axis=0), "lat", DOWN)
    pole = [jnp.where(lat == 0, v[:E], v[E:]) for v in (lle, rre)]
    l3 = lax.ppermute(pole[0], ("lat", "lon"), polar(1))
    r3 = lax.ppermute(pole[1], ("lat", "lon"), polar(-1))

    w = weights[:, 0]
    partial = near_call(near_idx, w, (q, le, lm, re, rm, up1, dn1))
    advected, mass_new = far_call(
        far_list, far_groups, area, w, (lle, llm, rre, rrm, up2, dn2, l3, r3), partial
    )
    change = lax.psum(mass_old - mass_new[0], ("lat", "lon"))
    fixed = advected + (change / total_area)[None, :, None]
    return fixed.reshape(ROWS, 32, 4, C).transpose(0, 3, 1, 2)


def solution(mesh):
    placed = (
        P("lat", "lon", None, None),
        P("lat", "lon", None, None, None),
        P("lat", "lon", None),
        P("lat", "lon", None),
        P("lat", "lon"),
    )
    return jax.shard_map(
        local, mesh=mesh, in_specs=placed, out_specs=P("lat", "lon", None, None), check_vma=False
    )
```

```python
import math

import jax
import jax.numpy as jnp
from jax import lax
from jax.experimental import pallas as pl
from jax.experimental.pallas import tpu as pltpu
from jax.sharding import PartitionSpec as P

ROWS = 64
C = 128
KMAX = 8
R = 4
E = R + 1
MID = ROWS - 2 * E
PAD = ROWS + 2 * R
NLAT, NLON_DEV, NLAT_DEV = 512, 16, 8
TB = 4
FAR = 2 * PAD
NT = (((1,), (1,)), ((), ()))


def ring(by):
    return [(i, (i + by) % NLON_DEV) for i in range(NLON_DEV)]


UP = [(i, i + 1) for i in range(NLAT_DEV - 1)]
DOWN = [(i + 1, i) for i in range(NLAT_DEV - 1)]


def polar(by):
    return [
        (a * NLON_DEV + i, a * NLON_DEV + (i + by) % NLON_DEV)
        for a in (0, NLAT_DEV - 1)
        for i in range(NLON_DEV)
    ]


def near_kernel(idx_ref, w_ref, *refs):
    parts, (out_ref, src, sem) = refs[:-3], refs[-3:]
    step = pl.program_id(0)
    own, le, lm, re, rm, up, dn = parts

    def copies():
        todo = [(own, 0, ROWS, 0 * PAD + R)]
        for n, (e, m) in enumerate(((le, lm), (re, rm))):
            at = (n + 1) * PAD + R
            todo.append((e, 0, E, at))
            todo.append((m, 0, MID, at + E))
            todo.append((e, E, E, at + E + MID))
        for n in range(3):
            todo.append((up, n * R, R, n * PAD))
            todo.append((dn, n * R, R, n * PAD + R + ROWS))
        return [
            pltpu.make_async_copy(ref.at[pl.ds(a, n)], src.at[pl.ds(to, n)], sem.at[i])
            for i, (ref, a, n, to) in enumerate(todo)
        ]

    @pl.when(step == 0)
    def _():
        for copy in copies():
            copy.start()
        src[3 * PAD] = jnp.zeros((C, C), src.dtype)
        for copy in copies():
            copy.wait()

    for j in range(TB):
        t = step * TB + j
        lhs = jnp.concatenate([src[idx_ref[k, t]] for k in range(KMAX)], axis=1)
        rhs = jnp.concatenate([w_ref[j, k] for k in range(KMAX)], axis=1)
        out_ref[j] = lax.dot_general(lhs, rhs, NT, preferred_element_type=jnp.float32)


def near_call(idx, weights, parts):
    n_copies = 7 + 6
    return pl.pallas_call(
        near_kernel,
        grid_spec=pltpu.PrefetchScalarGridSpec(
            num_scalar_prefetch=1,
            grid=(ROWS // TB,),
            in_specs=[pl.BlockSpec((TB, KMAX, C, C), lambda s, i: (s, 0, 0, 0))]
            + [pl.BlockSpec(memory_space=pltpu.HBM)] * len(parts),
            out_specs=pl.BlockSpec((TB, C, C), lambda s, i: (s, 0, 0)),
            scratch_shapes=[
                pltpu.VMEM((3 * PAD + 1, C, C), jnp.bfloat16),
                pltpu.SemaphoreType.DMA((n_copies,)),
            ],
        ),
        out_shape=jax.ShapeDtypeStruct((ROWS, C, C), jnp.float32),
        compiler_params=pltpu.CompilerParams(
            dimension_semantics=("arbitrary",), vmem_limit_bytes=20 << 20
        ),
        cost_estimate=pl.CostEstimate(
            flops=2 * ROWS * KMAX * C**3, bytes_accessed=28 << 20, transcendentals=0
        ),
        name="near",
    )(idx, weights, *parts)


GROUP = 8


def far_kernel(lst_ref, num_ref, area_ref, w_hbm, le, lm, re, rm, up, dn, l3, r3, part_ref, out_ref, mass_ref, src, wbuf, sem, wsem):
    todo = []
    for n, (e, m) in enumerate(((le, lm), (re, rm))):
        at = n * PAD + R
        todo.append((e, 0, E, at))
        todo.append((m, 0, MID, at + E))
        todo.append((e, E, E, at + E + MID))
        todo.append((up, n * R, R, n * PAD))
        todo.append((dn, n * R, R, n * PAD + R + ROWS))
    todo.append((l3, 0, E, FAR))
    todo.append((r3, 0, E, FAR + E))
    copies = [
        pltpu.make_async_copy(ref.at[pl.ds(a, n)], src.at[pl.ds(to, n)], sem.at[i])
        for i, (ref, a, n, to) in enumerate(todo)
    ]
    for copy in copies:
        copy.start()
    groups = num_ref[0]

    def entry(g, j):
        v = lst_ref[g * GROUP + j]
        slot = lax.shift_right_logical(v, 9)
        return lax.shift_right_logical(slot, 3), slot & (KMAX - 1), v & 511

    def weight_copy(g, j):
        t, k, _ = entry(g, j)
        return pltpu.make_async_copy(w_hbm.at[t, k], wbuf.at[g * GROUP + j], wsem.at[g])

    def issue(g, carry):
        for j in range(GROUP):
            weight_copy(g, j).start()
        return carry

    lax.fori_loop(0, groups, issue, 0)
    out_ref[...] = part_ref[...]
    src[FAR + 2 * E] = jnp.zeros((C, C), src.dtype)
    for copy in copies:
        copy.wait()

    def work(g, carry):
        for j in range(GROUP):
            weight_copy(g, j).wait()
        got = []
        for j in range(GROUP):
            t, _, s = entry(g, j)
            got.append(
                (t, lax.dot_general(src[s], wbuf[g * GROUP + j], NT, preferred_element_type=jnp.float32))
            )
        for t, d in got:
            out_ref[t] = out_ref[t] + d
        return carry

    lax.fori_loop(0, groups, work, 0)

    def add_up(t, acc):
        return acc + area_ref[t] * out_ref[t]

    acc = lax.fori_loop(0, ROWS, add_up, jnp.zeros((C, C), jnp.float32), unroll=4)
    mass_ref[...] = lax.dot_general(
        jnp.ones((8, C), jnp.float32), acc, NT,
        precision=lax.Precision.HIGHEST, preferred_element_type=jnp.float32,
    )


def far_call(lst, num, area, weights, parts, partial):
    smem = pl.BlockSpec(memory_space=pltpu.SMEM)
    hbm = pl.BlockSpec(memory_space=pltpu.HBM)
    vmem = pl.BlockSpec(memory_space=pltpu.VMEM)
    return pl.pallas_call(
        far_kernel,
        in_specs=[smem, smem, smem, hbm] + [hbm] * len(parts) + [vmem],
        out_specs=[vmem, vmem],
        out_shape=[
            jax.ShapeDtypeStruct((ROWS, C, C), jnp.float32),
            jax.ShapeDtypeStruct((8, C), jnp.float32),
        ],
        scratch_shapes=[
            pltpu.VMEM((FAR + 2 * E + 1, C, C), jnp.bfloat16),
            pltpu.VMEM((ROWS * KMAX, C, C), jnp.bfloat16),
            pltpu.SemaphoreType.DMA((12,)),
            pltpu.SemaphoreType.DMA((ROWS * KMAX // GROUP,)),
        ],
        compiler_params=pltpu.CompilerParams(vmem_limit_bytes=40 << 20),
        cost_estimate=pl.CostEstimate(
            flops=2 * ROWS * KMAX * C**3 // 2, bytes_accessed=20 << 20, transcendentals=0
        ),
        name="far",
    )(lst, num, area, weights, *parts, partial)


def latitude_area(first_row, count_rows):
    rows_all = jnp.arange(count_rows, dtype=jnp.int32) + first_row
    angle = -0.5 * math.pi + (rows_all.astype(jnp.float32) + 0.5) * (math.pi / NLAT)
    return jnp.cos(angle)


def slots(source_row, source_block, slot_count, lat, lon):
    row = source_row[:, 0, :].T - (lat * ROWS - R)
    row = jnp.clip(row, 0, PAD - 1)
    rel = (source_block[:, 0, :].T - lon + 3) % NLON_DEV - 3
    active = jnp.arange(KMAX, dtype=jnp.int32)[:, None] < slot_count[:, 0][None, :]
    size = jnp.abs(rel)
    side = (rel > 0).astype(jnp.int32)
    is_near = active & (size <= 1)
    near = jnp.where(is_near, jnp.where(rel == 0, 0, side + 1) * PAD + row, 3 * PAD)
    polar_row = jnp.clip(jnp.where(lat == 0, row - R, row - R - (ROWS - E)), 0, E - 1)
    far = jnp.where(size >= 3, FAR + side * E + polar_row, side * PAD + row)
    is_far = active & (size >= 2)
    target = jnp.arange(ROWS, dtype=jnp.int32)[None, :]
    slot = target * KMAX + jnp.arange(KMAX, dtype=jnp.int32)[:, None]
    order = jnp.where(is_far, slot, ROWS * KMAX + slot)
    zero = FAR + 2 * E
    packed = (order * 512 + jnp.where(is_far, far, zero)).reshape(-1)
    packed = jnp.sort(packed) & (ROWS * KMAX * 512 - 1)
    groups = (jnp.sum(is_far.astype(jnp.int32)) + GROUP - 1) // GROUP
    return near.astype(jnp.int32), packed.astype(jnp.int32), groups.reshape(1)


def everywhere(tracers, weights, source_row, source_block, slot_count):
    lat, lon = lax.axis_index("lat"), lax.axis_index("lon")
    q = tracers.transpose(0, 2, 3, 1).reshape(ROWS, C, C)
    qe = jnp.concatenate([q[:E], q[ROWS - E :]], axis=0)
    qm = q[E : ROWS - E]
    le, re = (lax.ppermute(qe, "lon", ring(1)), lax.ppermute(qe, "lon", ring(-1)))
    lm, rm = (lax.ppermute(qm, "lon", ring(1)), lax.ppermute(qm, "lon", ring(-1)))
    near_idx, far_list, far_groups = slots(source_row, source_block, slot_count, lat, lon)
    area = latitude_area(lat * ROWS, ROWS)
    total_area = C * NLON_DEV * jnp.sum(latitude_area(0, NLAT))
    mass_old = jnp.sum(area[:, None, None] * q.astype(jnp.float32), axis=(0, 2))

    up1 = lax.ppermute(jnp.concatenate([v[2 * E - R :] for v in (qe, le, re)], axis=0), "lat", UP)
    dn1 = lax.ppermute(jnp.concatenate([v[:R] for v in (qe, le, re)], axis=0), "lat", DOWN)
    lle, rre = (lax.ppermute(le, "lon", ring(1)), lax.ppermute(re, "lon", ring(-1)))
    llm, rrm = (lax.ppermute(lm, "lon", ring(1)), lax.ppermute(rm, "lon", ring(-1)))
    up2 = lax.ppermute(jnp.concatenate([v[2 * E - R :] for v in (lle, rre)], axis=0), "lat", UP)
    dn2 = lax.ppermute(jnp.concatenate([v[:R] for v in (lle, rre)], axis=0), "lat", DOWN)
    pole = [jnp.where(lat == 0, v[:E], v[E:]) for v in (lle, rre)]
    l3 = lax.ppermute(pole[0], ("lat", "lon"), polar(1))
    r3 = lax.ppermute(pole[1], ("lat", "lon"), polar(-1))

    w = weights[:, 0]
    partial = near_call(near_idx, w, (q, le, lm, re, rm, up1, dn1))
    advected, mass_new = far_call(
        far_list, far_groups, area, w, (lle, llm, rre, rrm, up2, dn2, l3, r3), partial
    )
    change = lax.psum(mass_old - mass_new[0], ("lat", "lon"))
    fixed = advected + (change / total_area)[None, :, None]
    return fixed


TOTAL_AREA = C * NLON_DEV * math.fsum(
    math.cos(-0.5 * math.pi + (j + 0.5) * math.pi / NLAT) for j in range(NLAT)
)
EDGE = 16
S = 2 * EDGE
M = ROWS - S
B = 16
SIDE = S + M + B + R
FAR2 = 2 * SIDE
SECT = 7 * PAD
CHUNKS = 4
PER = ROWS // CHUNKS
POLAR, NEXT = ((0, NLAT_DEV - 1), (1, NLAT_DEV - 2))


def some(by, lats):
    return [
        (a * NLON_DEV + i, a * NLON_DEV + (i + by) % NLON_DEV) for a in lats for i in range(NLON_DEV)
    ]


WC = 16
WT = ROWS // WC


def sums_kernel(idx_ref, area_ref, w_hbm, *refs):
    outs, (wv, acc, sem) = refs[:-3], refs[-3:]

    def copy(c):
        rows = pl.ds(c * WT, WT)
        return pltpu.make_async_copy(w_hbm.at[rows], wv.at[rows], sem.at[c])

    def start(c, carry):
        copy(c).start()
        return carry

    lax.fori_loop(0, WC, start, 0)
    acc[...] = jnp.zeros(acc.shape, acc.dtype)

    def work(c, carry):
        copy(c).wait()
        for j in range(WT):
            t = c * WT + j
            for k in range(KMAX):
                part = jnp.sum(wv[t, k].astype(jnp.float32).reshape(C // 8, 8, C), axis=0)
                at = idx_ref[k, t]
                acc[at] = acc[at] + area_ref[t] * part
        return carry

    lax.fori_loop(0, WC, work, 0)
    for n, out in enumerate(outs):
        out[...] = jnp.sum(acc[n * PAD : (n + 1) * PAD], axis=1)


def sums_call(idx, area, weights):
    smem = pl.BlockSpec(memory_space=pltpu.SMEM)
    vmem = pl.BlockSpec(memory_space=pltpu.VMEM)
    return pl.pallas_call(
        sums_kernel,
        in_specs=[smem, smem, pl.BlockSpec(memory_space=pltpu.HBM)],
        out_specs=[vmem] * 7,
        out_shape=[jax.ShapeDtypeStruct((PAD, C), jnp.float32)] * 7,
        scratch_shapes=[
            pltpu.VMEM(weights.shape, weights.dtype),
            pltpu.VMEM((SECT + 1, 8, C), jnp.float32),
            pltpu.SemaphoreType.DMA((WC,)),
        ],
        compiler_params=pltpu.CompilerParams(vmem_limit_bytes=22 << 20),
        cost_estimate=pl.CostEstimate(
            flops=20_000_000, bytes_accessed=17 << 20, transcendentals=0
        ),
        name="sums",
    )(idx, area, pltpu.with_memory_space_constraint(weights, pltpu.HBM))


def inner_kernel(idx_ref, w_hbm, own, ls, lm, rs, rm, up, dn, out_ref, wv, src, sem):
    def copy(c):
        rows = pl.ds(c * WT, WT)
        return pltpu.make_async_copy(w_hbm.at[rows], wv.at[rows], sem.at[c])

    def start(c, carry):
        copy(c).start()
        return carry

    lax.fori_loop(0, WC, start, 0)
    src[pl.ds(R, ROWS)] = own[...]
    for n, (e, m) in enumerate(((ls, lm), (rs, rm))):
        at = (n + 1) * PAD + R
        src[pl.ds(at, EDGE)] = e[:EDGE]
        src[pl.ds(at + EDGE, M)] = m[...]
        src[pl.ds(at + EDGE + M, EDGE)] = e[EDGE:]
    for n in range(3):
        src[pl.ds(n * PAD, R)] = up[pl.ds(n * R, R)]
        src[pl.ds(n * PAD + R + ROWS, R)] = dn[pl.ds(n * R, R)]
    src[3 * PAD] = jnp.zeros((C, C), src.dtype)

    def body(c, carry):
        copy(c).wait()
        for j in range(WT):
            t = c * WT + j
            lhs = jnp.concatenate([src[idx_ref[k, t]] for k in range(KMAX)], axis=1)
            rhs = jnp.concatenate([wv[t, k] for k in range(KMAX)], axis=1)
            out_ref[t] = lax.dot_general(lhs, rhs, NT, preferred_element_type=jnp.float32)
        return carry

    lax.fori_loop(0, WC, body, 0)


def inner_call(idx, weights, parts):
    vmem = pl.BlockSpec(memory_space=pltpu.VMEM)
    return pl.pallas_call(
        inner_kernel,
        in_specs=[pl.BlockSpec(memory_space=pltpu.SMEM), pl.BlockSpec(memory_space=pltpu.HBM)]
        + [vmem] * len(parts),
        out_specs=[vmem, vmem],
        out_shape=[
            pltpu.VMEM((ROWS, C, C), jnp.float32),
            pltpu.VMEM(weights.shape, weights.dtype),
        ],
        scratch_shapes=[
            pltpu.VMEM((3 * PAD + 1, C, C), jnp.bfloat16),
            pltpu.SemaphoreType.DMA((WC,)),
        ],
        compiler_params=pltpu.CompilerParams(vmem_limit_bytes=10 << 20),
        cost_estimate=pl.CostEstimate(
            flops=2 * ROWS * KMAX * C**3, bytes_accessed=17 << 20, transcendentals=0
        ),
        name="inner",
    )(idx, pltpu.with_memory_space_constraint(weights, pltpu.HBM), *parts)


def outer_kernel(idx_ref, w_ref, corr_ref, ls, lm, lb, rs, rm, rb, halo, l3, r3, part_ref, out_hbm, src, acc, sem):
    for n, (e, m, b) in enumerate(((ls, lm, lb), (rs, rm, rb))):
        at = n * SIDE
        src[pl.ds(at, S)] = e[...]
        src[pl.ds(at + S, M)] = m[...]
        src[pl.ds(at + S + M, B)] = b[...]
        src[pl.ds(at + S + M + B, R)] = halo[pl.ds(n * R, R)]
    src[pl.ds(FAR2, E)] = l3[...]
    src[pl.ds(FAR2 + E, E)] = r3[...]
    src[FAR2 + 2 * E] = jnp.zeros((C, C), src.dtype)

    def out_copy(c):
        rows = pl.ds(c * PER, PER)
        return pltpu.make_async_copy(acc.at[rows], out_hbm.at[rows], sem.at[c])

    for c in range(CHUNKS):

        def body(t, carry):
            lhs = jnp.concatenate([src[idx_ref[k, t]] for k in range(KMAX)], axis=1)
            rhs = jnp.concatenate([w_ref[t, k] for k in range(KMAX)], axis=1)
            got = lax.dot_general(lhs, rhs, NT, preferred_element_type=jnp.float32)
            acc[t] = (got + part_ref[t]) + corr_ref[...]
            return carry

        lax.fori_loop(c * PER, (c + 1) * PER, body, 0, unroll=4)
        out_copy(c).start()
    for c in range(CHUNKS):
        out_copy(c).wait()


def outer_call(idx, weights, corr, parts, partial):
    vmem = pl.BlockSpec(memory_space=pltpu.VMEM)
    return pl.pallas_call(
        outer_kernel,
        in_specs=[pl.BlockSpec(memory_space=pltpu.SMEM)] + [vmem] * (3 + len(parts)),
        out_specs=pl.BlockSpec(memory_space=pltpu.HBM),
        out_shape=jax.ShapeDtypeStruct((ROWS, C, C), jnp.float32),
        scratch_shapes=[
            pltpu.VMEM((FAR2 + 2 * E + 1, C, C), jnp.bfloat16),
            pltpu.VMEM((ROWS, C, C), jnp.float32),
            pltpu.SemaphoreType.DMA((CHUNKS,)),
        ],
        compiler_params=pltpu.CompilerParams(vmem_limit_bytes=14 << 20),
        cost_estimate=pl.CostEstimate(
            flops=2 * ROWS * KMAX * C**3, bytes_accessed=4 << 20, transcendentals=0
        ),
        name="outer",
    )(idx, weights, corr, *parts, partial)


def tables(source_row, source_block, slot_count, lat, lon):
    p = source_row[:, 0, :].T - (lat * ROWS - R)
    p = jnp.clip(p, 0, PAD - 1)
    rel = (source_block[:, 0, :].T - lon + 3) % NLON_DEV - 3
    rel = jnp.clip(rel, -3, 3)
    active = jnp.arange(KMAX, dtype=jnp.int32)[:, None] < slot_count[:, 0][None, :]
    sums_idx = jnp.where(active, (rel + 3) * PAD + p, SECT)
    size = jnp.abs(rel)
    side = (rel > 0).astype(jnp.int32)
    near_idx = jnp.where(
        active & (size <= 1), jnp.where(rel == 0, 0, side + 1) * PAD + p, 3 * PAD
    )
    r = p - R
    is_polar = (lat == 0) | (lat == NLAT_DEV - 1)
    in_band = jnp.where(r < EDGE, r, jnp.where(r < EDGE + M, r - EDGE + S, r - M))
    below = lat == NLAT_DEV - 2
    in_next = S + M + jnp.where(below, r - (ROWS - B), r)
    halo = S + M + B + jnp.where(r < 0, r + R, r - ROWS)
    two = jnp.where((r < 0) | (r >= ROWS), halo, jnp.where(is_polar, in_band, in_next))
    polar_row = jnp.clip(jnp.where(lat == 0, r, r - (ROWS - E)), 0, E - 1)
    far = jnp.where(size >= 3, FAR2 + side * E + polar_row, side * SIDE + two)
    is_far = active & (size >= 2)
    held = is_polar | ((lat == 1) & (r < B)) | (below & (r >= ROWS - B))
    lost = jnp.sum((is_far & ~held).astype(jnp.float32))
    far_idx = jnp.where(is_far & held, far, FAR2 + 2 * E)
    return sums_idx, near_idx, far_idx, lost


def swap(v, axis, size, to):
    return lax.ppermute(v, axis, [(i, to(i)) for i in range(size)])


def local(tracers, weights, source_row, source_block, slot_count):
    args = (tracers, weights, source_row, source_block, slot_count)
    lost, fixed = usual(*args)

    def redo(state):
        return jnp.zeros_like(state[0]), everywhere(*args)

    _, fixed = lax.while_loop(lambda state: state[0] > 0, redo, (lost, fixed))
    return fixed.reshape(ROWS, 32, 4, C).transpose(0, 3, 1, 2)


def usual(tracers, weights, source_row, source_block, slot_count):
    lat, lon = lax.axis_index("lat"), lax.axis_index("lon")
    both = ("lat", "lon")
    w = weights[:, 0]
    q = tracers.transpose(0, 2, 3, 1).reshape(ROWS, C, C)
    qs = jnp.concatenate([q[:EDGE], q[ROWS - EDGE :]], axis=0)
    ls, rs = lax.ppermute(qs, "lon", ring(1)), lax.ppermute(qs, "lon", ring(-1))
    sums_idx, near_idx, far_idx, lost = tables(source_row, source_block, slot_count, lat, lon)
    area = latitude_area(lat * ROWS, ROWS)
    sums = sums_call(sums_idx, area, w)
    got = sums[3]
    for d in (1, -1, 2, -2):
        got = got + lax.ppermute(sums[d + 3], "lon", ring(d))
    for d in (3, -3):
        got = got + lax.ppermute(sums[d + 3], both, some(d, POLAR))
    qm = q[EDGE : ROWS - EDGE]
    lm, rm = lax.ppermute(qm, "lon", ring(1)), lax.ppermute(qm, "lon", ring(-1))
    up1 = lax.ppermute(jnp.concatenate([v[S - R :] for v in (qs, ls, rs)], axis=0), "lat", UP)
    dn1 = lax.ppermute(jnp.concatenate([v[:R] for v in (qs, ls, rs)], axis=0), "lat", DOWN)

    def weigh(field, by):
        return jnp.sum(field.astype(jnp.float32) * by[:, None, :], axis=(0, 2))

    change = (
        weigh(q, area[:, None] - got[R : R + ROWS])
        - weigh(up1[:R], got[:R])
        - weigh(dn1[:R], got[R + ROWS :])
    )
    v = jnp.stack([change, jnp.full((C,), lost)])
    v = v + swap(v, "lat", NLAT_DEV, lambda i: i ^ 1)
    v = v + swap(v, "lat", NLAT_DEV, lambda i: i ^ 2)
    v = v + swap(v, "lat", NLAT_DEV, lambda i: i ^ 4)
    y = [swap(v, "lon", NLON_DEV, lambda i, by=by: i // 4 * 4 + (i + by) % 4) for by in (1, 2, 3)]
    v = v + (y[0] + y[2]) + y[1]
    v = v + swap(v, "lon", NLON_DEV, lambda i: i ^ 4)
    v = v + swap(v, "lon", NLON_DEV, lambda i: i ^ 8)
    corr = jnp.broadcast_to((v[0] * (1.0 / TOTAL_AREA))[:, None], (C, C))

    lls, rrs = (lax.ppermute(x, both, some(d, POLAR)) for x, d in ((ls, 1), (rs, -1)))
    llm, rrm = (lax.ppermute(x, both, some(d, POLAR)) for x, d in ((lm, 1), (rm, -1)))

    def next_rows(e):
        return jnp.where(lat == 1, e[:B], e[S - B :])

    llb = lax.ppermute(next_rows(ls), both, some(1, NEXT))
    rrb = lax.ppermute(next_rows(rs), both, some(-1, NEXT))

    def border(e, b):
        of_polar = jnp.where(lat == 0, e[S - R :], e[:R])
        return jnp.where(
            (lat == 0) | (lat == NLAT_DEV - 1), of_polar, jnp.where(lat == 1, b[:R], b[B - R :])
        )

    pairs = [(a * NLON_DEV + i, b * NLON_DEV + i) for a, b in ((0, 1), (1, 0), (6, 7), (7, 6)) for i in range(NLON_DEV)]
    halo = lax.ppermute(jnp.concatenate([border(lls, llb), border(rrs, rrb)], axis=0), both, pairs)
    pole = [jnp.where(lat == 0, x[:E], x[S - E :]) for x in (lls, rrs)]
    l3 = lax.ppermute(pole[0], both, some(1, POLAR))
    r3 = lax.ppermute(pole[1], both, some(-1, POLAR))

    partial, wv = inner_call(near_idx, w, (q, ls, lm, rs, rm, up1, dn1))
    fixed = outer_call(
        far_idx, pltpu.with_memory_space_constraint(wv, pltpu.VMEM), corr, (lls, llm, llb, rrs, rrm, rrb, halo, l3, r3),
        pltpu.with_memory_space_constraint(partial, pltpu.VMEM),
    )
    return v[1, 0], fixed


def solution(mesh):
    placed = (
        P("lat", "lon", None, None),
        P("lat", "lon", None, None, None),
        P("lat", "lon", None),
        P("lat", "lon", None),
        P("lat", "lon"),
    )
    return jax.shard_map(
        local, mesh=mesh, in_specs=placed, out_specs=P("lat", "lon", None, None), check_vma=False
    )
```

```python
import math

import jax
import jax.numpy as jnp
from jax import lax
from jax.experimental import pallas as pl
from jax.experimental.pallas import tpu as pltpu
from jax.sharding import PartitionSpec as P

ROWS = 64
C = 128
KMAX = 8
R = 4
E = R + 1
MID = ROWS - 2 * E
PAD = ROWS + 2 * R
NLAT, NLON_DEV, NLAT_DEV = 512, 16, 8
TB = 4
FAR = 2 * PAD
NT = (((1,), (1,)), ((), ()))


def ring(by):
    return [(i, (i + by) % NLON_DEV) for i in range(NLON_DEV)]


UP = [(i, i + 1) for i in range(NLAT_DEV - 1)]
DOWN = [(i + 1, i) for i in range(NLAT_DEV - 1)]


def polar(by):
    return [
        (a * NLON_DEV + i, a * NLON_DEV + (i + by) % NLON_DEV)
        for a in (0, NLAT_DEV - 1)
        for i in range(NLON_DEV)
    ]


def near_kernel(idx_ref, w_ref, *refs):
    parts, (out_ref, src, sem) = refs[:-3], refs[-3:]
    step = pl.program_id(0)
    own, le, lm, re, rm, up, dn = parts

    def copies():
        todo = [(own, 0, ROWS, 0 * PAD + R)]
        for n, (e, m) in enumerate(((le, lm), (re, rm))):
            at = (n + 1) * PAD + R
            todo.append((e, 0, E, at))
            todo.append((m, 0, MID, at + E))
            todo.append((e, E, E, at + E + MID))
        for n in range(3):
            todo.append((up, n * R, R, n * PAD))
            todo.append((dn, n * R, R, n * PAD + R + ROWS))
        return [
            pltpu.make_async_copy(ref.at[pl.ds(a, n)], src.at[pl.ds(to, n)], sem.at[i])
            for i, (ref, a, n, to) in enumerate(todo)
        ]

    @pl.when(step == 0)
    def _():
        for copy in copies():
            copy.start()
        src[3 * PAD] = jnp.zeros((C, C), src.dtype)
        for copy in copies():
            copy.wait()

    for j in range(TB):
        t = step * TB + j
        lhs = jnp.concatenate([src[idx_ref[k, t]] for k in range(KMAX)], axis=1)
        rhs = jnp.concatenate([w_ref[j, k] for k in range(KMAX)], axis=1)
        out_ref[j] = lax.dot_general(lhs, rhs, NT, preferred_element_type=jnp.float32)


def near_call(idx, weights, parts):
    n_copies = 7 + 6
    return pl.pallas_call(
        near_kernel,
        grid_spec=pltpu.PrefetchScalarGridSpec(
            num_scalar_prefetch=1,
            grid=(ROWS // TB,),
            in_specs=[pl.BlockSpec((TB, KMAX, C, C), lambda s, i: (s, 0, 0, 0))]
            + [pl.BlockSpec(memory_space=pltpu.HBM)] * len(parts),
            out_specs=pl.BlockSpec((TB, C, C), lambda s, i: (s, 0, 0)),
            scratch_shapes=[
                pltpu.VMEM((3 * PAD + 1, C, C), jnp.bfloat16),
                pltpu.SemaphoreType.DMA((n_copies,)),
            ],
        ),
        out_shape=jax.ShapeDtypeStruct((ROWS, C, C), jnp.float32),
        compiler_params=pltpu.CompilerParams(
            dimension_semantics=("arbitrary",), vmem_limit_bytes=20 << 20
        ),
        cost_estimate=pl.CostEstimate(
            flops=2 * ROWS * KMAX * C**3, bytes_accessed=28 << 20, transcendentals=0
        ),
        name="near",
    )(idx, weights, *parts)


GROUP = 8


def far_kernel(lst_ref, num_ref, area_ref, w_hbm, le, lm, re, rm, up, dn, l3, r3, part_ref, out_ref, mass_ref, src, wbuf, sem, wsem):
    todo = []
    for n, (e, m) in enumerate(((le, lm), (re, rm))):
        at = n * PAD + R
        todo.append((e, 0, E, at))
        todo.append((m, 0, MID, at + E))
        todo.append((e, E, E, at + E + MID))
        todo.append((up, n * R, R, n * PAD))
        todo.append((dn, n * R, R, n * PAD + R + ROWS))
    todo.append((l3, 0, E, FAR))
    todo.append((r3, 0, E, FAR + E))
    copies = [
        pltpu.make_async_copy(ref.at[pl.ds(a, n)], src.at[pl.ds(to, n)], sem.at[i])
        for i, (ref, a, n, to) in enumerate(todo)
    ]
    for copy in copies:
        copy.start()
    groups = num_ref[0]

    def entry(g, j):
        v = lst_ref[g * GROUP + j]
        slot = lax.shift_right_logical(v, 9)
        return lax.shift_right_logical(slot, 3), slot & (KMAX - 1), v & 511

    def weight_copy(g, j):
        t, k, _ = entry(g, j)
        return pltpu.make_async_copy(w_hbm.at[t, k], wbuf.at[g * GROUP + j], wsem.at[g])

    def issue(g, carry):
        for j in range(GROUP):
            weight_copy(g, j).start()
        return carry

    lax.fori_loop(0, groups, issue, 0)
    out_ref[...] = part_ref[...]
    src[FAR + 2 * E] = jnp.zeros((C, C), src.dtype)
    for copy in copies:
        copy.wait()

    def work(g, carry):
        for j in range(GROUP):
            weight_copy(g, j).wait()
        got = []
        for j in range(GROUP):
            t, _, s = entry(g, j)
            got.append(
                (t, lax.dot_general(src[s], wbuf[g * GROUP + j], NT, preferred_element_type=jnp.float32))
            )
        for t, d in got:
            out_ref[t] = out_ref[t] + d
        return carry

    lax.fori_loop(0, groups, work, 0)

    def add_up(t, acc):
        return acc + area_ref[t] * out_ref[t]

    acc = lax.fori_loop(0, ROWS, add_up, jnp.zeros((C, C), jnp.float32), unroll=4)
    mass_ref[...] = lax.dot_general(
        jnp.ones((8, C), jnp.float32), acc, NT,
        precision=lax.Precision.HIGHEST, preferred_element_type=jnp.float32,
    )


def far_call(lst, num, area, weights, parts, partial):
    smem = pl.BlockSpec(memory_space=pltpu.SMEM)
    hbm = pl.BlockSpec(memory_space=pltpu.HBM)
    vmem = pl.BlockSpec(memory_space=pltpu.VMEM)
    return pl.pallas_call(
        far_kernel,
        in_specs=[smem, smem, smem, hbm] + [hbm] * len(parts) + [vmem],
        out_specs=[vmem, vmem],
        out_shape=[
            jax.ShapeDtypeStruct((ROWS, C, C), jnp.float32),
            jax.ShapeDtypeStruct((8, C), jnp.float32),
        ],
        scratch_shapes=[
            pltpu.VMEM((FAR + 2 * E + 1, C, C), jnp.bfloat16),
            pltpu.VMEM((ROWS * KMAX, C, C), jnp.bfloat16),
            pltpu.SemaphoreType.DMA((12,)),
            pltpu.SemaphoreType.DMA((ROWS * KMAX // GROUP,)),
        ],
        compiler_params=pltpu.CompilerParams(vmem_limit_bytes=40 << 20),
        cost_estimate=pl.CostEstimate(
            flops=2 * ROWS * KMAX * C**3 // 2, bytes_accessed=20 << 20, transcendentals=0
        ),
        name="far",
    )(lst, num, area, weights, *parts, partial)


def latitude_area(first_row, count_rows):
    rows_all = jnp.arange(count_rows, dtype=jnp.int32) + first_row
    angle = -0.5 * math.pi + (rows_all.astype(jnp.float32) + 0.5) * (math.pi / NLAT)
    return jnp.cos(angle)


def slots(source_row, source_block, slot_count, lat, lon):
    row = source_row[:, 0, :].T - (lat * ROWS - R)
    row = jnp.clip(row, 0, PAD - 1)
    rel = (source_block[:, 0, :].T - lon + 3) % NLON_DEV - 3
    active = jnp.arange(KMAX, dtype=jnp.int32)[:, None] < slot_count[:, 0][None, :]
    size = jnp.abs(rel)
    side = (rel > 0).astype(jnp.int32)
    is_near = active & (size <= 1)
    near = jnp.where(is_near, jnp.where(rel == 0, 0, side + 1) * PAD + row, 3 * PAD)
    polar_row = jnp.clip(jnp.where(lat == 0, row - R, row - R - (ROWS - E)), 0, E - 1)
    far = jnp.where(size >= 3, FAR + side * E + polar_row, side * PAD + row)
    is_far = active & (size >= 2)
    target = jnp.arange(ROWS, dtype=jnp.int32)[None, :]
    slot = target * KMAX + jnp.arange(KMAX, dtype=jnp.int32)[:, None]
    order = jnp.where(is_far, slot, ROWS * KMAX + slot)
    zero = FAR + 2 * E
    packed = (order * 512 + jnp.where(is_far, far, zero)).reshape(-1)
    packed = jnp.sort(packed) & (ROWS * KMAX * 512 - 1)
    groups = (jnp.sum(is_far.astype(jnp.int32)) + GROUP - 1) // GROUP
    return near.astype(jnp.int32), packed.astype(jnp.int32), groups.reshape(1)


def everywhere(tracers, weights, source_row, source_block, slot_count):
    lat, lon = lax.axis_index("lat"), lax.axis_index("lon")
    q = tracers.transpose(0, 2, 3, 1).reshape(ROWS, C, C)
    qe = jnp.concatenate([q[:E], q[ROWS - E :]], axis=0)
    qm = q[E : ROWS - E]
    le, re = (lax.ppermute(qe, "lon", ring(1)), lax.ppermute(qe, "lon", ring(-1)))
    lm, rm = (lax.ppermute(qm, "lon", ring(1)), lax.ppermute(qm, "lon", ring(-1)))
    near_idx, far_list, far_groups = slots(source_row, source_block, slot_count, lat, lon)
    area = latitude_area(lat * ROWS, ROWS)
    total_area = C * NLON_DEV * jnp.sum(latitude_area(0, NLAT))
    mass_old = jnp.sum(area[:, None, None] * q.astype(jnp.float32), axis=(0, 2))

    up1 = lax.ppermute(jnp.concatenate([v[2 * E - R :] for v in (qe, le, re)], axis=0), "lat", UP)
    dn1 = lax.ppermute(jnp.concatenate([v[:R] for v in (qe, le, re)], axis=0), "lat", DOWN)
    lle, rre = (lax.ppermute(le, "lon", ring(1)), lax.ppermute(re, "lon", ring(-1)))
    llm, rrm = (lax.ppermute(lm, "lon", ring(1)), lax.ppermute(rm, "lon", ring(-1)))
    up2 = lax.ppermute(jnp.concatenate([v[2 * E - R :] for v in (lle, rre)], axis=0), "lat", UP)
    dn2 = lax.ppermute(jnp.concatenate([v[:R] for v in (lle, rre)], axis=0), "lat", DOWN)
    pole = [jnp.where(lat == 0, v[:E], v[E:]) for v in (lle, rre)]
    l3 = lax.ppermute(pole[0], ("lat", "lon"), polar(1))
    r3 = lax.ppermute(pole[1], ("lat", "lon"), polar(-1))

    w = weights[:, 0]
    partial = near_call(near_idx, w, (q, le, lm, re, rm, up1, dn1))
    advected, mass_new = far_call(
        far_list, far_groups, area, w, (lle, llm, rre, rrm, up2, dn2, l3, r3), partial
    )
    change = lax.psum(mass_old - mass_new[0], ("lat", "lon"))
    fixed = advected + (change / total_area)[None, :, None]
    return fixed


TOTAL_AREA = C * NLON_DEV * math.fsum(
    math.cos(-0.5 * math.pi + (j + 0.5) * math.pi / NLAT) for j in range(NLAT)
)
EDGE = 16
S = 2 * EDGE
M = ROWS - S
B = 16
SIDE = S + M + B + R
FAR2 = 2 * SIDE
SECT = 7 * PAD
CHUNKS = 4
PER = ROWS // CHUNKS
POLAR, NEXT = ((0, NLAT_DEV - 1), (1, NLAT_DEV - 2))


def some(by, lats):
    return [
        (a * NLON_DEV + i, a * NLON_DEV + (i + by) % NLON_DEV) for a in lats for i in range(NLON_DEV)
    ]


WC = 16
WT = ROWS // WC


def sums_kernel(idx_ref, area_ref, w_hbm, *refs):
    outs, (wv, acc, sem) = refs[:-3], refs[-3:]

    def copy(c):
        rows = pl.ds(c * WT, WT)
        return pltpu.make_async_copy(w_hbm.at[rows], wv.at[rows], sem.at[c])

    def start(c, carry):
        copy(c).start()
        return carry

    lax.fori_loop(0, WC, start, 0)
    acc[...] = jnp.zeros(acc.shape, acc.dtype)

    def work(c, carry):
        copy(c).wait()
        for j in range(WT):
            t = c * WT + j
            for k in range(KMAX):
                part = jnp.sum(wv[t, k].astype(jnp.float32).reshape(C // 8, 8, C), axis=0)
                at = idx_ref[k, t]
                acc[at] = acc[at] + area_ref[t] * part
        return carry

    lax.fori_loop(0, WC, work, 0)
    for n, out in enumerate(outs):
        out[...] = jnp.sum(acc[n * PAD : (n + 1) * PAD], axis=1)


def sums_call(idx, area, weights):
    smem = pl.BlockSpec(memory_space=pltpu.SMEM)
    vmem = pl.BlockSpec(memory_space=pltpu.VMEM)
    return pl.pallas_call(
        sums_kernel,
        in_specs=[smem, smem, pl.BlockSpec(memory_space=pltpu.HBM)],
        out_specs=[vmem] * 7,
        out_shape=[jax.ShapeDtypeStruct((PAD, C), jnp.float32)] * 7,
        scratch_shapes=[
            pltpu.VMEM(weights.shape, weights.dtype),
            pltpu.VMEM((SECT + 1, 8, C), jnp.float32),
            pltpu.SemaphoreType.DMA((WC,)),
        ],
        compiler_params=pltpu.CompilerParams(vmem_limit_bytes=22 << 20),
        cost_estimate=pl.CostEstimate(
            flops=20_000_000, bytes_accessed=17 << 20, transcendentals=0
        ),
        name="sums",
    )(idx, area, pltpu.with_memory_space_constraint(weights, pltpu.HBM))


def mass_kernel(area_ref, lost_ref, at_ref, c0, c1, c2, c3, c4, s3m, s3p, q, up, dn, l3, r3, out_ref, by):
    by[...] = -(((c0[...] + c1[...]) + (c2[...] + c3[...])) + c4[...])
    acc = jnp.zeros((C, C), jnp.float32)
    for i in range(R):
        acc = acc + by[i : i + 1] * up[i].astype(jnp.float32)
        acc = acc + by[R + ROWS + i : R + ROWS + i + 1] * dn[i].astype(jnp.float32)
    at = at_ref[0]
    for i in range(E):
        acc = acc - s3m[pl.ds(at + i, 1)] * l3[i].astype(jnp.float32)
        acc = acc - s3p[pl.ds(at + i, 1)] * r3[i].astype(jnp.float32)

    def body(r, acc):
        return acc + (by[pl.ds(r + R, 1)] + area_ref[r]) * q[r].astype(jnp.float32)

    acc = lax.fori_loop(0, ROWS, body, acc, unroll=4)
    change = lax.dot_general(
        jnp.ones((8, C), jnp.float32), acc, NT,
        precision=lax.Precision.HIGHEST, preferred_element_type=jnp.float32,
    )
    row = lax.broadcasted_iota(jnp.int32, (8, C), 0)
    out_ref[...] = jnp.where(row == 0, change, lost_ref[0])


def mass_call(area, lost, at, parts):
    smem = pl.BlockSpec(memory_space=pltpu.SMEM)
    vmem = pl.BlockSpec(memory_space=pltpu.VMEM)
    return pl.pallas_call(
        mass_kernel,
        in_specs=[smem] * 3 + [vmem] * len(parts),
        out_specs=vmem,
        out_shape=jax.ShapeDtypeStruct((8, C), jnp.float32),
        scratch_shapes=[pltpu.VMEM((PAD, C), jnp.float32)],
        compiler_params=pltpu.CompilerParams(vmem_limit_bytes=4 << 20),
        cost_estimate=pl.CostEstimate(
            flops=4_000_000, bytes_accessed=3 << 20, transcendentals=0
        ),
        name="mass",
    )(area, lost, at, *parts)


def inner_kernel(idx_ref, w_hbm, own, ls, lm, rs, rm, up, dn, out_ref, wv, src, sem):
    def copy(c):
        rows = pl.ds(c * WT, WT)
        return pltpu.make_async_copy(w_hbm.at[rows], wv.at[rows], sem.at[c])

    def start(c, carry):
        copy(c).start()
        return carry

    lax.fori_loop(0, WC, start, 0)
    src[pl.ds(R, ROWS)] = own[...]
    for n, (e, m) in enumerate(((ls, lm), (rs, rm))):
        at = (n + 1) * PAD + R
        src[pl.ds(at, EDGE)] = e[:EDGE]
        src[pl.ds(at + EDGE, M)] = m[...]
        src[pl.ds(at + EDGE + M, EDGE)] = e[EDGE:]
    for n in range(3):
        src[pl.ds(n * PAD, R)] = up[pl.ds(n * R, R)]
        src[pl.ds(n * PAD + R + ROWS, R)] = dn[pl.ds(n * R, R)]
    src[3 * PAD] = jnp.zeros((C, C), src.dtype)

    def body(c, carry):
        copy(c).wait()
        for j in range(WT):
            t = c * WT + j
            lhs = jnp.concatenate([src[idx_ref[k, t]] for k in range(KMAX)], axis=1)
            rhs = jnp.concatenate([wv[t, k] for k in range(KMAX)], axis=1)
            out_ref[t] = lax.dot_general(lhs, rhs, NT, preferred_element_type=jnp.float32)
        return carry

    lax.fori_loop(0, WC, body, 0)


def inner_call(idx, weights, parts):
    vmem = pl.BlockSpec(memory_space=pltpu.VMEM)
    return pl.pallas_call(
        inner_kernel,
        in_specs=[pl.BlockSpec(memory_space=pltpu.SMEM), pl.BlockSpec(memory_space=pltpu.HBM)]
        + [vmem] * len(parts),
        out_specs=[vmem, vmem],
        out_shape=[
            pltpu.VMEM((ROWS, C, C), jnp.float32),
            pltpu.VMEM(weights.shape, weights.dtype),
        ],
        scratch_shapes=[
            pltpu.VMEM((3 * PAD + 1, C, C), jnp.bfloat16),
            pltpu.SemaphoreType.DMA((WC,)),
        ],
        compiler_params=pltpu.CompilerParams(vmem_limit_bytes=10 << 20),
        cost_estimate=pl.CostEstimate(
            flops=2 * ROWS * KMAX * C**3, bytes_accessed=17 << 20, transcendentals=0
        ),
        name="inner",
    )(idx, pltpu.with_memory_space_constraint(weights, pltpu.HBM), *parts)


def outer_kernel(idx_ref, w_ref, corr_ref, ls, lm, lb, lh, rs, rm, rb, rh, l3, r3, part_ref, out_hbm, src, acc, sem):
    for n, (e, m, b, h) in enumerate(((ls, lm, lb, lh), (rs, rm, rb, rh))):
        at = n * SIDE
        src[pl.ds(at, S)] = e[...]
        src[pl.ds(at + S, M)] = m[...]
        src[pl.ds(at + S + M, B)] = b[...]
        src[pl.ds(at + S + M + B, R)] = h[...]
    src[pl.ds(FAR2, E)] = l3[...]
    src[pl.ds(FAR2 + E, E)] = r3[...]
    src[FAR2 + 2 * E] = jnp.zeros((C, C), src.dtype)

    def out_copy(c):
        rows = pl.ds(c * PER, PER)
        return pltpu.make_async_copy(acc.at[rows], out_hbm.at[rows], sem.at[c])

    for c in range(CHUNKS):

        def body(t, carry):
            lhs = jnp.concatenate([src[idx_ref[k, t]] for k in range(KMAX)], axis=1)
            rhs = jnp.concatenate([w_ref[t, k] for k in range(KMAX)], axis=1)
            got = lax.dot_general(lhs, rhs, NT, preferred_element_type=jnp.float32)
            acc[t] = (got + part_ref[t]) + corr_ref[...]
            return carry

        lax.fori_loop(c * PER, (c + 1) * PER, body, 0, unroll=4)
        out_copy(c).start()
    for c in range(CHUNKS):
        out_copy(c).wait()


def outer_call(idx, weights, corr, parts, partial):
    vmem = pl.BlockSpec(memory_space=pltpu.VMEM)
    return pl.pallas_call(
        outer_kernel,
        in_specs=[pl.BlockSpec(memory_space=pltpu.SMEM)] + [vmem] * (3 + len(parts)),
        out_specs=pl.BlockSpec(memory_space=pltpu.HBM),
        out_shape=jax.ShapeDtypeStruct((ROWS, C, C), jnp.float32),
        scratch_shapes=[
            pltpu.VMEM((FAR2 + 2 * E + 1, C, C), jnp.bfloat16),
            pltpu.VMEM((ROWS, C, C), jnp.float32),
            pltpu.SemaphoreType.DMA((CHUNKS,)),
        ],
        compiler_params=pltpu.CompilerParams(vmem_limit_bytes=14 << 20),
        cost_estimate=pl.CostEstimate(
            flops=2 * ROWS * KMAX * C**3, bytes_accessed=4 << 20, transcendentals=0
        ),
        name="outer",
    )(idx, weights, corr, *parts, partial)


def tables(source_row, source_block, slot_count, lat, lon):
    p = source_row[:, 0, :].T - (lat * ROWS - R)
    p = jnp.clip(p, 0, PAD - 1)
    rel = (source_block[:, 0, :].T - lon + 3) % NLON_DEV - 3
    rel = jnp.clip(rel, -3, 3)
    active = jnp.arange(KMAX, dtype=jnp.int32)[:, None] < slot_count[:, 0][None, :]
    sums_idx = jnp.where(active, (rel + 3) * PAD + p, SECT)
    size = jnp.abs(rel)
    side = (rel > 0).astype(jnp.int32)
    near_idx = jnp.where(
        active & (size <= 1), jnp.where(rel == 0, 0, side + 1) * PAD + p, 3 * PAD
    )
    r = p - R
    is_polar = (lat == 0) | (lat == NLAT_DEV - 1)
    in_band = jnp.where(r < EDGE, r, jnp.where(r < EDGE + M, r - EDGE + S, r - M))
    below = lat == NLAT_DEV - 2
    in_next = S + M + jnp.where(below, r - (ROWS - B), r)
    halo = S + M + B + jnp.where(r < 0, r + R, r - ROWS)
    two = jnp.where((r < 0) | (r >= ROWS), halo, jnp.where(is_polar, in_band, in_next))
    polar_row = jnp.clip(jnp.where(lat == 0, r, r - (ROWS - E)), 0, E - 1)
    far = jnp.where(size >= 3, FAR2 + side * E + polar_row, side * SIDE + two)
    is_far = active & (size >= 2)
    held = is_polar | ((lat == 1) & (r < B)) | (below & (r >= ROWS - B))
    lost = jnp.sum((is_far & ~held).astype(jnp.float32))
    far_idx = jnp.where(is_far & held, far, FAR2 + 2 * E)
    return sums_idx, near_idx, far_idx, lost


def swap(v, axis, size, to):
    return lax.ppermute(v, axis, [(i, to(i)) for i in range(size)])


def local(tracers, weights, source_row, source_block, slot_count):
    args = (tracers, weights, source_row, source_block, slot_count)
    lost, fixed = usual(*args)

    def redo(state):
        return jnp.zeros_like(state[0]), everywhere(*args)

    _, fixed = lax.while_loop(lambda state: state[0] > 0, redo, (lost, fixed))
    return fixed.reshape(ROWS, 32, 4, C).transpose(0, 3, 1, 2)


def usual(tracers, weights, source_row, source_block, slot_count):
    lat, lon = lax.axis_index("lat"), lax.axis_index("lon")
    both = ("lat", "lon")
    w = weights[:, 0]
    q = tracers.transpose(0, 2, 3, 1).reshape(ROWS, C, C)
    qs = jnp.concatenate([q[:EDGE], q[ROWS - EDGE :]], axis=0)
    ls, rs = lax.ppermute(qs, "lon", ring(1)), lax.ppermute(qs, "lon", ring(-1))
    pole = jnp.where(lat == 0, q[:E], q[ROWS - E :])
    l3 = lax.ppermute(pole, both, some(3, POLAR))
    r3 = lax.ppermute(pole, both, some(-3, POLAR))
    sums_idx, near_idx, far_idx, lost = tables(source_row, source_block, slot_count, lat, lon)
    area = latitude_area(lat * ROWS, ROWS)
    sums = sums_call(sums_idx, area, w)
    got = [lax.ppermute(sums[d + 3], "lon", ring(d)) for d in (1, -1, 2, -2)]
    qm = q[EDGE : ROWS - EDGE]
    lm, rm = lax.ppermute(qm, "lon", ring(1)), lax.ppermute(qm, "lon", ring(-1))
    up1 = lax.ppermute(jnp.concatenate([v[S - R :] for v in (qs, ls, rs)], axis=0), "lat", UP)
    dn1 = lax.ppermute(jnp.concatenate([v[:R] for v in (qs, ls, rs)], axis=0), "lat", DOWN)
    at = jnp.where(lat == 0, R, R + ROWS - E).reshape(1).astype(jnp.int32)
    v = mass_call(
        area, lost.reshape(1), at, (sums[3], *got, sums[0], sums[6], q, up1, dn1, l3, r3)
    )
    for axis, size, bit in (("lat", NLAT_DEV, 1), ("lat", NLAT_DEV, 2), ("lat", NLAT_DEV, 4), ("lon", NLON_DEV, 4), ("lon", NLON_DEV, 8)):
        v = v + swap(v, axis, size, lambda i, bit=bit: i ^ bit)
    y = [swap(v, "lon", NLON_DEV, lambda i, by=by: i // 4 * 4 + (i + by) % 4) for by in (1, 2, 3)]
    v = v + (y[0] + y[2]) + y[1]
    corr = jnp.broadcast_to((v[0] * (1.0 / TOTAL_AREA))[:, None], (C, C))

    lls, rrs = (lax.ppermute(x, both, some(d, POLAR)) for x, d in ((ls, 1), (rs, -1)))
    llm, rrm = (lax.ppermute(x, both, some(d, POLAR)) for x, d in ((lm, 1), (rm, -1)))

    def next_rows(e):
        return jnp.where(lat == 1, e[:B], e[S - B :])

    llb = lax.ppermute(next_rows(ls), both, some(1, NEXT))
    rrb = lax.ppermute(next_rows(rs), both, some(-1, NEXT))
    beyond = jnp.where((lat == 0) | (lat == NLAT_DEV - 2), dn1[R:], up1[R:])
    llh = lax.ppermute(beyond[:R], both, some(1, POLAR + NEXT))
    rrh = lax.ppermute(beyond[R:], both, some(-1, POLAR + NEXT))

    partial, wv = inner_call(near_idx, w, (q, ls, lm, rs, rm, up1, dn1))
    fixed = outer_call(
        far_idx, pltpu.with_memory_space_constraint(wv, pltpu.VMEM), corr, (lls, llm, llb, llh, rrs, rrm, rrb, rrh, l3, r3),
        pltpu.with_memory_space_constraint(partial, pltpu.VMEM),
    )
    return v[1, 0], fixed


def solution(mesh):
    placed = (
        P("lat", "lon", None, None),
        P("lat", "lon", None, None, None),
        P("lat", "lon", None),
        P("lat", "lon", None),
        P("lat", "lon"),
    )
    return jax.shard_map(
        local, mesh=mesh, in_specs=placed, out_specs=P("lat", "lon", None, None), check_vma=False
    )
```

```python
import functools
import math

import jax
import jax.numpy as jnp
from jax import lax
from jax.experimental import pallas as pl
from jax.experimental.pallas import tpu as pltpu
from jax.sharding import PartitionSpec as P

ROWS = 64
C = 128
KMAX = 8
R = 4
E = R + 1
MID = ROWS - 2 * E
PAD = ROWS + 2 * R
NLAT, NLON_DEV, NLAT_DEV = 512, 16, 8
TB = 4
FAR = 2 * PAD
NT = (((1,), (1,)), ((), ()))


def ring(by):
    return [(i, (i + by) % NLON_DEV) for i in range(NLON_DEV)]


UP = [(i, i + 1) for i in range(NLAT_DEV - 1)]
DOWN = [(i + 1, i) for i in range(NLAT_DEV - 1)]


def polar(by):
    return [
        (a * NLON_DEV + i, a * NLON_DEV + (i + by) % NLON_DEV)
        for a in (0, NLAT_DEV - 1)
        for i in range(NLON_DEV)
    ]


def near_kernel(idx_ref, w_ref, *refs):
    parts, (out_ref, src, sem) = refs[:-3], refs[-3:]
    step = pl.program_id(0)
    own, le, lm, re, rm, up, dn = parts

    def copies():
        todo = [(own, 0, ROWS, 0 * PAD + R)]
        for n, (e, m) in enumerate(((le, lm), (re, rm))):
            at = (n + 1) * PAD + R
            todo.append((e, 0, E, at))
            todo.append((m, 0, MID, at + E))
            todo.append((e, E, E, at + E + MID))
        for n in range(3):
            todo.append((up, n * R, R, n * PAD))
            todo.append((dn, n * R, R, n * PAD + R + ROWS))
        return [
            pltpu.make_async_copy(ref.at[pl.ds(a, n)], src.at[pl.ds(to, n)], sem.at[i])
            for i, (ref, a, n, to) in enumerate(todo)
        ]

    @pl.when(step == 0)
    def _():
        for copy in copies():
            copy.start()
        src[3 * PAD] = jnp.zeros((C, C), src.dtype)
        for copy in copies():
            copy.wait()

    for j in range(TB):
        t = step * TB + j
        lhs = jnp.concatenate([src[idx_ref[k, t]] for k in range(KMAX)], axis=1)
        rhs = jnp.concatenate([w_ref[j, k] for k in range(KMAX)], axis=1)
        out_ref[j] = lax.dot_general(lhs, rhs, NT, preferred_element_type=jnp.float32)


def near_call(idx, weights, parts):
    n_copies = 7 + 6
    return pl.pallas_call(
        near_kernel,
        grid_spec=pltpu.PrefetchScalarGridSpec(
            num_scalar_prefetch=1,
            grid=(ROWS // TB,),
            in_specs=[pl.BlockSpec((TB, KMAX, C, C), lambda s, i: (s, 0, 0, 0))]
            + [pl.BlockSpec(memory_space=pltpu.HBM)] * len(parts),
            out_specs=pl.BlockSpec((TB, C, C), lambda s, i: (s, 0, 0)),
            scratch_shapes=[
                pltpu.VMEM((3 * PAD + 1, C, C), jnp.bfloat16),
                pltpu.SemaphoreType.DMA((n_copies,)),
            ],
        ),
        out_shape=jax.ShapeDtypeStruct((ROWS, C, C), jnp.float32),
        compiler_params=pltpu.CompilerParams(
            dimension_semantics=("arbitrary",), vmem_limit_bytes=20 << 20
        ),
        cost_estimate=pl.CostEstimate(
            flops=2 * ROWS * KMAX * C**3, bytes_accessed=28 << 20, transcendentals=0
        ),
        name="near",
    )(idx, weights, *parts)


GROUP = 8


def far_kernel(lst_ref, num_ref, area_ref, w_hbm, le, lm, re, rm, up, dn, l3, r3, part_ref, out_ref, mass_ref, src, wbuf, sem, wsem):
    todo = []
    for n, (e, m) in enumerate(((le, lm), (re, rm))):
        at = n * PAD + R
        todo.append((e, 0, E, at))
        todo.append((m, 0, MID, at + E))
        todo.append((e, E, E, at + E + MID))
        todo.append((up, n * R, R, n * PAD))
        todo.append((dn, n * R, R, n * PAD + R + ROWS))
    todo.append((l3, 0, E, FAR))
    todo.append((r3, 0, E, FAR + E))
    copies = [
        pltpu.make_async_copy(ref.at[pl.ds(a, n)], src.at[pl.ds(to, n)], sem.at[i])
        for i, (ref, a, n, to) in enumerate(todo)
    ]
    for copy in copies:
        copy.start()
    groups = num_ref[0]

    def entry(g, j):
        v = lst_ref[g * GROUP + j]
        slot = lax.shift_right_logical(v, 9)
        return lax.shift_right_logical(slot, 3), slot & (KMAX - 1), v & 511

    def weight_copy(g, j):
        t, k, _ = entry(g, j)
        return pltpu.make_async_copy(w_hbm.at[t, k], wbuf.at[g * GROUP + j], wsem.at[g])

    def issue(g, carry):
        for j in range(GROUP):
            weight_copy(g, j).start()
        return carry

    lax.fori_loop(0, groups, issue, 0)
    out_ref[...] = part_ref[...]
    src[FAR + 2 * E] = jnp.zeros((C, C), src.dtype)
    for copy in copies:
        copy.wait()

    def work(g, carry):
        for j in range(GROUP):
            weight_copy(g, j).wait()
        got = []
        for j in range(GROUP):
            t, _, s = entry(g, j)
            got.append(
                (t, lax.dot_general(src[s], wbuf[g * GROUP + j], NT, preferred_element_type=jnp.float32))
            )
        for t, d in got:
            out_ref[t] = out_ref[t] + d
        return carry

    lax.fori_loop(0, groups, work, 0)

    def add_up(t, acc):
        return acc + area_ref[t] * out_ref[t]

    acc = lax.fori_loop(0, ROWS, add_up, jnp.zeros((C, C), jnp.float32), unroll=4)
    mass_ref[...] = lax.dot_general(
        jnp.ones((8, C), jnp.float32), acc, NT,
        precision=lax.Precision.HIGHEST, preferred_element_type=jnp.float32,
    )


def far_call(lst, num, area, weights, parts, partial):
    smem = pl.BlockSpec(memory_space=pltpu.SMEM)
    hbm = pl.BlockSpec(memory_space=pltpu.HBM)
    vmem = pl.BlockSpec(memory_space=pltpu.VMEM)
    return pl.pallas_call(
        far_kernel,
        in_specs=[smem, smem, smem, hbm] + [hbm] * len(parts) + [vmem],
        out_specs=[vmem, vmem],
        out_shape=[
            jax.ShapeDtypeStruct((ROWS, C, C), jnp.float32),
            jax.ShapeDtypeStruct((8, C), jnp.float32),
        ],
        scratch_shapes=[
            pltpu.VMEM((FAR + 2 * E + 1, C, C), jnp.bfloat16),
            pltpu.VMEM((ROWS * KMAX, C, C), jnp.bfloat16),
            pltpu.SemaphoreType.DMA((12,)),
            pltpu.SemaphoreType.DMA((ROWS * KMAX // GROUP,)),
        ],
        compiler_params=pltpu.CompilerParams(vmem_limit_bytes=40 << 20),
        cost_estimate=pl.CostEstimate(
            flops=2 * ROWS * KMAX * C**3 // 2, bytes_accessed=20 << 20, transcendentals=0
        ),
        name="far",
    )(lst, num, area, weights, *parts, partial)


def latitude_area(first_row, count_rows):
    rows_all = jnp.arange(count_rows, dtype=jnp.int32) + first_row
    angle = -0.5 * math.pi + (rows_all.astype(jnp.float32) + 0.5) * (math.pi / NLAT)
    return jnp.cos(angle)


def slots(source_row, source_block, slot_count, lat, lon):
    row = source_row[:, 0, :].T - (lat * ROWS - R)
    row = jnp.clip(row, 0, PAD - 1)
    rel = (source_block[:, 0, :].T - lon + 3) % NLON_DEV - 3
    active = jnp.arange(KMAX, dtype=jnp.int32)[:, None] < slot_count[:, 0][None, :]
    size = jnp.abs(rel)
    side = (rel > 0).astype(jnp.int32)
    is_near = active & (size <= 1)
    near = jnp.where(is_near, jnp.where(rel == 0, 0, side + 1) * PAD + row, 3 * PAD)
    polar_row = jnp.clip(jnp.where(lat == 0, row - R, row - R - (ROWS - E)), 0, E - 1)
    far = jnp.where(size >= 3, FAR + side * E + polar_row, side * PAD + row)
    is_far = active & (size >= 2)
    target = jnp.arange(ROWS, dtype=jnp.int32)[None, :]
    slot = target * KMAX + jnp.arange(KMAX, dtype=jnp.int32)[:, None]
    order = jnp.where(is_far, slot, ROWS * KMAX + slot)
    zero = FAR + 2 * E
    packed = (order * 512 + jnp.where(is_far, far, zero)).reshape(-1)
    packed = jnp.sort(packed) & (ROWS * KMAX * 512 - 1)
    groups = (jnp.sum(is_far.astype(jnp.int32)) + GROUP - 1) // GROUP
    return near.astype(jnp.int32), packed.astype(jnp.int32), groups.reshape(1)


def everywhere(tracers, weights, source_row, source_block, slot_count):
    lat, lon = lax.axis_index("lat"), lax.axis_index("lon")
    q = tracers.transpose(0, 2, 3, 1).reshape(ROWS, C, C)
    qe = jnp.concatenate([q[:E], q[ROWS - E :]], axis=0)
    qm = q[E : ROWS - E]
    le, re = (lax.ppermute(qe, "lon", ring(1)), lax.ppermute(qe, "lon", ring(-1)))
    lm, rm = (lax.ppermute(qm, "lon", ring(1)), lax.ppermute(qm, "lon", ring(-1)))
    near_idx, far_list, far_groups = slots(source_row, source_block, slot_count, lat, lon)
    area = latitude_area(lat * ROWS, ROWS)
    total_area = C * NLON_DEV * jnp.sum(latitude_area(0, NLAT))
    mass_old = jnp.sum(area[:, None, None] * q.astype(jnp.float32), axis=(0, 2))

    up1 = lax.ppermute(jnp.concatenate([v[2 * E - R :] for v in (qe, le, re)], axis=0), "lat", UP)
    dn1 = lax.ppermute(jnp.concatenate([v[:R] for v in (qe, le, re)], axis=0), "lat", DOWN)
    lle, rre = (lax.ppermute(le, "lon", ring(1)), lax.ppermute(re, "lon", ring(-1)))
    llm, rrm = (lax.ppermute(lm, "lon", ring(1)), lax.ppermute(rm, "lon", ring(-1)))
    up2 = lax.ppermute(jnp.concatenate([v[2 * E - R :] for v in (lle, rre)], axis=0), "lat", UP)
    dn2 = lax.ppermute(jnp.concatenate([v[:R] for v in (lle, rre)], axis=0), "lat", DOWN)
    pole = [jnp.where(lat == 0, v[:E], v[E:]) for v in (lle, rre)]
    l3 = lax.ppermute(pole[0], ("lat", "lon"), polar(1))
    r3 = lax.ppermute(pole[1], ("lat", "lon"), polar(-1))

    w = weights[:, 0]
    partial = near_call(near_idx, w, (q, le, lm, re, rm, up1, dn1))
    advected, mass_new = far_call(
        far_list, far_groups, area, w, (lle, llm, rre, rrm, up2, dn2, l3, r3), partial
    )
    change = lax.psum(mass_old - mass_new[0], ("lat", "lon"))
    fixed = advected + (change / total_area)[None, :, None]
    return fixed


TOTAL_AREA = C * NLON_DEV * math.fsum(
    math.cos(-0.5 * math.pi + (j + 0.5) * math.pi / NLAT) for j in range(NLAT)
)
EDGE = 16
S = 2 * EDGE
M = ROWS - S
B = 16
SIDE = S + M + B + R
FAR2 = 2 * SIDE
SECT = 7 * PAD
CHUNKS = 4
PER = ROWS // CHUNKS
POLAR, NEXT = ((0, NLAT_DEV - 1), (1, NLAT_DEV - 2))


def some(by, lats):
    return [
        (a * NLON_DEV + i, a * NLON_DEV + (i + by) % NLON_DEV) for a in lats for i in range(NLON_DEV)
    ]


WC = 16
WT = ROWS // WC


def sums_kernel(idx_ref, area_ref, w_hbm, *refs):
    left, right, own, s3m, s3p, wv, acc, sem = refs

    def copy(c):
        rows = pl.ds(c * WT, WT)
        return pltpu.make_async_copy(w_hbm.at[rows], wv.at[rows], sem.at[c])

    def start(c, carry):
        copy(c).start()
        return carry

    lax.fori_loop(0, WC, start, 0)
    acc[...] = jnp.zeros(acc.shape, acc.dtype)

    def work(c, carry):
        copy(c).wait()
        for j in range(WT):
            t = c * WT + j
            for k in range(KMAX):
                part = jnp.sum(wv[t, k].astype(jnp.float32).reshape(C // 8, 8, C), axis=0)
                at = idx_ref[k, t]
                acc[at] = acc[at] + area_ref[t] * part
        return carry

    lax.fori_loop(0, WC, work, 0)

    def summed(rel):
        at = (rel + 3) * PAD
        return jnp.sum(acc[at : at + PAD], axis=1)

    left[:PAD] = summed(-1)
    left[PAD:] = summed(-2)
    right[:PAD] = summed(1)
    right[PAD:] = summed(2)
    own[...] = summed(0)
    s3m[...] = summed(-3)
    s3p[...] = summed(3)


def sums_call(idx, area, weights):
    smem = pl.BlockSpec(memory_space=pltpu.SMEM)
    vmem = pl.BlockSpec(memory_space=pltpu.VMEM)
    return pl.pallas_call(
        sums_kernel,
        in_specs=[smem, smem, pl.BlockSpec(memory_space=pltpu.HBM)],
        out_specs=[vmem] * 5,
        out_shape=[jax.ShapeDtypeStruct((n * PAD, C), jnp.float32) for n in (2, 2, 1, 1, 1)],
        scratch_shapes=[
            pltpu.VMEM(weights.shape, weights.dtype),
            pltpu.VMEM((SECT + 1, 8, C), jnp.float32),
            pltpu.SemaphoreType.DMA((WC,)),
        ],
        compiler_params=pltpu.CompilerParams(vmem_limit_bytes=22 << 20),
        cost_estimate=pl.CostEstimate(
            flops=20_000_000, bytes_accessed=17 << 20, transcendentals=0
        ),
        name="sums",
    )(idx, area, pltpu.with_memory_space_constraint(weights, pltpu.HBM))


def mass_kernel(area_ref, lost_ref, at_ref, c0, cl, cr, s3m, s3p, own, ls, lm, rs, rm, up, dn, l3, r3, out_ref, src, by):
    src[pl.ds(R, ROWS)] = own[...]
    for n, (e, m) in enumerate(((ls, lm), (rs, rm))):
        at = (n + 1) * PAD + R
        src[pl.ds(at, EDGE)] = e[:EDGE]
        src[pl.ds(at + EDGE, M)] = m[...]
        src[pl.ds(at + EDGE + M, EDGE)] = e[EDGE:]
    for n in range(3):
        src[pl.ds(n * PAD, R)] = up[pl.ds(n * R, R)]
        src[pl.ds(n * PAD + R + ROWS, R)] = dn[pl.ds(n * R, R)]
    src[3 * PAD] = jnp.zeros((C, C), src.dtype)
    by[:PAD] = (c0[...] + cl[:PAD]) + cr[:PAD]
    by[PAD : 2 * PAD] = cl[PAD:]
    by[2 * PAD :] = cr[PAD:]
    for r in range(ROWS):
        by[R + r : R + r + 1] = by[R + r : R + r + 1] - area_ref[r]

    def body(p, acc):
        return acc + by[pl.ds(p, 1)] * src[p].astype(jnp.float32)

    acc = lax.fori_loop(0, 3 * PAD, body, jnp.zeros((C, C), jnp.float32), unroll=4)
    at = at_ref[0]
    for i in range(E):
        acc = acc + s3m[pl.ds(at + i, 1)] * l3[i].astype(jnp.float32)
        acc = acc + s3p[pl.ds(at + i, 1)] * r3[i].astype(jnp.float32)
    change = lax.dot_general(
        jnp.full((8, C), -1.0, jnp.float32), acc, NT,
        precision=lax.Precision.HIGHEST, preferred_element_type=jnp.float32,
    )
    row = lax.broadcasted_iota(jnp.int32, (8, C), 0)
    out_ref[...] = jnp.where(row == 0, change, lost_ref[0])


def mass_call(area, lost, at, parts):
    smem = pl.BlockSpec(memory_space=pltpu.SMEM)
    vmem = pl.BlockSpec(memory_space=pltpu.VMEM)
    return pl.pallas_call(
        mass_kernel,
        in_specs=[smem] * 3 + [vmem] * len(parts),
        out_specs=[vmem, vmem],
        out_shape=[
            jax.ShapeDtypeStruct((8, C), jnp.float32),
            pltpu.VMEM((3 * PAD + 1, C, C), jnp.bfloat16),
        ],
        scratch_shapes=[pltpu.VMEM((3 * PAD, C), jnp.float32)],
        compiler_params=pltpu.CompilerParams(vmem_limit_bytes=6 << 20),
        cost_estimate=pl.CostEstimate(
            flops=9_000_000, bytes_accessed=3 << 20, transcendentals=0
        ),
        name="mass",
    )(area, lost, at, *parts)


PARTS = 4
PT = PER // PARTS


def inner_kernel(first, idx_ref, w_hbm, src, out_ref, wv, sem):
    def copy(c):
        return pltpu.make_async_copy(
            w_hbm.at[pl.ds(first + c * PT, PT)], wv.at[pl.ds(c * PT, PT)], sem.at[c]
        )

    for c in range(PARTS):
        copy(c).start()

    def body(c, carry):
        copy(c).wait()
        for i in range(PT):
            j = c * PT + i
            lhs = jnp.concatenate([src[idx_ref[k, first + j]] for k in range(KMAX)], axis=1)
            rhs = jnp.concatenate([wv[j, k] for k in range(KMAX)], axis=1)
            out_ref[j] = lax.dot_general(lhs, rhs, NT, preferred_element_type=jnp.float32)
        return carry

    lax.fori_loop(0, PARTS, body, 0)


def inner_call(chunk, idx, weights, near):
    vmem = pl.BlockSpec(memory_space=pltpu.VMEM)
    return pl.pallas_call(
        functools.partial(inner_kernel, chunk * PER),
        in_specs=[
            pl.BlockSpec(memory_space=pltpu.SMEM), pl.BlockSpec(memory_space=pltpu.HBM), vmem
        ],
        out_specs=[vmem, vmem],
        out_shape=[
            pltpu.VMEM((PER, C, C), jnp.float32),
            pltpu.VMEM((PER, KMAX, C, C), jnp.bfloat16),
        ],
        scratch_shapes=[pltpu.SemaphoreType.DMA((PARTS,))],
        compiler_params=pltpu.CompilerParams(vmem_limit_bytes=2 << 20),
        cost_estimate=pl.CostEstimate(
            flops=2 * PER * KMAX * C**3, bytes_accessed=5 << 20, transcendentals=0
        ),
    )(idx, pltpu.with_memory_space_constraint(weights, pltpu.HBM), near)


def outer_kernel(idx_ref, corr_ref, ls, lm, lb, lh, rs, rm, rb, rh, l3, r3, *refs):
    partial, wv, (out_hbm, src, acc, sem) = refs[:CHUNKS], refs[CHUNKS : 2 * CHUNKS], refs[2 * CHUNKS :]
    for n, (e, m, b, h) in enumerate(((ls, lm, lb, lh), (rs, rm, rb, rh))):
        at = n * SIDE
        src[pl.ds(at, S)] = e[...]
        src[pl.ds(at + S, M)] = m[...]
        src[pl.ds(at + S + M, B)] = b[...]
        src[pl.ds(at + S + M + B, R)] = h[...]
    src[pl.ds(FAR2, E)] = l3[...]
    src[pl.ds(FAR2 + E, E)] = r3[...]
    src[FAR2 + 2 * E] = jnp.zeros((C, C), src.dtype)

    def out_copy(c):
        rows = pl.ds(c * PER, PER)
        return pltpu.make_async_copy(acc.at[rows], out_hbm.at[rows], sem.at[c])

    for c in range(CHUNKS):

        def body(t, carry):
            lhs = jnp.concatenate([src[idx_ref[k, t]] for k in range(KMAX)], axis=1)
            rhs = jnp.concatenate([wv[c][t - c * PER, k] for k in range(KMAX)], axis=1)
            got = lax.dot_general(lhs, rhs, NT, preferred_element_type=jnp.float32)
            acc[t] = (got + partial[c][t - c * PER]) + corr_ref[...]
            return carry

        lax.fori_loop(c * PER, (c + 1) * PER, body, 0, unroll=4)
        out_copy(c).start()
    for c in range(CHUNKS):
        out_copy(c).wait()


def outer_call(idx, corr, parts, partial, weights):
    vmem = pl.BlockSpec(memory_space=pltpu.VMEM)
    return pl.pallas_call(
        outer_kernel,
        in_specs=[pl.BlockSpec(memory_space=pltpu.SMEM)] + [vmem] * (1 + 2 * CHUNKS + len(parts)),
        out_specs=pl.BlockSpec(memory_space=pltpu.HBM),
        out_shape=jax.ShapeDtypeStruct((ROWS, C, C), jnp.float32),
        scratch_shapes=[
            pltpu.VMEM((FAR2 + 2 * E + 1, C, C), jnp.bfloat16),
            pltpu.VMEM((ROWS, C, C), jnp.float32),
            pltpu.SemaphoreType.DMA((CHUNKS,)),
        ],
        compiler_params=pltpu.CompilerParams(vmem_limit_bytes=18 << 20),
        cost_estimate=pl.CostEstimate(
            flops=2 * ROWS * KMAX * C**3, bytes_accessed=4 << 20, transcendentals=0
        ),
        name="outer",
    )(idx, corr, *parts, *partial, *weights)


def tables(source_row, source_block, slot_count, lat, lon):
    p = source_row[:, 0, :].T - (lat * ROWS - R)
    p = jnp.clip(p, 0, PAD - 1)
    rel = (source_block[:, 0, :].T - lon + 3) % NLON_DEV - 3
    rel = jnp.clip(rel, -3, 3)
    active = jnp.arange(KMAX, dtype=jnp.int32)[:, None] < slot_count[:, 0][None, :]
    sums_idx = jnp.where(active, (rel + 3) * PAD + p, SECT)
    size = jnp.abs(rel)
    side = (rel > 0).astype(jnp.int32)
    near_idx = jnp.where(
        active & (size <= 1), jnp.where(rel == 0, 0, side + 1) * PAD + p, 3 * PAD
    )
    r = p - R
    is_polar = (lat == 0) | (lat == NLAT_DEV - 1)
    in_band = jnp.where(r < EDGE, r, jnp.where(r < EDGE + M, r - EDGE + S, r - M))
    below = lat == NLAT_DEV - 2
    in_next = S + M + jnp.where(below, r - (ROWS - B), r)
    halo = S + M + B + jnp.where(r < 0, r + R, r - ROWS)
    two = jnp.where((r < 0) | (r >= ROWS), halo, jnp.where(is_polar, in_band, in_next))
    polar_row = jnp.clip(jnp.where(lat == 0, r, r - (ROWS - E)), 0, E - 1)
    far = jnp.where(size >= 3, FAR2 + side * E + polar_row, side * SIDE + two)
    is_far = active & (size >= 2)
    held = is_polar | ((lat == 1) & (r < B)) | (below & (r >= ROWS - B))
    lost = jnp.sum((is_far & ~held).astype(jnp.float32))
    far_idx = jnp.where(is_far & held, far, FAR2 + 2 * E)
    return sums_idx, near_idx, far_idx, lost


def swap(v, axis, size, to):
    return lax.ppermute(v, axis, [(i, to(i)) for i in range(size)])


def local(tracers, weights, source_row, source_block, slot_count):
    args = (tracers, weights, source_row, source_block, slot_count)
    lost, fixed = usual(*args)

    def redo(state):
        return jnp.zeros_like(state[0]), everywhere(*args)

    _, fixed = lax.while_loop(lambda state: state[0] > 0, redo, (lost, fixed))
    return fixed.reshape(ROWS, 32, 4, C).transpose(0, 3, 1, 2)


def usual(tracers, weights, source_row, source_block, slot_count):
    lat, lon = lax.axis_index("lat"), lax.axis_index("lon")
    both = ("lat", "lon")
    w = weights[:, 0]
    q = tracers.transpose(0, 2, 3, 1).reshape(ROWS, C, C)
    qs = jnp.concatenate([q[:EDGE], q[ROWS - EDGE :]], axis=0)
    ls, rs = lax.ppermute(qs, "lon", ring(1)), lax.ppermute(qs, "lon", ring(-1))
    qm = q[EDGE : ROWS - EDGE]
    lm, rm = lax.ppermute(qm, "lon", ring(1)), lax.ppermute(qm, "lon", ring(-1))
    pole = jnp.where(lat == 0, qs[:E], qs[S - E :])
    l3 = lax.ppermute(pole, both, some(3, POLAR))
    r3 = lax.ppermute(pole, both, some(-3, POLAR))
    sums_idx, near_idx, far_idx, lost = tables(source_row, source_block, slot_count, lat, lon)
    area = latitude_area(lat * ROWS, ROWS)
    to_left, to_right, own_sums, s3m, s3p = sums_call(sums_idx, area, w)
    cl = lax.ppermute(to_left, "lon", ring(-1))
    cr = lax.ppermute(to_right, "lon", ring(1))
    up1 = lax.ppermute(jnp.concatenate([v[S - R :] for v in (qs, ls, rs)], axis=0), "lat", UP)
    dn1 = lax.ppermute(jnp.concatenate([v[:R] for v in (qs, ls, rs)], axis=0), "lat", DOWN)
    at = jnp.where(jnp.arange(NLAT_DEV, dtype=jnp.int32) == lat, R, R + ROWS - E).astype(jnp.int32)
    v, near = mass_call(
        area, lost.reshape(1), at,
        (own_sums, cl, cr, s3m, s3p, q, ls, lm, rs, rm, up1, dn1, l3, r3),
    )
    near = pltpu.with_memory_space_constraint(near, pltpu.VMEM)
    for axis, size, bit in (("lat", NLAT_DEV, 1), ("lat", NLAT_DEV, 2), ("lat", NLAT_DEV, 4), ("lon", NLON_DEV, 4), ("lon", NLON_DEV, 8)):
        v = v + swap(v, axis, size, lambda i, bit=bit: i ^ bit)
    y = [swap(v, "lon", NLON_DEV, lambda i, by=by: i // 4 * 4 + (i + by) % 4) for by in (1, 2, 3)]
    v = v + (y[0] + y[2]) + y[1]
    corr = jnp.broadcast_to((v[0] * (1.0 / TOTAL_AREA))[:, None], (C, C))

    lls, rrs = (lax.ppermute(x, both, some(d, POLAR)) for x, d in ((ls, 1), (rs, -1)))
    llm, rrm = (lax.ppermute(x, both, some(d, POLAR)) for x, d in ((lm, 1), (rm, -1)))

    def next_rows(e):
        return jnp.where(lat == 1, e[:B], e[S - B :])

    llb = lax.ppermute(next_rows(ls), both, some(1, NEXT))
    rrb = lax.ppermute(next_rows(rs), both, some(-1, NEXT))
    beyond = jnp.where((lat == 0) | (lat == NLAT_DEV - 2), dn1[R:], up1[R:])
    llh = lax.ppermute(beyond[:R], both, some(1, POLAR + NEXT))
    rrh = lax.ppermute(beyond[R:], both, some(-1, POLAR + NEXT))

    pieces = [inner_call(c, near_idx, w, near) for c in range(CHUNKS)]
    partial, wv = ([pltpu.with_memory_space_constraint(x, pltpu.VMEM) for x in p] for p in zip(*pieces))
    fixed = outer_call(
        far_idx, corr, (lls, llm, llb, llh, rrs, rrm, rrb, rrh, l3, r3), partial, wv
    )
    return v[1, 0], fixed


def solution(mesh):
    placed = (
        P("lat", "lon", None, None),
        P("lat", "lon", None, None, None),
        P("lat", "lon", None),
        P("lat", "lon", None),
        P("lat", "lon"),
    )
    return jax.shard_map(
        local, mesh=mesh, in_specs=placed, out_specs=P("lat", "lon", None, None), check_vma=False
    )
```

```python
import functools
import math

import jax
import jax.numpy as jnp
from jax import lax
from jax.experimental import pallas as pl
from jax.experimental.pallas import tpu as pltpu
from jax.sharding import PartitionSpec as P

ROWS = 64
C = 128
KMAX = 8
R = 4
E = R + 1
MID = ROWS - 2 * E
PAD = ROWS + 2 * R
NLAT, NLON_DEV, NLAT_DEV = 512, 16, 8
TB = 4
FAR = 2 * PAD
NT = (((1,), (1,)), ((), ()))


def ring(by):
    return [(i, (i + by) % NLON_DEV) for i in range(NLON_DEV)]


UP = [(i, i + 1) for i in range(NLAT_DEV - 1)]
DOWN = [(i + 1, i) for i in range(NLAT_DEV - 1)]


def polar(by):
    return [
        (a * NLON_DEV + i, a * NLON_DEV + (i + by) % NLON_DEV)
        for a in (0, NLAT_DEV - 1)
        for i in range(NLON_DEV)
    ]


def near_kernel(idx_ref, w_ref, *refs):
    parts, (out_ref, src, sem) = refs[:-3], refs[-3:]
    step = pl.program_id(0)
    own, le, lm, re, rm, up, dn = parts

    def copies():
        todo = [(own, 0, ROWS, 0 * PAD + R)]
        for n, (e, m) in enumerate(((le, lm), (re, rm))):
            at = (n + 1) * PAD + R
            todo.append((e, 0, E, at))
            todo.append((m, 0, MID, at + E))
            todo.append((e, E, E, at + E + MID))
        for n in range(3):
            todo.append((up, n * R, R, n * PAD))
            todo.append((dn, n * R, R, n * PAD + R + ROWS))
        return [
            pltpu.make_async_copy(ref.at[pl.ds(a, n)], src.at[pl.ds(to, n)], sem.at[i])
            for i, (ref, a, n, to) in enumerate(todo)
        ]

    @pl.when(step == 0)
    def _():
        for copy in copies():
            copy.start()
        src[3 * PAD] = jnp.zeros((C, C), src.dtype)
        for copy in copies():
            copy.wait()

    for j in range(TB):
        t = step * TB + j
        lhs = jnp.concatenate([src[idx_ref[k, t]] for k in range(KMAX)], axis=1)
        rhs = jnp.concatenate([w_ref[j, k] for k in range(KMAX)], axis=1)
        out_ref[j] = lax.dot_general(lhs, rhs, NT, preferred_element_type=jnp.float32)


def near_call(idx, weights, parts):
    n_copies = 7 + 6
    return pl.pallas_call(
        near_kernel,
        grid_spec=pltpu.PrefetchScalarGridSpec(
            num_scalar_prefetch=1,
            grid=(ROWS // TB,),
            in_specs=[pl.BlockSpec((TB, KMAX, C, C), lambda s, i: (s, 0, 0, 0))]
            + [pl.BlockSpec(memory_space=pltpu.HBM)] * len(parts),
            out_specs=pl.BlockSpec((TB, C, C), lambda s, i: (s, 0, 0)),
            scratch_shapes=[
                pltpu.VMEM((3 * PAD + 1, C, C), jnp.bfloat16),
                pltpu.SemaphoreType.DMA((n_copies,)),
            ],
        ),
        out_shape=jax.ShapeDtypeStruct((ROWS, C, C), jnp.float32),
        compiler_params=pltpu.CompilerParams(
            dimension_semantics=("arbitrary",), vmem_limit_bytes=20 << 20
        ),
        cost_estimate=pl.CostEstimate(
            flops=2 * ROWS * KMAX * C**3, bytes_accessed=28 << 20, transcendentals=0
        ),
        name="near",
    )(idx, weights, *parts)


GROUP = 8


def far_kernel(lst_ref, num_ref, area_ref, w_hbm, le, lm, re, rm, up, dn, l3, r3, part_ref, out_ref, mass_ref, src, wbuf, sem, wsem):
    todo = []
    for n, (e, m) in enumerate(((le, lm), (re, rm))):
        at = n * PAD + R
        todo.append((e, 0, E, at))
        todo.append((m, 0, MID, at + E))
        todo.append((e, E, E, at + E + MID))
        todo.append((up, n * R, R, n * PAD))
        todo.append((dn, n * R, R, n * PAD + R + ROWS))
    todo.append((l3, 0, E, FAR))
    todo.append((r3, 0, E, FAR + E))
    copies = [
        pltpu.make_async_copy(ref.at[pl.ds(a, n)], src.at[pl.ds(to, n)], sem.at[i])
        for i, (ref, a, n, to) in enumerate(todo)
    ]
    for copy in copies:
        copy.start()
    groups = num_ref[0]

    def entry(g, j):
        v = lst_ref[g * GROUP + j]
        slot = lax.shift_right_logical(v, 9)
        return lax.shift_right_logical(slot, 3), slot & (KMAX - 1), v & 511

    def weight_copy(g, j):
        t, k, _ = entry(g, j)
        return pltpu.make_async_copy(w_hbm.at[t, k], wbuf.at[g * GROUP + j], wsem.at[g])

    def issue(g, carry):
        for j in range(GROUP):
            weight_copy(g, j).start()
        return carry

    lax.fori_loop(0, groups, issue, 0)
    out_ref[...] = part_ref[...]
    src[FAR + 2 * E] = jnp.zeros((C, C), src.dtype)
    for copy in copies:
        copy.wait()

    def work(g, carry):
        for j in range(GROUP):
            weight_copy(g, j).wait()
        got = []
        for j in range(GROUP):
            t, _, s = entry(g, j)
            got.append(
                (t, lax.dot_general(src[s], wbuf[g * GROUP + j], NT, preferred_element_type=jnp.float32))
            )
        for t, d in got:
            out_ref[t] = out_ref[t] + d
        return carry

    lax.fori_loop(0, groups, work, 0)

    def add_up(t, acc):
        return acc + area_ref[t] * out_ref[t]

    acc = lax.fori_loop(0, ROWS, add_up, jnp.zeros((C, C), jnp.float32), unroll=4)
    mass_ref[...] = lax.dot_general(
        jnp.ones((8, C), jnp.float32), acc, NT,
        precision=lax.Precision.HIGHEST, preferred_element_type=jnp.float32,
    )


def far_call(lst, num, area, weights, parts, partial):
    smem = pl.BlockSpec(memory_space=pltpu.SMEM)
    hbm = pl.BlockSpec(memory_space=pltpu.HBM)
    vmem = pl.BlockSpec(memory_space=pltpu.VMEM)
    return pl.pallas_call(
        far_kernel,
        in_specs=[smem, smem, smem, hbm] + [hbm] * len(parts) + [vmem],
        out_specs=[vmem, vmem],
        out_shape=[
            jax.ShapeDtypeStruct((ROWS, C, C), jnp.float32),
            jax.ShapeDtypeStruct((8, C), jnp.float32),
        ],
        scratch_shapes=[
            pltpu.VMEM((FAR + 2 * E + 1, C, C), jnp.bfloat16),
            pltpu.VMEM((ROWS * KMAX, C, C), jnp.bfloat16),
            pltpu.SemaphoreType.DMA((12,)),
            pltpu.SemaphoreType.DMA((ROWS * KMAX // GROUP,)),
        ],
        compiler_params=pltpu.CompilerParams(vmem_limit_bytes=40 << 20),
        cost_estimate=pl.CostEstimate(
            flops=2 * ROWS * KMAX * C**3 // 2, bytes_accessed=20 << 20, transcendentals=0
        ),
        name="far",
    )(lst, num, area, weights, *parts, partial)


def latitude_area(first_row, count_rows):
    rows_all = jnp.arange(count_rows, dtype=jnp.int32) + first_row
    angle = -0.5 * math.pi + (rows_all.astype(jnp.float32) + 0.5) * (math.pi / NLAT)
    return jnp.cos(angle)


def slots(source_row, source_block, slot_count, lat, lon):
    row = source_row[:, 0, :].T - (lat * ROWS - R)
    row = jnp.clip(row, 0, PAD - 1)
    rel = (source_block[:, 0, :].T - lon + 3) % NLON_DEV - 3
    active = jnp.arange(KMAX, dtype=jnp.int32)[:, None] < slot_count[:, 0][None, :]
    size = jnp.abs(rel)
    side = (rel > 0).astype(jnp.int32)
    is_near = active & (size <= 1)
    near = jnp.where(is_near, jnp.where(rel == 0, 0, side + 1) * PAD + row, 3 * PAD)
    polar_row = jnp.clip(jnp.where(lat == 0, row - R, row - R - (ROWS - E)), 0, E - 1)
    far = jnp.where(size >= 3, FAR + side * E + polar_row, side * PAD + row)
    is_far = active & (size >= 2)
    target = jnp.arange(ROWS, dtype=jnp.int32)[None, :]
    slot = target * KMAX + jnp.arange(KMAX, dtype=jnp.int32)[:, None]
    order = jnp.where(is_far, slot, ROWS * KMAX + slot)
    zero = FAR + 2 * E
    packed = (order * 512 + jnp.where(is_far, far, zero)).reshape(-1)
    packed = jnp.sort(packed) & (ROWS * KMAX * 512 - 1)
    groups = (jnp.sum(is_far.astype(jnp.int32)) + GROUP - 1) // GROUP
    return near.astype(jnp.int32), packed.astype(jnp.int32), groups.reshape(1)


def everywhere(tracers, weights, source_row, source_block, slot_count):
    lat, lon = lax.axis_index("lat"), lax.axis_index("lon")
    q = tracers.transpose(0, 2, 3, 1).reshape(ROWS, C, C)
    qe = jnp.concatenate([q[:E], q[ROWS - E :]], axis=0)
    qm = q[E : ROWS - E]
    le, re = (lax.ppermute(qe, "lon", ring(1)), lax.ppermute(qe, "lon", ring(-1)))
    lm, rm = (lax.ppermute(qm, "lon", ring(1)), lax.ppermute(qm, "lon", ring(-1)))
    near_idx, far_list, far_groups = slots(source_row, source_block, slot_count, lat, lon)
    area = latitude_area(lat * ROWS, ROWS)
    total_area = C * NLON_DEV * jnp.sum(latitude_area(0, NLAT))
    mass_old = jnp.sum(area[:, None, None] * q.astype(jnp.float32), axis=(0, 2))

    up1 = lax.ppermute(jnp.concatenate([v[2 * E - R :] for v in (qe, le, re)], axis=0), "lat", UP)
    dn1 = lax.ppermute(jnp.concatenate([v[:R] for v in (qe, le, re)], axis=0), "lat", DOWN)
    lle, rre = (lax.ppermute(le, "lon", ring(1)), lax.ppermute(re, "lon", ring(-1)))
    llm, rrm = (lax.ppermute(lm, "lon", ring(1)), lax.ppermute(rm, "lon", ring(-1)))
    up2 = lax.ppermute(jnp.concatenate([v[2 * E - R :] for v in (lle, rre)], axis=0), "lat", UP)
    dn2 = lax.ppermute(jnp.concatenate([v[:R] for v in (lle, rre)], axis=0), "lat", DOWN)
    pole = [jnp.where(lat == 0, v[:E], v[E:]) for v in (lle, rre)]
    l3 = lax.ppermute(pole[0], ("lat", "lon"), polar(1))
    r3 = lax.ppermute(pole[1], ("lat", "lon"), polar(-1))

    w = weights[:, 0]
    partial = near_call(near_idx, w, (q, le, lm, re, rm, up1, dn1))
    advected, mass_new = far_call(
        far_list, far_groups, area, w, (lle, llm, rre, rrm, up2, dn2, l3, r3), partial
    )
    change = lax.psum(mass_old - mass_new[0], ("lat", "lon"))
    fixed = advected + (change / total_area)[None, :, None]
    return fixed


TOTAL_AREA = C * NLON_DEV * math.fsum(
    math.cos(-0.5 * math.pi + (j + 0.5) * math.pi / NLAT) for j in range(NLAT)
)
EDGE = 16
S = 2 * EDGE
M = ROWS - S
B = 16
SIDE = S + R + M + B + R
FAR2 = 2 * SIDE
SECT = 7 * PAD
CHUNKS = 4
PER = ROWS // CHUNKS
POLAR, NEXT = ((0, NLAT_DEV - 1), (1, NLAT_DEV - 2))


def some(by, lats):
    return [
        (a * NLON_DEV + i, a * NLON_DEV + (i + by) % NLON_DEV) for a in lats for i in range(NLON_DEV)
    ]


WC = 16
WT = ROWS // WC


def sums_kernel(idx_ref, area_ref, w_hbm, *refs):
    left, right, own, wv, acc, sem = refs

    def copy(c):
        rows = pl.ds(c * WT, WT)
        return pltpu.make_async_copy(w_hbm.at[rows], wv.at[rows], sem.at[c])

    def start(c, carry):
        copy(c).start()
        return carry

    lax.fori_loop(0, WC, start, 0)
    acc[...] = jnp.zeros(acc.shape, acc.dtype)

    def work(c, carry):
        copy(c).wait()
        for j in range(WT):
            t = c * WT + j
            for k in range(KMAX):
                part = jnp.sum(wv[t, k].astype(jnp.float32).reshape(C // 8, 8, C), axis=0)
                at = idx_ref[k, t]
                acc[at] = acc[at] + area_ref[t] * part
        return carry

    lax.fori_loop(0, WC, work, 0)

    def summed(rel):
        at = (rel + 3) * PAD
        return jnp.sum(acc[at : at + PAD], axis=1)

    left[:PAD] = summed(-1)
    left[PAD:] = summed(-2)
    right[:PAD] = summed(1)
    right[PAD:] = summed(2)
    own[:PAD] = summed(0)
    own[PAD : 2 * PAD] = summed(-3)
    own[2 * PAD :] = summed(3)


def sums_call(idx, area, weights):
    smem = pl.BlockSpec(memory_space=pltpu.SMEM)
    vmem = pl.BlockSpec(memory_space=pltpu.VMEM)
    return pl.pallas_call(
        sums_kernel,
        in_specs=[smem, smem, pl.BlockSpec(memory_space=pltpu.HBM)],
        out_specs=[vmem] * 3,
        out_shape=[jax.ShapeDtypeStruct((n * PAD, C), jnp.float32) for n in (2, 2, 3)],
        scratch_shapes=[
            pltpu.VMEM(weights.shape, weights.dtype),
            pltpu.VMEM((SECT + 1, 8, C), jnp.float32),
            pltpu.SemaphoreType.DMA((WC,)),
        ],
        compiler_params=pltpu.CompilerParams(vmem_limit_bytes=22 << 20),
        cost_estimate=pl.CostEstimate(
            flops=20_000_000, bytes_accessed=17 << 20, transcendentals=0
        ),
        name="sums",
    )(idx, area, pltpu.with_memory_space_constraint(weights, pltpu.HBM))


def mass_kernel(area_ref, lost_ref, at_ref, c0, cl, cr, own, ls, lm, rs, rm, up, dn, l3, r3, out_ref, src, by):
    src[pl.ds(R, ROWS)] = own[...]
    for n, (e, m) in enumerate(((ls, lm), (rs, rm))):
        at = (n + 1) * PAD + R
        src[pl.ds(at, EDGE)] = e[:EDGE]
        src[pl.ds(at + EDGE, M)] = m[...]
        src[pl.ds(at + EDGE + M, EDGE)] = e[EDGE:]
    for n in range(3):
        src[pl.ds(n * PAD, R)] = up[pl.ds(n * R, R)]
        src[pl.ds(n * PAD + R + ROWS, R)] = dn[pl.ds(n * R, R)]
    src[3 * PAD] = jnp.zeros((C, C), src.dtype)
    by[:PAD] = (c0[:PAD] + cl[:PAD]) + cr[:PAD]
    by[PAD : 2 * PAD] = cl[PAD:]
    by[2 * PAD :] = cr[PAD:]
    for r in range(ROWS):
        by[R + r : R + r + 1] = by[R + r : R + r + 1] - area_ref[r]

    def body(p, acc):
        return acc + by[pl.ds(p, 1)] * src[p].astype(jnp.float32)

    acc = lax.fori_loop(0, 3 * PAD, body, jnp.zeros((C, C), jnp.float32), unroll=4)
    at = at_ref[0]
    for i in range(E):
        acc = acc + c0[pl.ds(PAD + at + i, 1)] * l3[i].astype(jnp.float32)
        acc = acc + c0[pl.ds(2 * PAD + at + i, 1)] * r3[i].astype(jnp.float32)
    change = lax.dot_general(
        jnp.full((8, C), -1.0, jnp.float32), acc, NT,
        precision=lax.Precision.HIGHEST, preferred_element_type=jnp.float32,
    )
    row = lax.broadcasted_iota(jnp.int32, (8, C), 0)
    out_ref[...] = jnp.where(row == 0, change, lost_ref[0])


def mass_call(area, lost, at, parts):
    smem = pl.BlockSpec(memory_space=pltpu.SMEM)
    vmem = pl.BlockSpec(memory_space=pltpu.VMEM)
    return pl.pallas_call(
        mass_kernel,
        in_specs=[smem] * 3 + [vmem] * len(parts),
        out_specs=[vmem, vmem],
        out_shape=[
            jax.ShapeDtypeStruct((8, C), jnp.float32),
            pltpu.VMEM((3 * PAD + 1, C, C), jnp.bfloat16),
        ],
        scratch_shapes=[pltpu.VMEM((3 * PAD, C), jnp.float32)],
        compiler_params=pltpu.CompilerParams(vmem_limit_bytes=6 << 20),
        cost_estimate=pl.CostEstimate(
            flops=9_000_000, bytes_accessed=3 << 20, transcendentals=0
        ),
        name="mass",
    )(area, lost, at, *parts)


PARTS = 4
PT = PER // PARTS


def inner_kernel(first, idx_ref, w_hbm, src, out_ref, wv, sem):
    def copy(c):
        return pltpu.make_async_copy(
            w_hbm.at[pl.ds(first + c * PT, PT)], wv.at[pl.ds(c * PT, PT)], sem.at[c]
        )

    for c in range(PARTS):
        copy(c).start()

    def body(c, carry):
        copy(c).wait()
        for i in range(PT):
            j = c * PT + i
            lhs = jnp.concatenate([src[idx_ref[k, first + j]] for k in range(KMAX)], axis=1)
            rhs = jnp.concatenate([wv[j, k] for k in range(KMAX)], axis=1)
            out_ref[j] = lax.dot_general(lhs, rhs, NT, preferred_element_type=jnp.float32)
        return carry

    lax.fori_loop(0, PARTS, body, 0)


def inner_call(chunk, idx, weights, near):
    vmem = pl.BlockSpec(memory_space=pltpu.VMEM)
    return pl.pallas_call(
        functools.partial(inner_kernel, chunk * PER),
        in_specs=[
            pl.BlockSpec(memory_space=pltpu.SMEM), pl.BlockSpec(memory_space=pltpu.HBM), vmem
        ],
        out_specs=[vmem, vmem],
        out_shape=[
            pltpu.VMEM((PER, C, C), jnp.float32),
            pltpu.VMEM((PER, KMAX, C, C), jnp.bfloat16),
        ],
        scratch_shapes=[pltpu.SemaphoreType.DMA((PARTS,))],
        compiler_params=pltpu.CompilerParams(vmem_limit_bytes=2 << 20),
        cost_estimate=pl.CostEstimate(
            flops=2 * PER * KMAX * C**3, bytes_accessed=5 << 20, transcendentals=0
        ),
    )(idx, pltpu.with_memory_space_constraint(weights, pltpu.HBM), near)


HALF = CHUNKS // 2


def far_part(first, idx_ref, src, partial, wv, out_ref):
    for c in range(HALF):

        def body(j, carry):
            t = first + c * PER + j
            lhs = jnp.concatenate([src[idx_ref[k, t]] for k in range(KMAX)], axis=1)
            rhs = jnp.concatenate([wv[c][j, k] for k in range(KMAX)], axis=1)
            got = lax.dot_general(lhs, rhs, NT, preferred_element_type=jnp.float32)
            out_ref[c * PER + j] = got + partial[c][j]
            return carry

        lax.fori_loop(0, PER, body, 0, unroll=4)


def outer0_kernel(idx_ref, ls, lm, lb, rs, rm, rb, l3, r3, *refs):
    partial, wv, (out_ref, src) = refs[:HALF], refs[HALF:CHUNKS], refs[CHUNKS:]
    for n, (e, m, b) in enumerate(((ls, lm, lb), (rs, rm, rb))):
        at = n * SIDE
        src[pl.ds(at, S + R)] = e[...]
        src[pl.ds(at + S + R, M)] = m[...]
        src[pl.ds(at + S + R + M, B + R)] = b[...]
    src[pl.ds(FAR2, E)] = l3[...]
    src[pl.ds(FAR2 + E, E)] = r3[...]
    src[FAR2 + 2 * E] = jnp.zeros((C, C), src.dtype)
    far_part(0, idx_ref, src, partial, wv, out_ref)


def outer1_kernel(idx_ref, src, *refs):
    partial, wv, out_ref = refs[:HALF], refs[HALF:CHUNKS], refs[CHUNKS]
    far_part(HALF * PER, idx_ref, src, partial, wv, out_ref)


def outer_call(half, idx, parts, partial, weights):
    vmem = pl.BlockSpec(memory_space=pltpu.VMEM)
    out_shape = [pltpu.VMEM((HALF * PER, C, C), jnp.float32)]
    if half == 0:
        out_shape.append(pltpu.VMEM((FAR2 + 2 * E + 1, C, C), jnp.bfloat16))
    return pl.pallas_call(
        (outer0_kernel, outer1_kernel)[half],
        in_specs=[pl.BlockSpec(memory_space=pltpu.SMEM)]
        + [vmem] * (len(parts) + len(partial) + len(weights)),
        out_specs=[vmem] * len(out_shape),
        out_shape=out_shape,
        compiler_params=pltpu.CompilerParams(vmem_limit_bytes=8 << 20),
        cost_estimate=pl.CostEstimate(
            flops=2 * HALF * PER * KMAX * C**3, bytes_accessed=1 << 20, transcendentals=0
        ),
    )(idx, *parts, *partial, *weights)


WRITES = 8


def write_kernel(corr_ref, a_ref, b_ref, out_hbm, buf, sem):
    rows = ROWS // WRITES

    def copy(c):
        at = pl.ds(c * rows, rows)
        return pltpu.make_async_copy(buf.at[at], out_hbm.at[at], sem.at[c])

    for c in range(WRITES):
        ref = a_ref if c < WRITES // 2 else b_ref
        for i in range(rows):
            t = c * rows + i
            buf[t] = ref[t % (ROWS // 2)] + corr_ref[...]
        copy(c).start()
    for c in range(WRITES):
        copy(c).wait()


def write_call(corr, first, second):
    vmem = pl.BlockSpec(memory_space=pltpu.VMEM)
    return pl.pallas_call(
        write_kernel,
        in_specs=[vmem] * 3,
        out_specs=pl.BlockSpec(memory_space=pltpu.HBM),
        out_shape=jax.ShapeDtypeStruct((ROWS, C, C), jnp.float32),
        scratch_shapes=[
            pltpu.VMEM((ROWS, C, C), jnp.float32),
            pltpu.SemaphoreType.DMA((WRITES,)),
        ],
        compiler_params=pltpu.CompilerParams(vmem_limit_bytes=6 << 20),
        cost_estimate=pl.CostEstimate(
            flops=1_000_000, bytes_accessed=4 << 20, transcendentals=0
        ),
        name="write",
    )(corr, first, second)


def tables(source_row, source_block, slot_count, lat, lon):
    p = source_row[:, 0, :].T - (lat * ROWS - R)
    p = jnp.clip(p, 0, PAD - 1)
    rel = (source_block[:, 0, :].T - lon + 3) % NLON_DEV - 3
    rel = jnp.clip(rel, -3, 3)
    active = jnp.arange(KMAX, dtype=jnp.int32)[:, None] < slot_count[:, 0][None, :]
    sums_idx = jnp.where(active, (rel + 3) * PAD + p, SECT)
    size = jnp.abs(rel)
    side = (rel > 0).astype(jnp.int32)
    near_idx = jnp.where(
        active & (size <= 1), jnp.where(rel == 0, 0, side + 1) * PAD + p, 3 * PAD
    )
    r = p - R
    is_polar = (lat == 0) | (lat == NLAT_DEV - 1)
    in_band = jnp.where(r < EDGE, r, jnp.where(r < EDGE + M, r - EDGE + S + R, r - M))
    below = lat == NLAT_DEV - 2
    in_next = S + R + M + jnp.where(below, r - (ROWS - B), r)
    halo = jnp.where(is_polar, S, S + R + M + B) + jnp.where(r < 0, r + R, r - ROWS)
    two = jnp.where((r < 0) | (r >= ROWS), halo, jnp.where(is_polar, in_band, in_next))
    polar_row = jnp.clip(jnp.where(lat == 0, r, r - (ROWS - E)), 0, E - 1)
    far = jnp.where(size >= 3, FAR2 + side * E + polar_row, side * SIDE + two)
    is_far = active & (size >= 2)
    held = is_polar | ((lat == 1) & (r < B)) | (below & (r >= ROWS - B))
    lost = jnp.sum((is_far & ~held).astype(jnp.float32))
    far_idx = jnp.where(is_far & held, far, FAR2 + 2 * E)
    return sums_idx, near_idx, far_idx, lost


def swap(v, axis, size, to):
    return lax.ppermute(v, axis, [(i, to(i)) for i in range(size)])


def local(tracers, weights, source_row, source_block, slot_count):
    args = (tracers, weights, source_row, source_block, slot_count)
    lost, fixed = usual(*args)

    def redo(state):
        return jnp.zeros_like(state[0]), everywhere(*args)

    _, fixed = lax.while_loop(lambda state: state[0] > 0, redo, (lost, fixed))
    return fixed.reshape(ROWS, 32, 4, C).transpose(0, 3, 1, 2)


def usual(tracers, weights, source_row, source_block, slot_count):
    lat, lon = lax.axis_index("lat"), lax.axis_index("lon")
    both = ("lat", "lon")
    w = weights[:, 0]
    q = tracers.transpose(0, 2, 3, 1).reshape(ROWS, C, C)
    qs = lax.optimization_barrier(jnp.concatenate([q[:EDGE], q[ROWS - EDGE :]], axis=0))
    ls, rs = lax.ppermute(qs, "lon", ring(1)), lax.ppermute(qs, "lon", ring(-1))
    qm = q[EDGE : ROWS - EDGE]
    lm, rm = lax.ppermute(qm, "lon", ring(1)), lax.ppermute(qm, "lon", ring(-1))
    pole = jnp.where(lat == 0, qs[:E], qs[S - E :])
    l3 = lax.ppermute(pole, both, some(3, POLAR))
    r3 = lax.ppermute(pole, both, some(-3, POLAR))
    sums_idx, near_idx, far_idx, lost = tables(source_row, source_block, slot_count, lat, lon)
    area = latitude_area(lat * ROWS, ROWS)
    to_left, to_right, own_sums = sums_call(sums_idx, area, w)
    cl = lax.ppermute(to_left, "lon", ring(-1))
    cr = lax.ppermute(to_right, "lon", ring(1))
    up1 = lax.ppermute(jnp.concatenate([v[S - R :] for v in (qs, ls, rs)], axis=0), "lat", UP)
    dn1 = lax.ppermute(jnp.concatenate([v[:R] for v in (qs, ls, rs)], axis=0), "lat", DOWN)
    at = jnp.where(jnp.arange(NLAT_DEV, dtype=jnp.int32) == lat, R, R + ROWS - E).astype(jnp.int32)
    v, near = mass_call(
        area, lost.reshape(1), at,
        (own_sums, cl, cr, q, ls, lm, rs, rm, up1, dn1, l3, r3),
    )
    near = pltpu.with_memory_space_constraint(near, pltpu.VMEM)
    for axis, size, bit in (("lat", NLAT_DEV, 1), ("lat", NLAT_DEV, 2), ("lat", NLAT_DEV, 4), ("lon", NLON_DEV, 4), ("lon", NLON_DEV, 8)):
        v = v + swap(v, axis, size, lambda i, bit=bit: i ^ bit)
    y = [swap(v, "lon", NLON_DEV, lambda i, by=by: i // 4 * 4 + (i + by) % 4) for by in (1, 2, 3)]
    v = v + (y[0] + y[2]) + y[1]
    corr = jnp.broadcast_to((v[0] * (1.0 / TOTAL_AREA))[:, None], (C, C))

    beyond = jnp.where((lat == 0) | (lat == NLAT_DEV - 2), dn1[R:], up1[R:])
    sides = ((ls, beyond[:R], 1), (rs, beyond[R:], -1))
    lls, rrs = (
        lax.ppermute(jnp.concatenate([x, h], axis=0), both, some(d, POLAR)) for x, h, d in sides
    )
    llb, rrb = (
        lax.ppermute(
            jnp.concatenate([jnp.where(lat == 1, x[:B], x[S - B :]), h], axis=0),
            both, some(d, NEXT),
        )
        for x, h, d in sides
    )
    llm, rrm = (lax.ppermute(x, both, some(d, POLAR)) for x, d in ((lm, 1), (rm, -1)))

    pieces = [inner_call(c, near_idx, w, near) for c in range(CHUNKS)]
    partial, wv = ([pltpu.with_memory_space_constraint(x, pltpu.VMEM) for x in p] for p in zip(*pieces))
    held = lambda x: pltpu.with_memory_space_constraint(x, pltpu.VMEM)
    first, src = outer_call(
        0, far_idx, (lls, llm, llb, rrs, rrm, rrb, l3, r3), partial[:HALF], wv[:HALF]
    )
    (second,) = outer_call(1, far_idx, (held(src),), partial[HALF:], wv[HALF:])
    fixed = write_call(corr, held(first), held(second))
    return v[1, 0], fixed


def solution(mesh):
    placed = (
        P("lat", "lon", None, None),
        P("lat", "lon", None, None, None),
        P("lat", "lon", None),
        P("lat", "lon", None),
        P("lat", "lon"),
    )
    return jax.shard_map(
        local, mesh=mesh, in_specs=placed, out_specs=P("lat", "lon", None, None), check_vma=False
    )
```

```python
import functools
import math

import jax
import jax.numpy as jnp
from jax import lax
from jax.experimental import pallas as pl
from jax.experimental.pallas import tpu as pltpu
from jax.sharding import PartitionSpec as P

ROWS = 64
C = 128
KMAX = 8
R = 4
E = R + 1
MID = ROWS - 2 * E
PAD = ROWS + 2 * R
NLAT, NLON_DEV, NLAT_DEV = 512, 16, 8
TB = 4
FAR = 2 * PAD
NT = (((1,), (1,)), ((), ()))


def ring(by):
    return [(i, (i + by) % NLON_DEV) for i in range(NLON_DEV)]


UP = [(i, i + 1) for i in range(NLAT_DEV - 1)]
DOWN = [(i + 1, i) for i in range(NLAT_DEV - 1)]


def polar(by):
    return [
        (a * NLON_DEV + i, a * NLON_DEV + (i + by) % NLON_DEV)
        for a in (0, NLAT_DEV - 1)
        for i in range(NLON_DEV)
    ]


def near_kernel(idx_ref, w_ref, *refs):
    parts, (out_ref, src, sem) = refs[:-3], refs[-3:]
    step = pl.program_id(0)
    own, le, lm, re, rm, up, dn = parts

    def copies():
        todo = [(own, 0, ROWS, 0 * PAD + R)]
        for n, (e, m) in enumerate(((le, lm), (re, rm))):
            at = (n + 1) * PAD + R
            todo.append((e, 0, E, at))
            todo.append((m, 0, MID, at + E))
            todo.append((e, E, E, at + E + MID))
        for n in range(3):
            todo.append((up, n * R, R, n * PAD))
            todo.append((dn, n * R, R, n * PAD + R + ROWS))
        return [
            pltpu.make_async_copy(ref.at[pl.ds(a, n)], src.at[pl.ds(to, n)], sem.at[i])
            for i, (ref, a, n, to) in enumerate(todo)
        ]

    @pl.when(step == 0)
    def _():
        for copy in copies():
            copy.start()
        src[3 * PAD] = jnp.zeros((C, C), src.dtype)
        for copy in copies():
            copy.wait()

    for j in range(TB):
        t = step * TB + j
        lhs = jnp.concatenate([src[idx_ref[k, t]] for k in range(KMAX)], axis=1)
        rhs = jnp.concatenate([w_ref[j, k] for k in range(KMAX)], axis=1)
        out_ref[j] = lax.dot_general(lhs, rhs, NT, preferred_element_type=jnp.float32)


def near_call(idx, weights, parts):
    n_copies = 7 + 6
    return pl.pallas_call(
        near_kernel,
        grid_spec=pltpu.PrefetchScalarGridSpec(
            num_scalar_prefetch=1,
            grid=(ROWS // TB,),
            in_specs=[pl.BlockSpec((TB, KMAX, C, C), lambda s, i: (s, 0, 0, 0))]
            + [pl.BlockSpec(memory_space=pltpu.HBM)] * len(parts),
            out_specs=pl.BlockSpec((TB, C, C), lambda s, i: (s, 0, 0)),
            scratch_shapes=[
                pltpu.VMEM((3 * PAD + 1, C, C), jnp.bfloat16),
                pltpu.SemaphoreType.DMA((n_copies,)),
            ],
        ),
        out_shape=jax.ShapeDtypeStruct((ROWS, C, C), jnp.float32),
        compiler_params=pltpu.CompilerParams(
            dimension_semantics=("arbitrary",), vmem_limit_bytes=20 << 20
        ),
        cost_estimate=pl.CostEstimate(
            flops=2 * ROWS * KMAX * C**3, bytes_accessed=28 << 20, transcendentals=0
        ),
        name="near",
    )(idx, weights, *parts)


GROUP = 8


def far_kernel(lst_ref, num_ref, area_ref, w_hbm, le, lm, re, rm, up, dn, l3, r3, part_ref, out_ref, mass_ref, src, wbuf, sem, wsem):
    todo = []
    for n, (e, m) in enumerate(((le, lm), (re, rm))):
        at = n * PAD + R
        todo.append((e, 0, E, at))
        todo.append((m, 0, MID, at + E))
        todo.append((e, E, E, at + E + MID))
        todo.append((up, n * R, R, n * PAD))
        todo.append((dn, n * R, R, n * PAD + R + ROWS))
    todo.append((l3, 0, E, FAR))
    todo.append((r3, 0, E, FAR + E))
    copies = [
        pltpu.make_async_copy(ref.at[pl.ds(a, n)], src.at[pl.ds(to, n)], sem.at[i])
        for i, (ref, a, n, to) in enumerate(todo)
    ]
    for copy in copies:
        copy.start()
    groups = num_ref[0]

    def entry(g, j):
        v = lst_ref[g * GROUP + j]
        slot = lax.shift_right_logical(v, 9)
        return lax.shift_right_logical(slot, 3), slot & (KMAX - 1), v & 511

    def weight_copy(g, j):
        t, k, _ = entry(g, j)
        return pltpu.make_async_copy(w_hbm.at[t, k], wbuf.at[g * GROUP + j], wsem.at[g])

    def issue(g, carry):
        for j in range(GROUP):
            weight_copy(g, j).start()
        return carry

    lax.fori_loop(0, groups, issue, 0)
    out_ref[...] = part_ref[...]
    src[FAR + 2 * E] = jnp.zeros((C, C), src.dtype)
    for copy in copies:
        copy.wait()

    def work(g, carry):
        for j in range(GROUP):
            weight_copy(g, j).wait()
        got = []
        for j in range(GROUP):
            t, _, s = entry(g, j)
            got.append(
                (t, lax.dot_general(src[s], wbuf[g * GROUP + j], NT, preferred_element_type=jnp.float32))
            )
        for t, d in got:
            out_ref[t] = out_ref[t] + d
        return carry

    lax.fori_loop(0, groups, work, 0)

    def add_up(t, acc):
        return acc + area_ref[t] * out_ref[t]

    acc = lax.fori_loop(0, ROWS, add_up, jnp.zeros((C, C), jnp.float32), unroll=4)
    mass_ref[...] = lax.dot_general(
        jnp.ones((8, C), jnp.float32), acc, NT,
        precision=lax.Precision.HIGHEST, preferred_element_type=jnp.float32,
    )


def far_call(lst, num, area, weights, parts, partial):
    smem = pl.BlockSpec(memory_space=pltpu.SMEM)
    hbm = pl.BlockSpec(memory_space=pltpu.HBM)
    vmem = pl.BlockSpec(memory_space=pltpu.VMEM)
    return pl.pallas_call(
        far_kernel,
        in_specs=[smem, smem, smem, hbm] + [hbm] * len(parts) + [vmem],
        out_specs=[vmem, vmem],
        out_shape=[
            jax.ShapeDtypeStruct((ROWS, C, C), jnp.float32),
            jax.ShapeDtypeStruct((8, C), jnp.float32),
        ],
        scratch_shapes=[
            pltpu.VMEM((FAR + 2 * E + 1, C, C), jnp.bfloat16),
            pltpu.VMEM((ROWS * KMAX, C, C), jnp.bfloat16),
            pltpu.SemaphoreType.DMA((12,)),
            pltpu.SemaphoreType.DMA((ROWS * KMAX // GROUP,)),
        ],
        compiler_params=pltpu.CompilerParams(vmem_limit_bytes=40 << 20),
        cost_estimate=pl.CostEstimate(
            flops=2 * ROWS * KMAX * C**3 // 2, bytes_accessed=20 << 20, transcendentals=0
        ),
        name="far",
    )(lst, num, area, weights, *parts, partial)


def latitude_area(first_row, count_rows):
    rows_all = jnp.arange(count_rows, dtype=jnp.int32) + first_row
    angle = -0.5 * math.pi + (rows_all.astype(jnp.float32) + 0.5) * (math.pi / NLAT)
    return jnp.cos(angle)


def slots(source_row, source_block, slot_count, lat, lon):
    row = source_row[:, 0, :].T - (lat * ROWS - R)
    row = jnp.clip(row, 0, PAD - 1)
    rel = (source_block[:, 0, :].T - lon + 3) % NLON_DEV - 3
    active = jnp.arange(KMAX, dtype=jnp.int32)[:, None] < slot_count[:, 0][None, :]
    size = jnp.abs(rel)
    side = (rel > 0).astype(jnp.int32)
    is_near = active & (size <= 1)
    near = jnp.where(is_near, jnp.where(rel == 0, 0, side + 1) * PAD + row, 3 * PAD)
    polar_row = jnp.clip(jnp.where(lat == 0, row - R, row - R - (ROWS - E)), 0, E - 1)
    far = jnp.where(size >= 3, FAR + side * E + polar_row, side * PAD + row)
    is_far = active & (size >= 2)
    target = jnp.arange(ROWS, dtype=jnp.int32)[None, :]
    slot = target * KMAX + jnp.arange(KMAX, dtype=jnp.int32)[:, None]
    order = jnp.where(is_far, slot, ROWS * KMAX + slot)
    zero = FAR + 2 * E
    packed = (order * 512 + jnp.where(is_far, far, zero)).reshape(-1)
    packed = jnp.sort(packed) & (ROWS * KMAX * 512 - 1)
    groups = (jnp.sum(is_far.astype(jnp.int32)) + GROUP - 1) // GROUP
    return near.astype(jnp.int32), packed.astype(jnp.int32), groups.reshape(1)


def everywhere(tracers, weights, source_row, source_block, slot_count):
    lat, lon = lax.axis_index("lat"), lax.axis_index("lon")
    q = tracers.transpose(0, 2, 3, 1).reshape(ROWS, C, C)
    qe = jnp.concatenate([q[:E], q[ROWS - E :]], axis=0)
    qm = q[E : ROWS - E]
    le, re = (lax.ppermute(qe, "lon", ring(1)), lax.ppermute(qe, "lon", ring(-1)))
    lm, rm = (lax.ppermute(qm, "lon", ring(1)), lax.ppermute(qm, "lon", ring(-1)))
    near_idx, far_list, far_groups = slots(source_row, source_block, slot_count, lat, lon)
    area = latitude_area(lat * ROWS, ROWS)
    total_area = C * NLON_DEV * jnp.sum(latitude_area(0, NLAT))
    mass_old = jnp.sum(area[:, None, None] * q.astype(jnp.float32), axis=(0, 2))

    up1 = lax.ppermute(jnp.concatenate([v[2 * E - R :] for v in (qe, le, re)], axis=0), "lat", UP)
    dn1 = lax.ppermute(jnp.concatenate([v[:R] for v in (qe, le, re)], axis=0), "lat", DOWN)
    lle, rre = (lax.ppermute(le, "lon", ring(1)), lax.ppermute(re, "lon", ring(-1)))
    llm, rrm = (lax.ppermute(lm, "lon", ring(1)), lax.ppermute(rm, "lon", ring(-1)))
    up2 = lax.ppermute(jnp.concatenate([v[2 * E - R :] for v in (lle, rre)], axis=0), "lat", UP)
    dn2 = lax.ppermute(jnp.concatenate([v[:R] for v in (lle, rre)], axis=0), "lat", DOWN)
    pole = [jnp.where(lat == 0, v[:E], v[E:]) for v in (lle, rre)]
    l3 = lax.ppermute(pole[0], ("lat", "lon"), polar(1))
    r3 = lax.ppermute(pole[1], ("lat", "lon"), polar(-1))

    w = weights[:, 0]
    partial = near_call(near_idx, w, (q, le, lm, re, rm, up1, dn1))
    advected, mass_new = far_call(
        far_list, far_groups, area, w, (lle, llm, rre, rrm, up2, dn2, l3, r3), partial
    )
    change = lax.psum(mass_old - mass_new[0], ("lat", "lon"))
    fixed = advected + (change / total_area)[None, :, None]
    return fixed


TOTAL_AREA = C * NLON_DEV * math.fsum(
    math.cos(-0.5 * math.pi + (j + 0.5) * math.pi / NLAT) for j in range(NLAT)
)
EDGE = 16
S = 2 * EDGE
M = ROWS - S
B = 16
SIDE = S + R + M + B + R
FAR2 = 2 * SIDE
SECT = 7 * PAD
CHUNKS = 4
PER = ROWS // CHUNKS
POLAR, NEXT = ((0, NLAT_DEV - 1), (1, NLAT_DEV - 2))


def some(by, lats):
    return [
        (a * NLON_DEV + i, a * NLON_DEV + (i + by) % NLON_DEV) for a in lats for i in range(NLON_DEV)
    ]


WC = 16
WT = ROWS // WC


def sums_kernel(idx_ref, area_ref, w_hbm, *refs):
    left, right, own, wv, acc, sem = refs

    def copy(c):
        rows = pl.ds(c * WT, WT)
        return pltpu.make_async_copy(w_hbm.at[rows], wv.at[rows], sem.at[c])

    def start(c, carry):
        copy(c).start()
        return carry

    lax.fori_loop(0, WC, start, 0)
    acc[...] = jnp.zeros(acc.shape, acc.dtype)

    def work(c, carry):
        copy(c).wait()
        for j in range(WT):
            t = c * WT + j
            for k in range(KMAX):
                part = jnp.sum(wv[t, k].astype(jnp.float32).reshape(C // 8, 8, C), axis=0)
                at = idx_ref[k, t]
                acc[at] = acc[at] + area_ref[t] * part
        return carry

    lax.fori_loop(0, WC, work, 0)

    def summed(rel):
        at = (rel + 3) * PAD
        return jnp.sum(acc[at : at + PAD], axis=1)

    left[:PAD] = summed(-1)
    left[PAD:] = summed(-2)
    right[:PAD] = summed(1)
    right[PAD:] = summed(2)
    own[:PAD] = summed(0)
    own[PAD : 2 * PAD] = summed(-3)
    own[2 * PAD :] = summed(3)


def sums_call(idx, area, weights):
    smem = pl.BlockSpec(memory_space=pltpu.SMEM)
    vmem = pl.BlockSpec(memory_space=pltpu.VMEM)
    return pl.pallas_call(
        sums_kernel,
        in_specs=[smem, smem, pl.BlockSpec(memory_space=pltpu.HBM)],
        out_specs=[vmem] * 3,
        out_shape=[jax.ShapeDtypeStruct((n * PAD, C), jnp.float32) for n in (2, 2, 3)],
        scratch_shapes=[
            pltpu.VMEM(weights.shape, weights.dtype),
            pltpu.VMEM((SECT + 1, 8, C), jnp.float32),
            pltpu.SemaphoreType.DMA((WC,)),
        ],
        compiler_params=pltpu.CompilerParams(vmem_limit_bytes=22 << 20),
        cost_estimate=pl.CostEstimate(
            flops=20_000_000, bytes_accessed=17 << 20, transcendentals=0
        ),
        name="sums",
    )(idx, area, pltpu.with_memory_space_constraint(weights, pltpu.HBM))


def split_kernel(q_hbm, qs, qm, sem):
    copies = [
        pltpu.make_async_copy(q_hbm.at[pl.ds(at, n)], ref.at[pl.ds(to, n)], sem.at[i])
        for i, (at, n, ref, to) in enumerate(
            ((0, EDGE, qs, 0), (ROWS - EDGE, EDGE, qs, EDGE), (EDGE, M, qm, 0))
        )
    ]
    for copy in copies:
        copy.start()
    for copy in copies:
        copy.wait()


def split_call(q):
    vmem = pl.BlockSpec(memory_space=pltpu.VMEM)
    return pl.pallas_call(
        split_kernel,
        in_specs=[pl.BlockSpec(memory_space=pltpu.HBM)],
        out_specs=[vmem, vmem],
        out_shape=[pltpu.VMEM((n, C, C), jnp.bfloat16) for n in (S, M)],
        scratch_shapes=[pltpu.SemaphoreType.DMA((3,))],
        compiler_params=pltpu.CompilerParams(vmem_limit_bytes=1 << 20),
        cost_estimate=pl.CostEstimate(flops=1000, bytes_accessed=2 << 20, transcendentals=0),
        name="split",
    )(pltpu.with_memory_space_constraint(q, pltpu.HBM))


def pack_kernel(qs, ls, rs, up, dn):
    for n, v in enumerate((qs, ls, rs)):
        up[pl.ds(n * R, R)] = v[S - R :]
        dn[pl.ds(n * R, R)] = v[:R]


def pack_call(parts):
    vmem = pl.BlockSpec(memory_space=pltpu.VMEM)
    return pl.pallas_call(
        pack_kernel,
        in_specs=[vmem] * 3,
        out_specs=[vmem, vmem],
        out_shape=[pltpu.VMEM((3 * R, C, C), jnp.bfloat16)] * 2,
        compiler_params=pltpu.CompilerParams(vmem_limit_bytes=6 << 20),
        cost_estimate=pl.CostEstimate(flops=1000, bytes_accessed=1000, transcendentals=0),
        name="pack",
    )(*parts)


def mass_kernel(area_ref, lost_ref, at_ref, w_hbm, c0, cl, cr, qs, qm, ls, lm, rs, rm, up, dn, l3, r3, out_ref, src, wv, by, sem):
    def copy(c):
        rows = pl.ds(c * WT, WT)
        return pltpu.make_async_copy(w_hbm.at[rows], wv.at[rows], sem.at[c])

    for c in range(WC):
        copy(c).start()
    for n, (e, m) in enumerate(((qs, qm), (ls, lm), (rs, rm))):
        at = n * PAD + R
        src[pl.ds(at, EDGE)] = e[:EDGE]
        src[pl.ds(at + EDGE, M)] = m[...]
        src[pl.ds(at + EDGE + M, EDGE)] = e[EDGE:]
    for n in range(3):
        src[pl.ds(n * PAD, R)] = up[pl.ds(n * R, R)]
        src[pl.ds(n * PAD + R + ROWS, R)] = dn[pl.ds(n * R, R)]
    src[3 * PAD] = jnp.zeros((C, C), src.dtype)
    by[:PAD] = (c0[:PAD] + cl[:PAD]) + cr[:PAD]
    by[PAD : 2 * PAD] = cl[PAD:]
    by[2 * PAD :] = cr[PAD:]
    for r in range(ROWS):
        by[R + r : R + r + 1] = by[R + r : R + r + 1] - area_ref[r]

    def body(p, acc):
        return acc + by[pl.ds(p, 1)] * src[p].astype(jnp.float32)

    acc = lax.fori_loop(0, 3 * PAD, body, jnp.zeros((C, C), jnp.float32), unroll=4)
    at = at_ref[0]
    for i in range(E):
        acc = acc + c0[pl.ds(PAD + at + i, 1)] * l3[i].astype(jnp.float32)
        acc = acc + c0[pl.ds(2 * PAD + at + i, 1)] * r3[i].astype(jnp.float32)
    change = lax.dot_general(
        jnp.full((8, C), -1.0, jnp.float32), acc, NT,
        precision=lax.Precision.HIGHEST, preferred_element_type=jnp.float32,
    )
    row = lax.broadcasted_iota(jnp.int32, (8, C), 0)
    out_ref[...] = jnp.where(row == 0, change, lost_ref[0])
    for c in range(WC):
        copy(c).wait()


def mass_call(area, lost, at, weights, parts):
    smem = pl.BlockSpec(memory_space=pltpu.SMEM)
    vmem = pl.BlockSpec(memory_space=pltpu.VMEM)
    return pl.pallas_call(
        mass_kernel,
        in_specs=[smem] * 3 + [pl.BlockSpec(memory_space=pltpu.HBM)] + [vmem] * len(parts),
        out_specs=[vmem] * 3,
        out_shape=[
            jax.ShapeDtypeStruct((8, C), jnp.float32),
            pltpu.VMEM((3 * PAD + 1, C, C), jnp.bfloat16),
            pltpu.VMEM(weights.shape, weights.dtype),
        ],
        scratch_shapes=[
            pltpu.VMEM((3 * PAD, C), jnp.float32),
            pltpu.SemaphoreType.DMA((WC,)),
        ],
        compiler_params=pltpu.CompilerParams(vmem_limit_bytes=6 << 20),
        cost_estimate=pl.CostEstimate(
            flops=9_000_000, bytes_accessed=3 << 20, transcendentals=0
        ),
        name="mass",
    )(area, lost, at, pltpu.with_memory_space_constraint(weights, pltpu.HBM), *parts)


def inner_kernel(first, idx_ref, wv, src, out_ref):
    def body(j, carry):
        t = first + j
        lhs = jnp.concatenate([src[idx_ref[k, t]] for k in range(KMAX)], axis=1)
        rhs = jnp.concatenate([wv[t, k] for k in range(KMAX)], axis=1)
        out_ref[j] = lax.dot_general(lhs, rhs, NT, preferred_element_type=jnp.float32)
        return carry

    lax.fori_loop(0, PER, body, 0, unroll=4)


def inner_call(chunk, idx, wv, near):
    vmem = pl.BlockSpec(memory_space=pltpu.VMEM)
    return pl.pallas_call(
        functools.partial(inner_kernel, chunk * PER),
        in_specs=[pl.BlockSpec(memory_space=pltpu.SMEM), vmem, vmem],
        out_specs=vmem,
        out_shape=pltpu.VMEM((PER, C, C), jnp.float32),
        compiler_params=pltpu.CompilerParams(vmem_limit_bytes=2 << 20),
        cost_estimate=pl.CostEstimate(
            flops=2 * PER * KMAX * C**3, bytes_accessed=1 << 20, transcendentals=0
        ),
    )(idx, wv, near)


HALF = CHUNKS // 2


def far_part(first, idx_ref, wv, src, partial, out_ref):
    for c in range(HALF):

        def body(j, carry):
            t = first + c * PER + j
            lhs = jnp.concatenate([src[idx_ref[k, t]] for k in range(KMAX)], axis=1)
            rhs = jnp.concatenate([wv[t, k] for k in range(KMAX)], axis=1)
            got = lax.dot_general(lhs, rhs, NT, preferred_element_type=jnp.float32)
            out_ref[c * PER + j] = got + partial[c][j]
            return carry

        lax.fori_loop(0, PER, body, 0, unroll=4)


def outer0_kernel(idx_ref, wv, ls, lm, lb, rs, rm, rb, l3, r3, *refs):
    partial, (out_ref, src) = refs[:HALF], refs[HALF:]
    for n, (e, m, b) in enumerate(((ls, lm, lb), (rs, rm, rb))):
        at = n * SIDE
        src[pl.ds(at, S + R)] = e[...]
        src[pl.ds(at + S + R, M)] = m[...]
        src[pl.ds(at + S + R + M, B + R)] = b[...]
    src[pl.ds(FAR2, E)] = l3[...]
    src[pl.ds(FAR2 + E, E)] = r3[...]
    src[FAR2 + 2 * E] = jnp.zeros((C, C), src.dtype)
    far_part(0, idx_ref, wv, src, partial, out_ref)


def outer1_kernel(idx_ref, wv, src, *refs):
    far_part(HALF * PER, idx_ref, wv, src, refs[:HALF], refs[HALF])


def outer_call(half, idx, wv, parts, partial):
    vmem = pl.BlockSpec(memory_space=pltpu.VMEM)
    out_shape = [pltpu.VMEM((HALF * PER, C, C), jnp.float32)]
    if half == 0:
        out_shape.append(pltpu.VMEM((FAR2 + 2 * E + 1, C, C), jnp.bfloat16))
    return pl.pallas_call(
        (outer0_kernel, outer1_kernel)[half],
        in_specs=[pl.BlockSpec(memory_space=pltpu.SMEM)]
        + [vmem] * (1 + len(parts) + len(partial)),
        out_specs=[vmem] * len(out_shape),
        out_shape=out_shape,
        compiler_params=pltpu.CompilerParams(vmem_limit_bytes=8 << 20),
        cost_estimate=pl.CostEstimate(
            flops=2 * HALF * PER * KMAX * C**3, bytes_accessed=1 << 20, transcendentals=0
        ),
    )(idx, wv, *parts, *partial)


WRITES = 8


def write_kernel(corr_ref, a_ref, b_ref, out_hbm, buf, sem):
    rows = ROWS // WRITES

    def copy(c):
        at = pl.ds(c * rows, rows)
        return pltpu.make_async_copy(buf.at[at], out_hbm.at[at], sem.at[c])

    for c in range(WRITES):
        ref = a_ref if c < WRITES // 2 else b_ref
        for i in range(rows):
            t = c * rows + i
            buf[t] = ref[t % (ROWS // 2)] + corr_ref[...]
        copy(c).start()
    for c in range(WRITES):
        copy(c).wait()


def write_call(corr, first, second):
    vmem = pl.BlockSpec(memory_space=pltpu.VMEM)
    return pl.pallas_call(
        write_kernel,
        in_specs=[vmem] * 3,
        out_specs=pl.BlockSpec(memory_space=pltpu.HBM),
        out_shape=jax.ShapeDtypeStruct((ROWS, C, C), jnp.float32),
        scratch_shapes=[
            pltpu.VMEM((ROWS, C, C), jnp.float32),
            pltpu.SemaphoreType.DMA((WRITES,)),
        ],
        compiler_params=pltpu.CompilerParams(vmem_limit_bytes=6 << 20),
        cost_estimate=pl.CostEstimate(
            flops=1_000_000, bytes_accessed=4 << 20, transcendentals=0
        ),
        name="write",
    )(corr, first, second)


def tables(source_row, source_block, slot_count, lat, lon):
    p = source_row[:, 0, :].T - (lat * ROWS - R)
    p = jnp.clip(p, 0, PAD - 1)
    rel = (source_block[:, 0, :].T - lon + 3) % NLON_DEV - 3
    rel = jnp.clip(rel, -3, 3)
    active = jnp.arange(KMAX, dtype=jnp.int32)[:, None] < slot_count[:, 0][None, :]
    sums_idx = jnp.where(active, (rel + 3) * PAD + p, SECT)
    size = jnp.abs(rel)
    side = (rel > 0).astype(jnp.int32)
    near_idx = jnp.where(
        active & (size <= 1), jnp.where(rel == 0, 0, side + 1) * PAD + p, 3 * PAD
    )
    r = p - R
    is_polar = (lat == 0) | (lat == NLAT_DEV - 1)
    in_band = jnp.where(r < EDGE, r, jnp.where(r < EDGE + M, r - EDGE + S + R, r - M))
    below = lat == NLAT_DEV - 2
    in_next = S + R + M + jnp.where(below, r - (ROWS - B), r)
    halo = jnp.where(is_polar, S, S + R + M + B) + jnp.where(r < 0, r + R, r - ROWS)
    two = jnp.where((r < 0) | (r >= ROWS), halo, jnp.where(is_polar, in_band, in_next))
    polar_row = jnp.clip(jnp.where(lat == 0, r, r - (ROWS - E)), 0, E - 1)
    far = jnp.where(size >= 3, FAR2 + side * E + polar_row, side * SIDE + two)
    is_far = active & (size >= 2)
    held = is_polar | ((lat == 1) & (r < B)) | (below & (r >= ROWS - B))
    lost = jnp.sum((is_far & ~held).astype(jnp.float32))
    far_idx = jnp.where(is_far & held, far, FAR2 + 2 * E)
    return sums_idx, near_idx, far_idx, lost


def swap(v, axis, size, to):
    return lax.ppermute(v, axis, [(i, to(i)) for i in range(size)])


def local(tracers, weights, source_row, source_block, slot_count):
    args = (tracers, weights, source_row, source_block, slot_count)
    lost, fixed = usual(*args)

    def redo(state):
        return jnp.zeros_like(state[0]), everywhere(*args)

    _, fixed = lax.while_loop(lambda state: state[0] > 0, redo, (lost, fixed))
    return fixed.reshape(ROWS, 32, 4, C).transpose(0, 3, 1, 2)


def usual(tracers, weights, source_row, source_block, slot_count):
    lat, lon = lax.axis_index("lat"), lax.axis_index("lon")
    both = ("lat", "lon")
    w = weights[:, 0]
    q = tracers.transpose(0, 2, 3, 1).reshape(ROWS, C, C)
    qs, qm = split_call(q)
    ls, rs = lax.ppermute(qs, "lon", ring(1)), lax.ppermute(qs, "lon", ring(-1))
    lm, rm = lax.ppermute(qm, "lon", ring(1)), lax.ppermute(qm, "lon", ring(-1))
    pole = jnp.where(lat == 0, qs[:E], qs[S - E :])
    l3 = lax.ppermute(pole, both, some(3, POLAR))
    r3 = lax.ppermute(pole, both, some(-3, POLAR))
    sums_idx, near_idx, far_idx, lost = tables(source_row, source_block, slot_count, lat, lon)
    area = latitude_area(lat * ROWS, ROWS)
    to_left, to_right, own_sums = sums_call(sums_idx, area, w)
    cl = lax.ppermute(to_left, "lon", ring(-1))
    cr = lax.ppermute(to_right, "lon", ring(1))
    first, last = pack_call((qs, ls, rs))
    up1, dn1 = lax.ppermute(first, "lat", UP), lax.ppermute(last, "lat", DOWN)
    at = jnp.where(jnp.arange(NLAT_DEV, dtype=jnp.int32) == lat, R, R + ROWS - E).astype(jnp.int32)
    v, near, wv = mass_call(
        area, lost.reshape(1), at, w,
        (own_sums, cl, cr, qs, qm, ls, lm, rs, rm, up1, dn1, l3, r3),
    )
    held = lambda x: pltpu.with_memory_space_constraint(x, pltpu.VMEM)
    near, wv = held(near), held(wv)
    for axis, size, bit in (("lat", NLAT_DEV, 1), ("lat", NLAT_DEV, 2), ("lat", NLAT_DEV, 4), ("lon", NLON_DEV, 4), ("lon", NLON_DEV, 8)):
        v = v + swap(v, axis, size, lambda i, bit=bit: i ^ bit)
    y = [swap(v, "lon", NLON_DEV, lambda i, by=by: i // 4 * 4 + (i + by) % 4) for by in (1, 2, 3)]
    v = v + (y[0] + y[2]) + y[1]
    corr = jnp.broadcast_to((v[0] * (1.0 / TOTAL_AREA))[:, None], (C, C))

    beyond = jnp.where((lat == 0) | (lat == NLAT_DEV - 2), dn1[R:], up1[R:])
    sides = ((ls, beyond[:R], 1), (rs, beyond[R:], -1))
    lls, rrs = (
        lax.ppermute(jnp.concatenate([x, h], axis=0), both, some(d, POLAR)) for x, h, d in sides
    )
    llb, rrb = (
        lax.ppermute(
            jnp.concatenate([jnp.where(lat == 1, x[:B], x[S - B :]), h], axis=0),
            both, some(d, NEXT),
        )
        for x, h, d in sides
    )
    llm, rrm = (lax.ppermute(x, both, some(d, POLAR)) for x, d in ((lm, 1), (rm, -1)))

    partial = [held(inner_call(c, near_idx, wv, near)) for c in range(CHUNKS)]
    first, src = outer_call(
        0, far_idx, wv, (lls, llm, llb, rrs, rrm, rrb, l3, r3), partial[:HALF]
    )
    (second,) = outer_call(1, far_idx, wv, (held(src),), partial[HALF:])
    fixed = write_call(corr, held(first), held(second))
    return v[1, 0], fixed


def solution(mesh):
    placed = (
        P("lat", "lon", None, None),
        P("lat", "lon", None, None, None),
        P("lat", "lon", None),
        P("lat", "lon", None),
        P("lat", "lon"),
    )
    return jax.shard_map(
        local, mesh=mesh, in_specs=placed, out_specs=P("lat", "lon", None, None), check_vma=False
    )
```

```python
import functools
import math

import jax
import jax.numpy as jnp
from jax import lax
from jax.experimental import pallas as pl
from jax.experimental.pallas import tpu as pltpu
from jax.sharding import PartitionSpec as P

ROWS = 64
C = 128
KMAX = 8
R = 4
E = R + 1
MID = ROWS - 2 * E
PAD = ROWS + 2 * R
NLAT, NLON_DEV, NLAT_DEV = 512, 16, 8
TB = 4
FAR = 2 * PAD
NT = (((1,), (1,)), ((), ()))


def ring(by):
    return [(i, (i + by) % NLON_DEV) for i in range(NLON_DEV)]


UP = [(i, i + 1) for i in range(NLAT_DEV - 1)]
DOWN = [(i + 1, i) for i in range(NLAT_DEV - 1)]


def polar(by):
    return [
        (a * NLON_DEV + i, a * NLON_DEV + (i + by) % NLON_DEV)
        for a in (0, NLAT_DEV - 1)
        for i in range(NLON_DEV)
    ]


def near_kernel(idx_ref, w_ref, *refs):
    parts, (out_ref, src, sem) = refs[:-3], refs[-3:]
    step = pl.program_id(0)
    own, le, lm, re, rm, up, dn = parts

    def copies():
        todo = [(own, 0, ROWS, 0 * PAD + R)]
        for n, (e, m) in enumerate(((le, lm), (re, rm))):
            at = (n + 1) * PAD + R
            todo.append((e, 0, E, at))
            todo.append((m, 0, MID, at + E))
            todo.append((e, E, E, at + E + MID))
        for n in range(3):
            todo.append((up, n * R, R, n * PAD))
            todo.append((dn, n * R, R, n * PAD + R + ROWS))
        return [
            pltpu.make_async_copy(ref.at[pl.ds(a, n)], src.at[pl.ds(to, n)], sem.at[i])
            for i, (ref, a, n, to) in enumerate(todo)
        ]

    @pl.when(step == 0)
    def _():
        for copy in copies():
            copy.start()
        src[3 * PAD] = jnp.zeros((C, C), src.dtype)
        for copy in copies():
            copy.wait()

    for j in range(TB):
        t = step * TB + j
        lhs = jnp.concatenate([src[idx_ref[k, t]] for k in range(KMAX)], axis=1)
        rhs = jnp.concatenate([w_ref[j, k] for k in range(KMAX)], axis=1)
        out_ref[j] = lax.dot_general(lhs, rhs, NT, preferred_element_type=jnp.float32)


def near_call(idx, weights, parts):
    n_copies = 7 + 6
    return pl.pallas_call(
        near_kernel,
        grid_spec=pltpu.PrefetchScalarGridSpec(
            num_scalar_prefetch=1,
            grid=(ROWS // TB,),
            in_specs=[pl.BlockSpec((TB, KMAX, C, C), lambda s, i: (s, 0, 0, 0))]
            + [pl.BlockSpec(memory_space=pltpu.HBM)] * len(parts),
            out_specs=pl.BlockSpec((TB, C, C), lambda s, i: (s, 0, 0)),
            scratch_shapes=[
                pltpu.VMEM((3 * PAD + 1, C, C), jnp.bfloat16),
                pltpu.SemaphoreType.DMA((n_copies,)),
            ],
        ),
        out_shape=jax.ShapeDtypeStruct((ROWS, C, C), jnp.float32),
        compiler_params=pltpu.CompilerParams(
            dimension_semantics=("arbitrary",), vmem_limit_bytes=20 << 20
        ),
        cost_estimate=pl.CostEstimate(
            flops=2 * ROWS * KMAX * C**3, bytes_accessed=28 << 20, transcendentals=0
        ),
        name="near",
    )(idx, weights, *parts)


GROUP = 8


def far_kernel(lst_ref, num_ref, area_ref, w_hbm, le, lm, re, rm, up, dn, l3, r3, part_ref, out_ref, mass_ref, src, wbuf, sem, wsem):
    todo = []
    for n, (e, m) in enumerate(((le, lm), (re, rm))):
        at = n * PAD + R
        todo.append((e, 0, E, at))
        todo.append((m, 0, MID, at + E))
        todo.append((e, E, E, at + E + MID))
        todo.append((up, n * R, R, n * PAD))
        todo.append((dn, n * R, R, n * PAD + R + ROWS))
    todo.append((l3, 0, E, FAR))
    todo.append((r3, 0, E, FAR + E))
    copies = [
        pltpu.make_async_copy(ref.at[pl.ds(a, n)], src.at[pl.ds(to, n)], sem.at[i])
        for i, (ref, a, n, to) in enumerate(todo)
    ]
    for copy in copies:
        copy.start()
    groups = num_ref[0]

    def entry(g, j):
        v = lst_ref[g * GROUP + j]
        slot = lax.shift_right_logical(v, 9)
        return lax.shift_right_logical(slot, 3), slot & (KMAX - 1), v & 511

    def weight_copy(g, j):
        t, k, _ = entry(g, j)
        return pltpu.make_async_copy(w_hbm.at[t, k], wbuf.at[g * GROUP + j], wsem.at[g])

    def issue(g, carry):
        for j in range(GROUP):
            weight_copy(g, j).start()
        return carry

    lax.fori_loop(0, groups, issue, 0)
    out_ref[...] = part_ref[...]
    src[FAR + 2 * E] = jnp.zeros((C, C), src.dtype)
    for copy in copies:
        copy.wait()

    def work(g, carry):
        for j in range(GROUP):
            weight_copy(g, j).wait()
        got = []
        for j in range(GROUP):
            t, _, s = entry(g, j)
            got.append(
                (t, lax.dot_general(src[s], wbuf[g * GROUP + j], NT, preferred_element_type=jnp.float32))
            )
        for t, d in got:
            out_ref[t] = out_ref[t] + d
        return carry

    lax.fori_loop(0, groups, work, 0)

    def add_up(t, acc):
        return acc + area_ref[t] * out_ref[t]

    acc = lax.fori_loop(0, ROWS, add_up, jnp.zeros((C, C), jnp.float32), unroll=4)
    mass_ref[...] = lax.dot_general(
        jnp.ones((8, C), jnp.float32), acc, NT,
        precision=lax.Precision.HIGHEST, preferred_element_type=jnp.float32,
    )


def far_call(lst, num, area, weights, parts, partial):
    smem = pl.BlockSpec(memory_space=pltpu.SMEM)
    hbm = pl.BlockSpec(memory_space=pltpu.HBM)
    vmem = pl.BlockSpec(memory_space=pltpu.VMEM)
    return pl.pallas_call(
        far_kernel,
        in_specs=[smem, smem, smem, hbm] + [hbm] * len(parts) + [vmem],
        out_specs=[vmem, vmem],
        out_shape=[
            jax.ShapeDtypeStruct((ROWS, C, C), jnp.float32),
            jax.ShapeDtypeStruct((8, C), jnp.float32),
        ],
        scratch_shapes=[
            pltpu.VMEM((FAR + 2 * E + 1, C, C), jnp.bfloat16),
            pltpu.VMEM((ROWS * KMAX, C, C), jnp.bfloat16),
            pltpu.SemaphoreType.DMA((12,)),
            pltpu.SemaphoreType.DMA((ROWS * KMAX // GROUP,)),
        ],
        compiler_params=pltpu.CompilerParams(vmem_limit_bytes=40 << 20),
        cost_estimate=pl.CostEstimate(
            flops=2 * ROWS * KMAX * C**3 // 2, bytes_accessed=20 << 20, transcendentals=0
        ),
        name="far",
    )(lst, num, area, weights, *parts, partial)


def latitude_area(first_row, count_rows):
    rows_all = jnp.arange(count_rows, dtype=jnp.int32) + first_row
    angle = -0.5 * math.pi + (rows_all.astype(jnp.float32) + 0.5) * (math.pi / NLAT)
    return jnp.cos(angle)


def slots(source_row, source_block, slot_count, lat, lon):
    row = source_row[:, 0, :].T - (lat * ROWS - R)
    row = jnp.clip(row, 0, PAD - 1)
    rel = (source_block[:, 0, :].T - lon + 3) % NLON_DEV - 3
    active = jnp.arange(KMAX, dtype=jnp.int32)[:, None] < slot_count[:, 0][None, :]
    size = jnp.abs(rel)
    side = (rel > 0).astype(jnp.int32)
    is_near = active & (size <= 1)
    near = jnp.where(is_near, jnp.where(rel == 0, 0, side + 1) * PAD + row, 3 * PAD)
    polar_row = jnp.clip(jnp.where(lat == 0, row - R, row - R - (ROWS - E)), 0, E - 1)
    far = jnp.where(size >= 3, FAR + side * E + polar_row, side * PAD + row)
    is_far = active & (size >= 2)
    target = jnp.arange(ROWS, dtype=jnp.int32)[None, :]
    slot = target * KMAX + jnp.arange(KMAX, dtype=jnp.int32)[:, None]
    order = jnp.where(is_far, slot, ROWS * KMAX + slot)
    zero = FAR + 2 * E
    packed = (order * 512 + jnp.where(is_far, far, zero)).reshape(-1)
    packed = jnp.sort(packed) & (ROWS * KMAX * 512 - 1)
    groups = (jnp.sum(is_far.astype(jnp.int32)) + GROUP - 1) // GROUP
    return near.astype(jnp.int32), packed.astype(jnp.int32), groups.reshape(1)


def everywhere(tracers, weights, source_row, source_block, slot_count):
    lat, lon = lax.axis_index("lat"), lax.axis_index("lon")
    q = tracers.transpose(0, 2, 3, 1).reshape(ROWS, C, C)
    qe = jnp.concatenate([q[:E], q[ROWS - E :]], axis=0)
    qm = q[E : ROWS - E]
    le, re = (lax.ppermute(qe, "lon", ring(1)), lax.ppermute(qe, "lon", ring(-1)))
    lm, rm = (lax.ppermute(qm, "lon", ring(1)), lax.ppermute(qm, "lon", ring(-1)))
    near_idx, far_list, far_groups = slots(source_row, source_block, slot_count, lat, lon)
    area = latitude_area(lat * ROWS, ROWS)
    total_area = C * NLON_DEV * jnp.sum(latitude_area(0, NLAT))
    mass_old = jnp.sum(area[:, None, None] * q.astype(jnp.float32), axis=(0, 2))

    up1 = lax.ppermute(jnp.concatenate([v[2 * E - R :] for v in (qe, le, re)], axis=0), "lat", UP)
    dn1 = lax.ppermute(jnp.concatenate([v[:R] for v in (qe, le, re)], axis=0), "lat", DOWN)
    lle, rre = (lax.ppermute(le, "lon", ring(1)), lax.ppermute(re, "lon", ring(-1)))
    llm, rrm = (lax.ppermute(lm, "lon", ring(1)), lax.ppermute(rm, "lon", ring(-1)))
    up2 = lax.ppermute(jnp.concatenate([v[2 * E - R :] for v in (lle, rre)], axis=0), "lat", UP)
    dn2 = lax.ppermute(jnp.concatenate([v[:R] for v in (lle, rre)], axis=0), "lat", DOWN)
    pole = [jnp.where(lat == 0, v[:E], v[E:]) for v in (lle, rre)]
    l3 = lax.ppermute(pole[0], ("lat", "lon"), polar(1))
    r3 = lax.ppermute(pole[1], ("lat", "lon"), polar(-1))

    w = weights[:, 0]
    partial = near_call(near_idx, w, (q, le, lm, re, rm, up1, dn1))
    advected, mass_new = far_call(
        far_list, far_groups, area, w, (lle, llm, rre, rrm, up2, dn2, l3, r3), partial
    )
    change = lax.psum(mass_old - mass_new[0], ("lat", "lon"))
    fixed = advected + (change / total_area)[None, :, None]
    return fixed


TOTAL_AREA = C * NLON_DEV * math.fsum(
    math.cos(-0.5 * math.pi + (j + 0.5) * math.pi / NLAT) for j in range(NLAT)
)
EDGE = 16
S = 2 * EDGE
M = ROWS - S
B = 16
SIDE = S + R + M + B + R
FAR2 = 2 * SIDE
SECT = 7 * PAD
CHUNKS = 4
PER = ROWS // CHUNKS
POLAR, NEXT = ((0, NLAT_DEV - 1), (1, NLAT_DEV - 2))


def some(by, lats):
    return [
        (a * NLON_DEV + i, a * NLON_DEV + (i + by) % NLON_DEV) for a in lats for i in range(NLON_DEV)
    ]


WC = 16
WT = ROWS // WC


def sums_kernel(idx_ref, area_ref, w_hbm, *refs):
    wv, left, right, own, acc, sem = refs

    def copy(c):
        rows = pl.ds(c * WT, WT)
        return pltpu.make_async_copy(w_hbm.at[rows], wv.at[rows], sem.at[c])

    def start(c, carry):
        copy(c).start()
        return carry

    lax.fori_loop(0, WC, start, 0)
    acc[...] = jnp.zeros(acc.shape, acc.dtype)

    def work(c, carry):
        copy(c).wait()
        for j in range(WT):
            t = c * WT + j
            for k in range(KMAX):
                part = jnp.sum(wv[t, k].astype(jnp.float32).reshape(C // 8, 8, C), axis=0)
                at = idx_ref[k, t]
                acc[at] = acc[at] + area_ref[t] * part
        return carry

    lax.fori_loop(0, WC, work, 0)

    def summed(rel):
        at = (rel + 3) * PAD
        return jnp.sum(acc[at : at + PAD], axis=1)

    left[:PAD] = summed(-1)
    left[PAD:] = summed(-2)
    right[:PAD] = summed(1)
    right[PAD:] = summed(2)
    own[:PAD] = summed(0)
    own[PAD : 2 * PAD] = summed(-3)
    own[2 * PAD :] = summed(3)


def sums_call(idx, area, weights):
    smem = pl.BlockSpec(memory_space=pltpu.SMEM)
    vmem = pl.BlockSpec(memory_space=pltpu.VMEM)
    return pl.pallas_call(
        sums_kernel,
        in_specs=[smem, smem, pl.BlockSpec(memory_space=pltpu.HBM)],
        out_specs=[vmem] * 4,
        out_shape=[pltpu.VMEM(weights.shape, weights.dtype)]
        + [jax.ShapeDtypeStruct((n * PAD, C), jnp.float32) for n in (2, 2, 3)],
        scratch_shapes=[
            pltpu.VMEM((SECT + 1, 8, C), jnp.float32),
            pltpu.SemaphoreType.DMA((WC,)),
        ],
        compiler_params=pltpu.CompilerParams(vmem_limit_bytes=6 << 20),
        cost_estimate=pl.CostEstimate(
            flops=20_000_000, bytes_accessed=17 << 20, transcendentals=0
        ),
        name="sums",
    )(idx, area, pltpu.with_memory_space_constraint(weights, pltpu.HBM))


def split_kernel(q_hbm, qs, qm, sem):
    copies = [
        pltpu.make_async_copy(q_hbm.at[pl.ds(at, n)], ref.at[pl.ds(to, n)], sem.at[i])
        for i, (at, n, ref, to) in enumerate(
            ((0, EDGE, qs, 0), (ROWS - EDGE, EDGE, qs, EDGE), (EDGE, M, qm, 0))
        )
    ]
    for copy in copies:
        copy.start()
    for copy in copies:
        copy.wait()


def split_call(q):
    vmem = pl.BlockSpec(memory_space=pltpu.VMEM)
    return pl.pallas_call(
        split_kernel,
        in_specs=[pl.BlockSpec(memory_space=pltpu.HBM)],
        out_specs=[vmem, vmem],
        out_shape=[pltpu.VMEM((n, C, C), jnp.bfloat16) for n in (S, M)],
        scratch_shapes=[pltpu.SemaphoreType.DMA((3,))],
        compiler_params=pltpu.CompilerParams(vmem_limit_bytes=1 << 20),
        cost_estimate=pl.CostEstimate(flops=1000, bytes_accessed=2 << 20, transcendentals=0),
        name="split",
    )(pltpu.with_memory_space_constraint(q, pltpu.HBM))


def pack_kernel(qs, ls, rs, up, dn):
    for n, v in enumerate((qs, ls, rs)):
        up[pl.ds(n * R, R)] = v[S - R :]
        dn[pl.ds(n * R, R)] = v[:R]


def pack_call(parts):
    vmem = pl.BlockSpec(memory_space=pltpu.VMEM)
    return pl.pallas_call(
        pack_kernel,
        in_specs=[vmem] * 3,
        out_specs=[vmem, vmem],
        out_shape=[pltpu.VMEM((3 * R, C, C), jnp.bfloat16)] * 2,
        compiler_params=pltpu.CompilerParams(vmem_limit_bytes=6 << 20),
        cost_estimate=pl.CostEstimate(flops=1000, bytes_accessed=1000, transcendentals=0),
        name="pack",
    )(*parts)


def mass_kernel(area_ref, lost_ref, at_ref, c0, cl, cr, qs, qm, ls, lm, rs, rm, up, dn, l3, r3, out_ref, src, by):
    for n, (e, m) in enumerate(((qs, qm), (ls, lm), (rs, rm))):
        at = n * PAD + R
        src[pl.ds(at, EDGE)] = e[:EDGE]
        src[pl.ds(at + EDGE, M)] = m[...]
        src[pl.ds(at + EDGE + M, EDGE)] = e[EDGE:]
    for n in range(3):
        src[pl.ds(n * PAD, R)] = up[pl.ds(n * R, R)]
        src[pl.ds(n * PAD + R + ROWS, R)] = dn[pl.ds(n * R, R)]
    src[3 * PAD] = jnp.zeros((C, C), src.dtype)
    by[:PAD] = (c0[:PAD] + cl[:PAD]) + cr[:PAD]
    by[PAD : 2 * PAD] = cl[PAD:]
    by[2 * PAD :] = cr[PAD:]
    for r in range(ROWS):
        by[R + r : R + r + 1] = by[R + r : R + r + 1] - area_ref[r]

    def body(p, acc):
        return acc + by[pl.ds(p, 1)] * src[p].astype(jnp.float32)

    acc = lax.fori_loop(0, 3 * PAD, body, jnp.zeros((C, C), jnp.float32), unroll=4)
    at = at_ref[0]
    for i in range(E):
        acc = acc + c0[pl.ds(PAD + at + i, 1)] * l3[i].astype(jnp.float32)
        acc = acc + c0[pl.ds(2 * PAD + at + i, 1)] * r3[i].astype(jnp.float32)
    change = lax.dot_general(
        jnp.full((8, C), -1.0, jnp.float32), acc, NT,
        precision=lax.Precision.HIGHEST, preferred_element_type=jnp.float32,
    )
    row = lax.broadcasted_iota(jnp.int32, (8, C), 0)
    out_ref[...] = jnp.where(row == 0, change, lost_ref[0])


def mass_call(area, lost, at, parts):
    smem = pl.BlockSpec(memory_space=pltpu.SMEM)
    vmem = pl.BlockSpec(memory_space=pltpu.VMEM)
    return pl.pallas_call(
        mass_kernel,
        in_specs=[smem] * 3 + [vmem] * len(parts),
        out_specs=[vmem] * 2,
        out_shape=[
            jax.ShapeDtypeStruct((8, C), jnp.float32),
            pltpu.VMEM((3 * PAD + 1, C, C), jnp.bfloat16),
        ],
        scratch_shapes=[
            pltpu.VMEM((3 * PAD, C), jnp.float32),
        ],
        compiler_params=pltpu.CompilerParams(vmem_limit_bytes=6 << 20),
        cost_estimate=pl.CostEstimate(
            flops=9_000_000, bytes_accessed=3 << 20, transcendentals=0
        ),
        name="mass",
    )(area, lost, at, *parts)


def inner_kernel(first, idx_ref, wv, src, out_ref):
    def body(j, carry):
        t = first + j
        lhs = jnp.concatenate([src[idx_ref[k, t]] for k in range(KMAX)], axis=1)
        rhs = jnp.concatenate([wv[t, k] for k in range(KMAX)], axis=1)
        out_ref[j] = lax.dot_general(lhs, rhs, NT, preferred_element_type=jnp.float32)
        return carry

    lax.fori_loop(0, PER, body, 0, unroll=4)


def inner_call(chunk, idx, wv, near):
    vmem = pl.BlockSpec(memory_space=pltpu.VMEM)
    return pl.pallas_call(
        functools.partial(inner_kernel, chunk * PER),
        in_specs=[pl.BlockSpec(memory_space=pltpu.SMEM), vmem, vmem],
        out_specs=vmem,
        out_shape=pltpu.VMEM((PER, C, C), jnp.float32),
        compiler_params=pltpu.CompilerParams(vmem_limit_bytes=2 << 20),
        cost_estimate=pl.CostEstimate(
            flops=2 * PER * KMAX * C**3, bytes_accessed=1 << 20, transcendentals=0
        ),
    )(idx, wv, near)


def outer_kernel(idx_ref, wv, ls, lm, lb, rs, rm, rb, l3, r3, *refs):
    partial, (out_ref, src) = refs[:CHUNKS], refs[CHUNKS:]
    for n, (e, m, b) in enumerate(((ls, lm, lb), (rs, rm, rb))):
        at = n * SIDE
        src[pl.ds(at, S + R)] = e[...]
        src[pl.ds(at + S + R, M)] = m[...]
        src[pl.ds(at + S + R + M, B + R)] = b[...]
    src[pl.ds(FAR2, E)] = l3[...]
    src[pl.ds(FAR2 + E, E)] = r3[...]
    src[FAR2 + 2 * E] = jnp.zeros((C, C), src.dtype)
    for c in range(CHUNKS):

        def body(j, carry):
            t = c * PER + j
            lhs = jnp.concatenate([src[idx_ref[k, t]] for k in range(KMAX)], axis=1)
            rhs = jnp.concatenate([wv[t, k] for k in range(KMAX)], axis=1)
            got = lax.dot_general(lhs, rhs, NT, preferred_element_type=jnp.float32)
            out_ref[t] = got + partial[c][j]
            return carry

        lax.fori_loop(0, PER, body, 0, unroll=4)


def outer_call(idx, wv, parts, partial):
    vmem = pl.BlockSpec(memory_space=pltpu.VMEM)
    return pl.pallas_call(
        outer_kernel,
        in_specs=[pl.BlockSpec(memory_space=pltpu.SMEM)]
        + [vmem] * (1 + len(parts) + len(partial)),
        out_specs=vmem,
        out_shape=pltpu.VMEM((ROWS, C, C), jnp.float32),
        scratch_shapes=[pltpu.VMEM((FAR2 + 2 * E + 1, C, C), jnp.bfloat16)],
        compiler_params=pltpu.CompilerParams(vmem_limit_bytes=8 << 20),
        cost_estimate=pl.CostEstimate(
            flops=2 * ROWS * KMAX * C**3, bytes_accessed=1 << 20, transcendentals=0
        ),
        name="outer",
    )(idx, wv, *parts, *partial)


WRITES = 8


def write_kernel(corr_ref, in_ref, out_hbm, buf, sem):
    rows = ROWS // WRITES

    def copy(c):
        at = pl.ds(c * rows, rows)
        return pltpu.make_async_copy(buf.at[at], out_hbm.at[at], sem.at[c])

    for c in range(WRITES):
        for i in range(rows):
            t = c * rows + i
            buf[t] = in_ref[t] + corr_ref[...]
        copy(c).start()
    for c in range(WRITES):
        copy(c).wait()


def write_call(corr, advected):
    vmem = pl.BlockSpec(memory_space=pltpu.VMEM)
    return pl.pallas_call(
        write_kernel,
        in_specs=[vmem] * 2,
        out_specs=pl.BlockSpec(memory_space=pltpu.HBM),
        out_shape=jax.ShapeDtypeStruct((ROWS, C, C), jnp.float32),
        scratch_shapes=[
            pltpu.VMEM((ROWS, C, C), jnp.float32),
            pltpu.SemaphoreType.DMA((WRITES,)),
        ],
        compiler_params=pltpu.CompilerParams(vmem_limit_bytes=6 << 20),
        cost_estimate=pl.CostEstimate(
            flops=1_000_000, bytes_accessed=4 << 20, transcendentals=0
        ),
        name="write",
    )(corr, advected)


def tables(source_row, source_block, slot_count, lat, lon):
    p = source_row[:, 0, :].T - (lat * ROWS - R)
    p = jnp.clip(p, 0, PAD - 1)
    rel = (source_block[:, 0, :].T - lon + 3) % NLON_DEV - 3
    rel = jnp.clip(rel, -3, 3)
    active = jnp.arange(KMAX, dtype=jnp.int32)[:, None] < slot_count[:, 0][None, :]
    sums_idx = jnp.where(active, (rel + 3) * PAD + p, SECT)
    size = jnp.abs(rel)
    side = (rel > 0).astype(jnp.int32)
    near_idx = jnp.where(
        active & (size <= 1), jnp.where(rel == 0, 0, side + 1) * PAD + p, 3 * PAD
    )
    r = p - R
    is_polar = (lat == 0) | (lat == NLAT_DEV - 1)
    in_band = jnp.where(r < EDGE, r, jnp.where(r < EDGE + M, r - EDGE + S + R, r - M))
    below = lat == NLAT_DEV - 2
    in_next = S + R + M + jnp.where(below, r - (ROWS - B), r)
    halo = jnp.where(is_polar, S, S + R + M + B) + jnp.where(r < 0, r + R, r - ROWS)
    two = jnp.where((r < 0) | (r >= ROWS), halo, jnp.where(is_polar, in_band, in_next))
    polar_row = jnp.clip(jnp.where(lat == 0, r, r - (ROWS - E)), 0, E - 1)
    far = jnp.where(size >= 3, FAR2 + side * E + polar_row, side * SIDE + two)
    is_far = active & (size >= 2)
    held = is_polar | ((lat == 1) & (r < B)) | (below & (r >= ROWS - B))
    lost = jnp.sum((is_far & ~held).astype(jnp.float32))
    far_idx = jnp.where(is_far & held, far, FAR2 + 2 * E)
    return sums_idx, near_idx, far_idx, lost


def swap(v, axis, size, to):
    return lax.ppermute(v, axis, [(i, to(i)) for i in range(size)])


def three(v, axis, size, to):
    got = [swap(v, axis, size, functools.partial(to, by=by)) for by in (1, 2, 3)]
    return (got[0] + got[2]) + got[1]


def local(tracers, weights, source_row, source_block, slot_count):
    args = (tracers, weights, source_row, source_block, slot_count)
    lost, fixed = usual(*args)

    def redo(state):
        return jnp.zeros_like(state[0]), everywhere(*args)

    _, fixed = lax.while_loop(lambda state: state[0] > 0, redo, (lost, fixed))
    return fixed.reshape(ROWS, 32, 4, C).transpose(0, 3, 1, 2)


def usual(tracers, weights, source_row, source_block, slot_count):
    lat, lon = lax.axis_index("lat"), lax.axis_index("lon")
    both = ("lat", "lon")
    w = weights[:, 0]
    q = tracers.transpose(0, 2, 3, 1).reshape(ROWS, C, C)
    qs, qm = split_call(q)
    ls, rs = lax.ppermute(qs, "lon", ring(1)), lax.ppermute(qs, "lon", ring(-1))
    lm, rm = lax.ppermute(qm, "lon", ring(1)), lax.ppermute(qm, "lon", ring(-1))
    pole = jnp.where(lat == 0, qs[:E], qs[S - E :])
    l3 = lax.ppermute(pole, both, some(3, POLAR))
    r3 = lax.ppermute(pole, both, some(-3, POLAR))
    sums_idx, near_idx, far_idx, lost = tables(source_row, source_block, slot_count, lat, lon)
    area = latitude_area(lat * ROWS, ROWS)
    wv, to_left, to_right, own_sums = sums_call(sums_idx, area, w)
    cl = lax.ppermute(to_left, "lon", ring(-1))
    cr = lax.ppermute(to_right, "lon", ring(1))
    first, last = pack_call((qs, ls, rs))
    up1, dn1 = lax.ppermute(first, "lat", UP), lax.ppermute(last, "lat", DOWN)
    at = jnp.where(jnp.arange(NLAT_DEV, dtype=jnp.int32) == lat, R, R + ROWS - E).astype(jnp.int32)
    v, near = mass_call(
        area, lost.reshape(1), at,
        (own_sums, cl, cr, qs, qm, ls, lm, rs, rm, up1, dn1, l3, r3),
    )
    held = lambda x: pltpu.with_memory_space_constraint(x, pltpu.VMEM)
    near, wv = held(near), held(wv)
    v = v + swap(v, "lat", NLAT_DEV, lambda i: i ^ 1)
    v = v + three(v, "lat", NLAT_DEV, lambda i, by: (i + 2 * by) % NLAT_DEV)
    v = v + three(v, "lon", NLON_DEV, lambda i, by: (i + 4 * by) % NLON_DEV)
    v = v + three(v, "lon", NLON_DEV, lambda i, by: i // 4 * 4 + (i + by) % 4)
    corr = jnp.broadcast_to((v[0] * (1.0 / TOTAL_AREA))[:, None], (C, C))

    beyond = jnp.where(lat == 0, dn1[R:], jnp.where(lat == NLAT_DEV - 2, dn1[R:], up1[R:]))
    sides = ((ls, beyond[:R], 1), (rs, beyond[R:], -1))
    lls, rrs = (
        lax.ppermute(jnp.concatenate([x, h], axis=0), both, some(d, POLAR)) for x, h, d in sides
    )
    llb, rrb = (
        lax.ppermute(
            jnp.concatenate([jnp.where(lat == 1, x[:B], x[S - B :]), h], axis=0),
            both, some(d, NEXT),
        )
        for x, h, d in sides
    )
    llm, rrm = (lax.ppermute(x, both, some(d, POLAR)) for x, d in ((lm, 1), (rm, -1)))

    partial = [held(inner_call(c, near_idx, wv, near)) for c in range(CHUNKS)]
    advected = outer_call(far_idx, wv, (lls, llm, llb, rrs, rrm, rrb, l3, r3), partial)
    fixed = write_call(corr, held(advected))
    return v[1, 0], fixed


def solution(mesh):
    placed = (
        P("lat", "lon", None, None),
        P("lat", "lon", None, None, None),
        P("lat", "lon", None),
        P("lat", "lon", None),
        P("lat", "lon"),
    )
    return jax.shard_map(
        local, mesh=mesh, in_specs=placed, out_specs=P("lat", "lon", None, None), check_vma=False
    )
```

```python
import functools
import math

import jax
import jax.numpy as jnp
from jax import lax
from jax.experimental import pallas as pl
from jax.experimental.pallas import tpu as pltpu
from jax.sharding import PartitionSpec as P

ROWS = 64
C = 128
KMAX = 8
R = 4
E = R + 1
MID = ROWS - 2 * E
PAD = ROWS + 2 * R
NLAT, NLON_DEV, NLAT_DEV = 512, 16, 8
TB = 4
FAR = 2 * PAD
NT = (((1,), (1,)), ((), ()))


def ring(by):
    return [(i, (i + by) % NLON_DEV) for i in range(NLON_DEV)]


UP = [(i, i + 1) for i in range(NLAT_DEV - 1)]
DOWN = [(i + 1, i) for i in range(NLAT_DEV - 1)]


def polar(by):
    return [
        (a * NLON_DEV + i, a * NLON_DEV + (i + by) % NLON_DEV)
        for a in (0, NLAT_DEV - 1)
        for i in range(NLON_DEV)
    ]


def near_kernel(idx_ref, w_ref, *refs):
    parts, (out_ref, src, sem) = refs[:-3], refs[-3:]
    step = pl.program_id(0)
    own, le, lm, re, rm, up, dn = parts

    def copies():
        todo = [(own, 0, ROWS, 0 * PAD + R)]
        for n, (e, m) in enumerate(((le, lm), (re, rm))):
            at = (n + 1) * PAD + R
            todo.append((e, 0, E, at))
            todo.append((m, 0, MID, at + E))
            todo.append((e, E, E, at + E + MID))
        for n in range(3):
            todo.append((up, n * R, R, n * PAD))
            todo.append((dn, n * R, R, n * PAD + R + ROWS))
        return [
            pltpu.make_async_copy(ref.at[pl.ds(a, n)], src.at[pl.ds(to, n)], sem.at[i])
            for i, (ref, a, n, to) in enumerate(todo)
        ]

    @pl.when(step == 0)
    def _():
        for copy in copies():
            copy.start()
        src[3 * PAD] = jnp.zeros((C, C), src.dtype)
        for copy in copies():
            copy.wait()

    for j in range(TB):
        t = step * TB + j
        lhs = jnp.concatenate([src[idx_ref[k, t]] for k in range(KMAX)], axis=1)
        rhs = jnp.concatenate([w_ref[j, k] for k in range(KMAX)], axis=1)
        out_ref[j] = lax.dot_general(lhs, rhs, NT, preferred_element_type=jnp.float32)


def near_call(idx, weights, parts):
    n_copies = 7 + 6
    return pl.pallas_call(
        near_kernel,
        grid_spec=pltpu.PrefetchScalarGridSpec(
            num_scalar_prefetch=1,
            grid=(ROWS // TB,),
            in_specs=[pl.BlockSpec((TB, KMAX, C, C), lambda s, i: (s, 0, 0, 0))]
            + [pl.BlockSpec(memory_space=pltpu.HBM)] * len(parts),
            out_specs=pl.BlockSpec((TB, C, C), lambda s, i: (s, 0, 0)),
            scratch_shapes=[
                pltpu.VMEM((3 * PAD + 1, C, C), jnp.bfloat16),
                pltpu.SemaphoreType.DMA((n_copies,)),
            ],
        ),
        out_shape=jax.ShapeDtypeStruct((ROWS, C, C), jnp.float32),
        compiler_params=pltpu.CompilerParams(
            dimension_semantics=("arbitrary",), vmem_limit_bytes=20 << 20
        ),
        cost_estimate=pl.CostEstimate(
            flops=2 * ROWS * KMAX * C**3, bytes_accessed=28 << 20, transcendentals=0
        ),
        name="near",
    )(idx, weights, *parts)


GROUP = 8


def far_kernel(lst_ref, num_ref, area_ref, w_hbm, le, lm, re, rm, up, dn, l3, r3, part_ref, out_ref, mass_ref, src, wbuf, sem, wsem):
    todo = []
    for n, (e, m) in enumerate(((le, lm), (re, rm))):
        at = n * PAD + R
        todo.append((e, 0, E, at))
        todo.append((m, 0, MID, at + E))
        todo.append((e, E, E, at + E + MID))
        todo.append((up, n * R, R, n * PAD))
        todo.append((dn, n * R, R, n * PAD + R + ROWS))
    todo.append((l3, 0, E, FAR))
    todo.append((r3, 0, E, FAR + E))
    copies = [
        pltpu.make_async_copy(ref.at[pl.ds(a, n)], src.at[pl.ds(to, n)], sem.at[i])
        for i, (ref, a, n, to) in enumerate(todo)
    ]
    for copy in copies:
        copy.start()
    groups = num_ref[0]

    def entry(g, j):
        v = lst_ref[g * GROUP + j]
        slot = lax.shift_right_logical(v, 9)
        return lax.shift_right_logical(slot, 3), slot & (KMAX - 1), v & 511

    def weight_copy(g, j):
        t, k, _ = entry(g, j)
        return pltpu.make_async_copy(w_hbm.at[t, k], wbuf.at[g * GROUP + j], wsem.at[g])

    def issue(g, carry):
        for j in range(GROUP):
            weight_copy(g, j).start()
        return carry

    lax.fori_loop(0, groups, issue, 0)
    out_ref[...] = part_ref[...]
    src[FAR + 2 * E] = jnp.zeros((C, C), src.dtype)
    for copy in copies:
        copy.wait()

    def work(g, carry):
        for j in range(GROUP):
            weight_copy(g, j).wait()
        got = []
        for j in range(GROUP):
            t, _, s = entry(g, j)
            got.append(
                (t, lax.dot_general(src[s], wbuf[g * GROUP + j], NT, preferred_element_type=jnp.float32))
            )
        for t, d in got:
            out_ref[t] = out_ref[t] + d
        return carry

    lax.fori_loop(0, groups, work, 0)

    def add_up(t, acc):
        return acc + area_ref[t] * out_ref[t]

    acc = lax.fori_loop(0, ROWS, add_up, jnp.zeros((C, C), jnp.float32), unroll=4)
    mass_ref[...] = lax.dot_general(
        jnp.ones((8, C), jnp.float32), acc, NT,
        precision=lax.Precision.HIGHEST, preferred_element_type=jnp.float32,
    )


def far_call(lst, num, area, weights, parts, partial):
    smem = pl.BlockSpec(memory_space=pltpu.SMEM)
    hbm = pl.BlockSpec(memory_space=pltpu.HBM)
    vmem = pl.BlockSpec(memory_space=pltpu.VMEM)
    return pl.pallas_call(
        far_kernel,
        in_specs=[smem, smem, smem, hbm] + [hbm] * len(parts) + [vmem],
        out_specs=[vmem, vmem],
        out_shape=[
            jax.ShapeDtypeStruct((ROWS, C, C), jnp.float32),
            jax.ShapeDtypeStruct((8, C), jnp.float32),
        ],
        scratch_shapes=[
            pltpu.VMEM((FAR + 2 * E + 1, C, C), jnp.bfloat16),
            pltpu.VMEM((ROWS * KMAX, C, C), jnp.bfloat16),
            pltpu.SemaphoreType.DMA((12,)),
            pltpu.SemaphoreType.DMA((ROWS * KMAX // GROUP,)),
        ],
        compiler_params=pltpu.CompilerParams(vmem_limit_bytes=40 << 20),
        cost_estimate=pl.CostEstimate(
            flops=2 * ROWS * KMAX * C**3 // 2, bytes_accessed=20 << 20, transcendentals=0
        ),
        name="far",
    )(lst, num, area, weights, *parts, partial)


def latitude_area(first_row, count_rows):
    rows_all = jnp.arange(count_rows, dtype=jnp.int32) + first_row
    angle = -0.5 * math.pi + (rows_all.astype(jnp.float32) + 0.5) * (math.pi / NLAT)
    return jnp.cos(angle)


def slots(source_row, source_block, slot_count, lat, lon):
    row = source_row[:, 0, :].T - (lat * ROWS - R)
    row = jnp.clip(row, 0, PAD - 1)
    rel = (source_block[:, 0, :].T - lon + 3) % NLON_DEV - 3
    active = jnp.arange(KMAX, dtype=jnp.int32)[:, None] < slot_count[:, 0][None, :]
    size = jnp.abs(rel)
    side = (rel > 0).astype(jnp.int32)
    is_near = active & (size <= 1)
    near = jnp.where(is_near, jnp.where(rel == 0, 0, side + 1) * PAD + row, 3 * PAD)
    polar_row = jnp.clip(jnp.where(lat == 0, row - R, row - R - (ROWS - E)), 0, E - 1)
    far = jnp.where(size >= 3, FAR + side * E + polar_row, side * PAD + row)
    is_far = active & (size >= 2)
    target = jnp.arange(ROWS, dtype=jnp.int32)[None, :]
    slot = target * KMAX + jnp.arange(KMAX, dtype=jnp.int32)[:, None]
    order = jnp.where(is_far, slot, ROWS * KMAX + slot)
    zero = FAR + 2 * E
    packed = (order * 512 + jnp.where(is_far, far, zero)).reshape(-1)
    packed = jnp.sort(packed) & (ROWS * KMAX * 512 - 1)
    groups = (jnp.sum(is_far.astype(jnp.int32)) + GROUP - 1) // GROUP
    return near.astype(jnp.int32), packed.astype(jnp.int32), groups.reshape(1)


def everywhere(tracers, weights, source_row, source_block, slot_count):
    lat, lon = lax.axis_index("lat"), lax.axis_index("lon")
    q = tracers.transpose(0, 2, 3, 1).reshape(ROWS, C, C)
    qe = jnp.concatenate([q[:E], q[ROWS - E :]], axis=0)
    qm = q[E : ROWS - E]
    le, re = (lax.ppermute(qe, "lon", ring(1)), lax.ppermute(qe, "lon", ring(-1)))
    lm, rm = (lax.ppermute(qm, "lon", ring(1)), lax.ppermute(qm, "lon", ring(-1)))
    near_idx, far_list, far_groups = slots(source_row, source_block, slot_count, lat, lon)
    area = latitude_area(lat * ROWS, ROWS)
    total_area = C * NLON_DEV * jnp.sum(latitude_area(0, NLAT))
    mass_old = jnp.sum(area[:, None, None] * q.astype(jnp.float32), axis=(0, 2))

    up1 = lax.ppermute(jnp.concatenate([v[2 * E - R :] for v in (qe, le, re)], axis=0), "lat", UP)
    dn1 = lax.ppermute(jnp.concatenate([v[:R] for v in (qe, le, re)], axis=0), "lat", DOWN)
    lle, rre = (lax.ppermute(le, "lon", ring(1)), lax.ppermute(re, "lon", ring(-1)))
    llm, rrm = (lax.ppermute(lm, "lon", ring(1)), lax.ppermute(rm, "lon", ring(-1)))
    up2 = lax.ppermute(jnp.concatenate([v[2 * E - R :] for v in (lle, rre)], axis=0), "lat", UP)
    dn2 = lax.ppermute(jnp.concatenate([v[:R] for v in (lle, rre)], axis=0), "lat", DOWN)
    pole = [jnp.where(lat == 0, v[:E], v[E:]) for v in (lle, rre)]
    l3 = lax.ppermute(pole[0], ("lat", "lon"), polar(1))
    r3 = lax.ppermute(pole[1], ("lat", "lon"), polar(-1))

    w = weights[:, 0]
    partial = near_call(near_idx, w, (q, le, lm, re, rm, up1, dn1))
    advected, mass_new = far_call(
        far_list, far_groups, area, w, (lle, llm, rre, rrm, up2, dn2, l3, r3), partial
    )
    change = lax.psum(mass_old - mass_new[0], ("lat", "lon"))
    fixed = advected + (change / total_area)[None, :, None]
    return fixed


TOTAL_AREA = C * NLON_DEV * math.fsum(
    math.cos(-0.5 * math.pi + (j + 0.5) * math.pi / NLAT) for j in range(NLAT)
)
EDGE = 16
S = 2 * EDGE
M = ROWS - S
B = 16
SIDE = S + R + M + B + R
FAR2 = 2 * SIDE
SECT = 7 * PAD
CHUNKS = 4
PER = ROWS // CHUNKS
POLAR, NEXT = ((0, NLAT_DEV - 1), (1, NLAT_DEV - 2))


def some(by, lats):
    return [
        (a * NLON_DEV + i, a * NLON_DEV + (i + by) % NLON_DEV) for a in lats for i in range(NLON_DEV)
    ]


WC = 16
WT = ROWS // WC


def sums_kernel(idx_ref, area_ref, lost_ref, w_hbm, *refs):
    wv, left, right, own, acc, sem = refs

    def copy(c):
        rows = pl.ds(c * WT, WT)
        return pltpu.make_async_copy(w_hbm.at[rows], wv.at[rows], sem.at[c])

    def start(c, carry):
        copy(c).start()
        return carry

    lax.fori_loop(0, WC, start, 0)
    acc[...] = jnp.zeros(acc.shape, acc.dtype)

    def work(c, carry):
        copy(c).wait()
        for j in range(WT):
            t = c * WT + j
            for k in range(KMAX):
                part = jnp.sum(wv[t, k].astype(jnp.float32).reshape(C // 8, 8, C), axis=0)
                at = idx_ref[k, t]
                acc[at] = acc[at] + area_ref[t] * part
        return carry

    lax.fori_loop(0, WC, work, 0)

    def summed(rel):
        at = (rel + 3) * PAD
        return jnp.sum(acc[at : at + PAD], axis=1)

    left[:PAD] = summed(-1)
    left[PAD:] = summed(-2)
    right[:PAD] = summed(1)
    right[PAD:] = summed(2)
    own[:PAD] = summed(0)
    own[PAD : 2 * PAD] = summed(-3)
    own[2 * PAD : 3 * PAD] = summed(3)
    own[3 * PAD :] = jnp.full((8, C), lost_ref[0])


def sums_call(idx, area, lost, weights):
    smem = pl.BlockSpec(memory_space=pltpu.SMEM)
    vmem = pl.BlockSpec(memory_space=pltpu.VMEM)
    return pl.pallas_call(
        sums_kernel,
        in_specs=[smem, smem, smem, pl.BlockSpec(memory_space=pltpu.HBM)],
        out_specs=[vmem] * 4,
        out_shape=[pltpu.VMEM(weights.shape, weights.dtype)]
        + [jax.ShapeDtypeStruct((n, C), jnp.float32) for n in (2 * PAD, 2 * PAD, 3 * PAD + 8)],
        scratch_shapes=[
            pltpu.VMEM((SECT + 1, 8, C), jnp.float32),
            pltpu.SemaphoreType.DMA((WC,)),
        ],
        compiler_params=pltpu.CompilerParams(vmem_limit_bytes=6 << 20),
        cost_estimate=pl.CostEstimate(
            flops=20_000_000, bytes_accessed=17 << 20, transcendentals=0
        ),
        name="sums",
    )(idx, area, lost, pltpu.with_memory_space_constraint(weights, pltpu.HBM))


def rows_kernel(ranges, q_hbm, out, sem):
    copies = [
        pltpu.make_async_copy(q_hbm.at[pl.ds(at, n)], out.at[pl.ds(to, n)], sem.at[i])
        for i, (at, n, to) in enumerate(ranges)
    ]
    for copy in copies:
        copy.start()
    for copy in copies:
        copy.wait()


def rows_call(ranges, q):
    count = sum(n for _, n, _ in ranges)
    return pl.pallas_call(
        functools.partial(rows_kernel, ranges),
        in_specs=[pl.BlockSpec(memory_space=pltpu.HBM)],
        out_specs=pl.BlockSpec(memory_space=pltpu.VMEM),
        out_shape=pltpu.VMEM((count, C, C), jnp.bfloat16),
        scratch_shapes=[pltpu.SemaphoreType.DMA((len(ranges),))],
        compiler_params=pltpu.CompilerParams(vmem_limit_bytes=1 << 20),
        cost_estimate=pl.CostEstimate(flops=1000, bytes_accessed=1 << 20, transcendentals=0),
    )(pltpu.with_memory_space_constraint(q, pltpu.HBM))


def pack_kernel(qs, ls, rs, up, dn):
    for n, v in enumerate((qs, ls, rs)):
        up[pl.ds(n * R, R)] = v[S - R :]
        dn[pl.ds(n * R, R)] = v[:R]


def pack_call(parts):
    vmem = pl.BlockSpec(memory_space=pltpu.VMEM)
    return pl.pallas_call(
        pack_kernel,
        in_specs=[vmem] * 3,
        out_specs=[vmem, vmem],
        out_shape=[pltpu.VMEM((3 * R, C, C), jnp.bfloat16)] * 2,
        compiler_params=pltpu.CompilerParams(vmem_limit_bytes=6 << 20),
        cost_estimate=pl.CostEstimate(flops=1000, bytes_accessed=1000, transcendentals=0),
        name="pack",
    )(*parts)


def mass_kernel(area_ref, at_ref, c0, cl, cr, qs, qm, ls, lm, rs, rm, up, dn, l3, r3, out_ref, src, by):
    for n, (e, m) in enumerate(((qs, qm), (ls, lm), (rs, rm))):
        at = n * PAD + R
        src[pl.ds(at, EDGE)] = e[:EDGE]
        src[pl.ds(at + EDGE, M)] = m[...]
        src[pl.ds(at + EDGE + M, EDGE)] = e[EDGE:]
    for n in range(3):
        src[pl.ds(n * PAD, R)] = up[pl.ds(n * R, R)]
        src[pl.ds(n * PAD + R + ROWS, R)] = dn[pl.ds(n * R, R)]
    src[3 * PAD] = jnp.zeros((C, C), src.dtype)
    by[:PAD] = (c0[:PAD] + cl[:PAD]) + cr[:PAD]
    by[PAD : 2 * PAD] = cl[PAD:]
    by[2 * PAD :] = cr[PAD:]
    for r in range(ROWS):
        by[R + r : R + r + 1] = by[R + r : R + r + 1] - area_ref[r]

    def body(p, acc):
        return acc + by[pl.ds(p, 1)] * src[p].astype(jnp.float32)

    acc = lax.fori_loop(0, 3 * PAD, body, jnp.zeros((C, C), jnp.float32), unroll=8)
    at = at_ref[0]
    for i in range(E):
        acc = acc + c0[pl.ds(PAD + at + i, 1)] * l3[i].astype(jnp.float32)
        acc = acc + c0[pl.ds(2 * PAD + at + i, 1)] * r3[i].astype(jnp.float32)
    change = lax.dot_general(
        jnp.full((8, C), -1.0, jnp.float32), acc, NT,
        precision=lax.Precision.HIGHEST, preferred_element_type=jnp.float32,
    )
    row = lax.broadcasted_iota(jnp.int32, (8, C), 0)
    out_ref[...] = jnp.where(row == 0, change, c0[3 * PAD :])


def mass_call(area, at, parts):
    smem = pl.BlockSpec(memory_space=pltpu.SMEM)
    vmem = pl.BlockSpec(memory_space=pltpu.VMEM)
    return pl.pallas_call(
        mass_kernel,
        in_specs=[smem] * 2 + [vmem] * len(parts),
        out_specs=[vmem] * 2,
        out_shape=[
            jax.ShapeDtypeStruct((8, C), jnp.float32),
            pltpu.VMEM((3 * PAD + 1, C, C), jnp.bfloat16),
        ],
        scratch_shapes=[
            pltpu.VMEM((3 * PAD, C), jnp.float32),
        ],
        compiler_params=pltpu.CompilerParams(vmem_limit_bytes=6 << 20),
        cost_estimate=pl.CostEstimate(
            flops=9_000_000, bytes_accessed=3 << 20, transcendentals=0
        ),
        name="mass",
    )(area, at, *parts)


def inner_kernel(first, idx_ref, wv, src, out_ref):
    def body(j, carry):
        t = first + j
        lhs = jnp.concatenate([src[idx_ref[k, t]] for k in range(KMAX)], axis=1)
        rhs = jnp.concatenate([wv[t, k] for k in range(KMAX)], axis=1)
        out_ref[j] = lax.dot_general(lhs, rhs, NT, preferred_element_type=jnp.float32)
        return carry

    lax.fori_loop(0, PER, body, 0, unroll=8)


def inner_call(chunk, idx, wv, near):
    vmem = pl.BlockSpec(memory_space=pltpu.VMEM)
    return pl.pallas_call(
        functools.partial(inner_kernel, chunk * PER),
        in_specs=[pl.BlockSpec(memory_space=pltpu.SMEM), vmem, vmem],
        out_specs=vmem,
        out_shape=pltpu.VMEM((PER, C, C), jnp.float32),
        compiler_params=pltpu.CompilerParams(vmem_limit_bytes=2 << 20),
        cost_estimate=pl.CostEstimate(
            flops=2 * PER * KMAX * C**3, bytes_accessed=1 << 20, transcendentals=0
        ),
    )(idx, wv, near)


HALF = CHUNKS // 2


def far_part(half, idx_ref, wv, src, partial, out_ref):
    for c in range(HALF):

        def body(j, carry):
            t = (half * HALF + c) * PER + j
            lhs = jnp.concatenate([src[idx_ref[k, t]] for k in range(KMAX)], axis=1)
            rhs = jnp.concatenate([wv[t, k] for k in range(KMAX)], axis=1)
            got = lax.dot_general(lhs, rhs, NT, preferred_element_type=jnp.float32)
            out_ref[c * PER + j] = got + partial[c][j]
            return carry

        lax.fori_loop(0, PER, body, 0, unroll=8)


def outer0_kernel(idx_ref, wv, ls, lm, lb, rs, rm, rb, l3, r3, *refs):
    partial, (out_ref, src) = refs[:HALF], refs[HALF:]
    for n, (e, m, b) in enumerate(((ls, lm, lb), (rs, rm, rb))):
        at = n * SIDE
        src[pl.ds(at, S + R)] = e[...]
        src[pl.ds(at + S + R, M)] = m[...]
        src[pl.ds(at + S + R + M, B + R)] = b[...]
    src[pl.ds(FAR2, E)] = l3[...]
    src[pl.ds(FAR2 + E, E)] = r3[...]
    src[FAR2 + 2 * E] = jnp.zeros((C, C), src.dtype)
    far_part(0, idx_ref, wv, src, partial, out_ref)


def outer1_kernel(idx_ref, wv, src, *refs):
    far_part(1, idx_ref, wv, src, refs[:HALF], refs[HALF])


def outer_call(half, idx, wv, parts, partial):
    vmem = pl.BlockSpec(memory_space=pltpu.VMEM)
    out_shape = [pltpu.VMEM((HALF * PER, C, C), jnp.float32)]
    if half == 0:
        out_shape.append(pltpu.VMEM((FAR2 + 2 * E + 1, C, C), jnp.bfloat16))
    return pl.pallas_call(
        (outer0_kernel, outer1_kernel)[half],
        in_specs=[pl.BlockSpec(memory_space=pltpu.SMEM)]
        + [vmem] * (1 + len(parts) + len(partial)),
        out_specs=[vmem] * len(out_shape),
        out_shape=out_shape,
        compiler_params=pltpu.CompilerParams(vmem_limit_bytes=8 << 20),
        cost_estimate=pl.CostEstimate(
            flops=2 * HALF * PER * KMAX * C**3, bytes_accessed=1 << 20, transcendentals=0
        ),
    )(idx, wv, *parts, *partial)


WRITES = 8


def write_kernel(corr_ref, a_ref, b_ref, out_hbm, buf, sem):
    rows = ROWS // WRITES

    def copy(c):
        at = pl.ds(c * rows, rows)
        return pltpu.make_async_copy(buf.at[at], out_hbm.at[at], sem.at[c])

    for c in range(WRITES):
        ref = a_ref if c < WRITES // 2 else b_ref
        for i in range(rows):
            t = c * rows + i
            buf[t] = ref[t % (ROWS // 2)] + corr_ref[...]
        copy(c).start()
    for c in range(WRITES):
        copy(c).wait()


def write_call(corr, first, second):
    vmem = pl.BlockSpec(memory_space=pltpu.VMEM)
    return pl.pallas_call(
        write_kernel,
        in_specs=[vmem] * 3,
        out_specs=pl.BlockSpec(memory_space=pltpu.HBM),
        out_shape=jax.ShapeDtypeStruct((ROWS, C, C), jnp.float32),
        scratch_shapes=[
            pltpu.VMEM((ROWS, C, C), jnp.float32),
            pltpu.SemaphoreType.DMA((WRITES,)),
        ],
        compiler_params=pltpu.CompilerParams(vmem_limit_bytes=6 << 20),
        cost_estimate=pl.CostEstimate(
            flops=1_000_000, bytes_accessed=4 << 20, transcendentals=0
        ),
        name="write",
    )(corr, first, second)


def tables(source_row, source_block, slot_count, lat, lon):
    p = source_row[:, 0, :].T - (lat * ROWS - R)
    p = jnp.clip(p, 0, PAD - 1)
    rel = (source_block[:, 0, :].T - lon + 3) % NLON_DEV - 3
    rel = jnp.clip(rel, -3, 3)
    active = jnp.arange(KMAX, dtype=jnp.int32)[:, None] < slot_count[:, 0][None, :]
    sums_idx = jnp.where(active, (rel + 3) * PAD + p, SECT)
    size = jnp.abs(rel)
    side = (rel > 0).astype(jnp.int32)
    near_idx = jnp.where(
        active & (size <= 1), jnp.where(rel == 0, 0, side + 1) * PAD + p, 3 * PAD
    )
    r = p - R
    is_polar = (lat == 0) | (lat == NLAT_DEV - 1)
    in_band = jnp.where(r < EDGE, r, jnp.where(r < EDGE + M, r - EDGE + S + R, r - M))
    below = lat == NLAT_DEV - 2
    in_next = S + R + M + jnp.where(below, r - (ROWS - B), r)
    halo = jnp.where(is_polar, S, S + R + M + B) + jnp.where(r < 0, r + R, r - ROWS)
    two = jnp.where((r < 0) | (r >= ROWS), halo, jnp.where(is_polar, in_band, in_next))
    polar_row = jnp.clip(jnp.where(lat == 0, r, r - (ROWS - E)), 0, E - 1)
    far = jnp.where(size >= 3, FAR2 + side * E + polar_row, side * SIDE + two)
    is_far = active & (size >= 2)
    held = is_polar | ((lat == 1) & (r < B)) | (below & (r >= ROWS - B))
    lost = jnp.sum((is_far & ~held).astype(jnp.float32))
    far_idx = jnp.where(is_far & held, far, FAR2 + 2 * E)
    return sums_idx, near_idx, far_idx, lost


def swap(v, axis, size, to):
    return lax.ppermute(v, axis, [(i, to(i)) for i in range(size)])


def three(v, axis, size, to):
    got = [swap(v, axis, size, functools.partial(to, by=by)) for by in (1, 2, 3)]
    return (got[0] + got[2]) + got[1]


def local(tracers, weights, source_row, source_block, slot_count):
    args = (tracers, weights, source_row, source_block, slot_count)
    lost, fixed = usual(*args)

    def redo(state):
        return jnp.zeros_like(state[0]), everywhere(*args)

    _, fixed = lax.while_loop(lambda state: state[0] > 0, redo, (lost, fixed))
    return fixed.reshape(ROWS, 32, 4, C).transpose(0, 3, 1, 2)


def usual(tracers, weights, source_row, source_block, slot_count):
    lat, lon = lax.axis_index("lat"), lax.axis_index("lon")
    both = ("lat", "lon")
    w = weights[:, 0]
    q = tracers.transpose(0, 2, 3, 1).reshape(ROWS, C, C)
    qs = rows_call(((0, EDGE, 0), (ROWS - EDGE, EDGE, EDGE)), q)
    qm = rows_call(((EDGE, M, 0),), q)
    ls, rs = lax.ppermute(qs, "lon", ring(1)), lax.ppermute(qs, "lon", ring(-1))
    lm, rm = lax.ppermute(qm, "lon", ring(1)), lax.ppermute(qm, "lon", ring(-1))
    pole = jnp.where(lat == 0, qs[:E], qs[S - E :])
    l3 = lax.ppermute(pole, both, some(3, POLAR))
    r3 = lax.ppermute(pole, both, some(-3, POLAR))
    sums_idx, near_idx, far_idx, lost = tables(source_row, source_block, slot_count, lat, lon)
    area = latitude_area(lat * ROWS, ROWS)
    wv, to_left, to_right, own_sums = sums_call(sums_idx, area, lost.reshape(1), w)
    cl = lax.ppermute(to_left, "lon", ring(-1))
    cr = lax.ppermute(to_right, "lon", ring(1))
    first, last = pack_call((qs, ls, rs))
    up1, dn1 = lax.ppermute(first, "lat", UP), lax.ppermute(last, "lat", DOWN)
    at = jnp.where(jnp.arange(NLAT_DEV, dtype=jnp.int32) == lat, R, R + ROWS - E).astype(jnp.int32)
    v, near = mass_call(
        area, at,
        (own_sums, cl, cr, qs, qm, ls, lm, rs, rm, up1, dn1, l3, r3),
    )
    held = lambda x: pltpu.with_memory_space_constraint(x, pltpu.VMEM)
    near, wv = held(near), held(wv)
    v = v + swap(v, "lat", NLAT_DEV, lambda i: i ^ 1)
    v = v + three(v, "lat", NLAT_DEV, lambda i, by: (i + 2 * by) % NLAT_DEV)
    v = v + three(v, "lon", NLON_DEV, lambda i, by: (i + 4 * by) % NLON_DEV)
    v = v + three(v, "lon", NLON_DEV, lambda i, by: i // 4 * 4 + (i + by) % 4)
    corr = jnp.broadcast_to((v[0] * (1.0 / TOTAL_AREA))[:, None], (C, C))

    beyond = jnp.where(lat == 0, dn1[R:], jnp.where(lat == NLAT_DEV - 2, dn1[R:], up1[R:]))
    sides = ((ls, beyond[:R], 1), (rs, beyond[R:], -1))
    lls, rrs = (
        lax.ppermute(jnp.concatenate([x, h], axis=0), both, some(d, POLAR)) for x, h, d in sides
    )
    llb, rrb = (
        lax.ppermute(
            jnp.concatenate([jnp.where(lat == 1, x[:B], x[S - B :]), h], axis=0),
            both, some(d, NEXT),
        )
        for x, h, d in sides
    )
    llm, rrm = (lax.ppermute(x, both, some(d, POLAR)) for x, d in ((lm, 1), (rm, -1)))

    partial = [held(inner_call(c, near_idx, wv, near)) for c in range(CHUNKS)]
    first, src = outer_call(
        0, far_idx, wv, (lls, llm, llb, rrs, rrm, rrb, l3, r3), partial[:HALF]
    )
    (second,) = outer_call(1, far_idx, wv, (held(src),), partial[HALF:])
    fixed = write_call(corr, held(first), held(second))
    return v[1, 0], fixed


def solution(mesh):
    placed = (
        P("lat", "lon", None, None),
        P("lat", "lon", None, None, None),
        P("lat", "lon", None),
        P("lat", "lon", None),
        P("lat", "lon"),
    )
    return jax.shard_map(
        local, mesh=mesh, in_specs=placed, out_specs=P("lat", "lon", None, None), check_vma=False
    )
```

```python
import functools
import math

import jax
import jax.numpy as jnp
from jax import lax
from jax.experimental import pallas as pl
from jax.experimental.pallas import tpu as pltpu
from jax.sharding import PartitionSpec as P

ROWS = 64
C = 128
KMAX = 8
R = 4
E = R + 1
MID = ROWS - 2 * E
PAD = ROWS + 2 * R
NLAT, NLON_DEV, NLAT_DEV = 512, 16, 8
TB = 4
FAR = 2 * PAD
NT = (((1,), (1,)), ((), ()))


def ring(by):
    return [(i, (i + by) % NLON_DEV) for i in range(NLON_DEV)]


UP = [(i, i + 1) for i in range(NLAT_DEV - 1)]
DOWN = [(i + 1, i) for i in range(NLAT_DEV - 1)]


def polar(by):
    return [
        (a * NLON_DEV + i, a * NLON_DEV + (i + by) % NLON_DEV)
        for a in (0, NLAT_DEV - 1)
        for i in range(NLON_DEV)
    ]


def near_kernel(idx_ref, w_ref, *refs):
    parts, (out_ref, src, sem) = refs[:-3], refs[-3:]
    step = pl.program_id(0)
    own, le, lm, re, rm, up, dn = parts

    def copies():
        todo = [(own, 0, ROWS, 0 * PAD + R)]
        for n, (e, m) in enumerate(((le, lm), (re, rm))):
            at = (n + 1) * PAD + R
            todo.append((e, 0, E, at))
            todo.append((m, 0, MID, at + E))
            todo.append((e, E, E, at + E + MID))
        for n in range(3):
            todo.append((up, n * R, R, n * PAD))
            todo.append((dn, n * R, R, n * PAD + R + ROWS))
        return [
            pltpu.make_async_copy(ref.at[pl.ds(a, n)], src.at[pl.ds(to, n)], sem.at[i])
            for i, (ref, a, n, to) in enumerate(todo)
        ]

    @pl.when(step == 0)
    def _():
        for copy in copies():
            copy.start()
        src[3 * PAD] = jnp.zeros((C, C), src.dtype)
        for copy in copies():
            copy.wait()

    for j in range(TB):
        t = step * TB + j
        lhs = jnp.concatenate([src[idx_ref[k, t]] for k in range(KMAX)], axis=1)
        rhs = jnp.concatenate([w_ref[j, k] for k in range(KMAX)], axis=1)
        out_ref[j] = lax.dot_general(lhs, rhs, NT, preferred_element_type=jnp.float32)


def near_call(idx, weights, parts):
    n_copies = 7 + 6
    return pl.pallas_call(
        near_kernel,
        grid_spec=pltpu.PrefetchScalarGridSpec(
            num_scalar_prefetch=1,
            grid=(ROWS // TB,),
            in_specs=[pl.BlockSpec((TB, KMAX, C, C), lambda s, i: (s, 0, 0, 0))]
            + [pl.BlockSpec(memory_space=pltpu.HBM)] * len(parts),
            out_specs=pl.BlockSpec((TB, C, C), lambda s, i: (s, 0, 0)),
            scratch_shapes=[
                pltpu.VMEM((3 * PAD + 1, C, C), jnp.bfloat16),
                pltpu.SemaphoreType.DMA((n_copies,)),
            ],
        ),
        out_shape=jax.ShapeDtypeStruct((ROWS, C, C), jnp.float32),
        compiler_params=pltpu.CompilerParams(
            dimension_semantics=("arbitrary",), vmem_limit_bytes=20 << 20
        ),
        cost_estimate=pl.CostEstimate(
            flops=2 * ROWS * KMAX * C**3, bytes_accessed=28 << 20, transcendentals=0
        ),
        name="near",
    )(idx, weights, *parts)


GROUP = 8


def far_kernel(lst_ref, num_ref, area_ref, w_hbm, le, lm, re, rm, up, dn, l3, r3, part_ref, out_ref, mass_ref, src, wbuf, sem, wsem):
    todo = []
    for n, (e, m) in enumerate(((le, lm), (re, rm))):
        at = n * PAD + R
        todo.append((e, 0, E, at))
        todo.append((m, 0, MID, at + E))
        todo.append((e, E, E, at + E + MID))
        todo.append((up, n * R, R, n * PAD))
        todo.append((dn, n * R, R, n * PAD + R + ROWS))
    todo.append((l3, 0, E, FAR))
    todo.append((r3, 0, E, FAR + E))
    copies = [
        pltpu.make_async_copy(ref.at[pl.ds(a, n)], src.at[pl.ds(to, n)], sem.at[i])
        for i, (ref, a, n, to) in enumerate(todo)
    ]
    for copy in copies:
        copy.start()
    groups = num_ref[0]

    def entry(g, j):
        v = lst_ref[g * GROUP + j]
        slot = lax.shift_right_logical(v, 9)
        return lax.shift_right_logical(slot, 3), slot & (KMAX - 1), v & 511

    def weight_copy(g, j):
        t, k, _ = entry(g, j)
        return pltpu.make_async_copy(w_hbm.at[t, k], wbuf.at[g * GROUP + j], wsem.at[g])

    def issue(g, carry):
        for j in range(GROUP):
            weight_copy(g, j).start()
        return carry

    lax.fori_loop(0, groups, issue, 0)
    out_ref[...] = part_ref[...]
    src[FAR + 2 * E] = jnp.zeros((C, C), src.dtype)
    for copy in copies:
        copy.wait()

    def work(g, carry):
        for j in range(GROUP):
            weight_copy(g, j).wait()
        got = []
        for j in range(GROUP):
            t, _, s = entry(g, j)
            got.append(
                (t, lax.dot_general(src[s], wbuf[g * GROUP + j], NT, preferred_element_type=jnp.float32))
            )
        for t, d in got:
            out_ref[t] = out_ref[t] + d
        return carry

    lax.fori_loop(0, groups, work, 0)

    def add_up(t, acc):
        return acc + area_ref[t] * out_ref[t]

    acc = lax.fori_loop(0, ROWS, add_up, jnp.zeros((C, C), jnp.float32), unroll=4)
    mass_ref[...] = lax.dot_general(
        jnp.ones((8, C), jnp.float32), acc, NT,
        precision=lax.Precision.HIGHEST, preferred_element_type=jnp.float32,
    )


def far_call(lst, num, area, weights, parts, partial):
    smem = pl.BlockSpec(memory_space=pltpu.SMEM)
    hbm = pl.BlockSpec(memory_space=pltpu.HBM)
    vmem = pl.BlockSpec(memory_space=pltpu.VMEM)
    return pl.pallas_call(
        far_kernel,
        in_specs=[smem, smem, smem, hbm] + [hbm] * len(parts) + [vmem],
        out_specs=[vmem, vmem],
        out_shape=[
            jax.ShapeDtypeStruct((ROWS, C, C), jnp.float32),
            jax.ShapeDtypeStruct((8, C), jnp.float32),
        ],
        scratch_shapes=[
            pltpu.VMEM((FAR + 2 * E + 1, C, C), jnp.bfloat16),
            pltpu.VMEM((ROWS * KMAX, C, C), jnp.bfloat16),
            pltpu.SemaphoreType.DMA((12,)),
            pltpu.SemaphoreType.DMA((ROWS * KMAX // GROUP,)),
        ],
        compiler_params=pltpu.CompilerParams(vmem_limit_bytes=40 << 20),
        cost_estimate=pl.CostEstimate(
            flops=2 * ROWS * KMAX * C**3 // 2, bytes_accessed=20 << 20, transcendentals=0
        ),
        name="far",
    )(lst, num, area, weights, *parts, partial)


def latitude_area(first_row, count_rows):
    rows_all = jnp.arange(count_rows, dtype=jnp.int32) + first_row
    angle = -0.5 * math.pi + (rows_all.astype(jnp.float32) + 0.5) * (math.pi / NLAT)
    return jnp.cos(angle)


def slots(source_row, source_block, slot_count, lat, lon):
    row = source_row[:, 0, :].T - (lat * ROWS - R)
    row = jnp.clip(row, 0, PAD - 1)
    rel = (source_block[:, 0, :].T - lon + 3) % NLON_DEV - 3
    active = jnp.arange(KMAX, dtype=jnp.int32)[:, None] < slot_count[:, 0][None, :]
    size = jnp.abs(rel)
    side = (rel > 0).astype(jnp.int32)
    is_near = active & (size <= 1)
    near = jnp.where(is_near, jnp.where(rel == 0, 0, side + 1) * PAD + row, 3 * PAD)
    polar_row = jnp.clip(jnp.where(lat == 0, row - R, row - R - (ROWS - E)), 0, E - 1)
    far = jnp.where(size >= 3, FAR + side * E + polar_row, side * PAD + row)
    is_far = active & (size >= 2)
    target = jnp.arange(ROWS, dtype=jnp.int32)[None, :]
    slot = target * KMAX + jnp.arange(KMAX, dtype=jnp.int32)[:, None]
    order = jnp.where(is_far, slot, ROWS * KMAX + slot)
    zero = FAR + 2 * E
    packed = (order * 512 + jnp.where(is_far, far, zero)).reshape(-1)
    packed = jnp.sort(packed) & (ROWS * KMAX * 512 - 1)
    groups = (jnp.sum(is_far.astype(jnp.int32)) + GROUP - 1) // GROUP
    return near.astype(jnp.int32), packed.astype(jnp.int32), groups.reshape(1)


def everywhere(tracers, weights, source_row, source_block, slot_count):
    lat, lon = lax.axis_index("lat"), lax.axis_index("lon")
    q = tracers.transpose(0, 2, 3, 1).reshape(ROWS, C, C)
    qe = jnp.concatenate([q[:E], q[ROWS - E :]], axis=0)
    qm = q[E : ROWS - E]
    le, re = (lax.ppermute(qe, "lon", ring(1)), lax.ppermute(qe, "lon", ring(-1)))
    lm, rm = (lax.ppermute(qm, "lon", ring(1)), lax.ppermute(qm, "lon", ring(-1)))
    near_idx, far_list, far_groups = slots(source_row, source_block, slot_count, lat, lon)
    area = latitude_area(lat * ROWS, ROWS)
    total_area = C * NLON_DEV * jnp.sum(latitude_area(0, NLAT))
    mass_old = jnp.sum(area[:, None, None] * q.astype(jnp.float32), axis=(0, 2))

    up1 = lax.ppermute(jnp.concatenate([v[2 * E - R :] for v in (qe, le, re)], axis=0), "lat", UP)
    dn1 = lax.ppermute(jnp.concatenate([v[:R] for v in (qe, le, re)], axis=0), "lat", DOWN)
    lle, rre = (lax.ppermute(le, "lon", ring(1)), lax.ppermute(re, "lon", ring(-1)))
    llm, rrm = (lax.ppermute(lm, "lon", ring(1)), lax.ppermute(rm, "lon", ring(-1)))
    up2 = lax.ppermute(jnp.concatenate([v[2 * E - R :] for v in (lle, rre)], axis=0), "lat", UP)
    dn2 = lax.ppermute(jnp.concatenate([v[:R] for v in (lle, rre)], axis=0), "lat", DOWN)
    pole = [jnp.where(lat == 0, v[:E], v[E:]) for v in (lle, rre)]
    l3 = lax.ppermute(pole[0], ("lat", "lon"), polar(1))
    r3 = lax.ppermute(pole[1], ("lat", "lon"), polar(-1))

    w = weights[:, 0]
    partial = near_call(near_idx, w, (q, le, lm, re, rm, up1, dn1))
    advected, mass_new = far_call(
        far_list, far_groups, area, w, (lle, llm, rre, rrm, up2, dn2, l3, r3), partial
    )
    change = lax.psum(mass_old - mass_new[0], ("lat", "lon"))
    fixed = advected + (change / total_area)[None, :, None]
    return fixed


TOTAL_AREA = C * NLON_DEV * math.fsum(
    math.cos(-0.5 * math.pi + (j + 0.5) * math.pi / NLAT) for j in range(NLAT)
)
EDGE = 16
S = 2 * EDGE
M = ROWS - S
B = 16
SIDE = S + R + M + B + R
FAR2 = 2 * SIDE
SECT = 7 * PAD
CHUNKS = 4
PER = ROWS // CHUNKS
POLAR, NEXT = ((0, NLAT_DEV - 1), (1, NLAT_DEV - 2))


def some(by, lats):
    return [
        (a * NLON_DEV + i, a * NLON_DEV + (i + by) % NLON_DEV) for a in lats for i in range(NLON_DEV)
    ]


WC = 16
WT = ROWS // WC


def sums_kernel(idx_ref, area_ref, w_hbm, *refs):
    wv, left, right, own, acc, sem = refs

    def copy(c):
        rows = pl.ds(c * WT, WT)
        return pltpu.make_async_copy(w_hbm.at[rows], wv.at[rows], sem.at[c])

    def start(c, carry):
        copy(c).start()
        return carry

    lax.fori_loop(0, WC, start, 0)
    acc[...] = jnp.zeros(acc.shape, acc.dtype)

    def work(c, carry):
        copy(c).wait()
        for j in range(WT):
            t = c * WT + j
            for k in range(KMAX):
                part = jnp.sum(wv[t, k].astype(jnp.float32).reshape(C // 8, 8, C), axis=0)
                at = idx_ref[k, t]
                acc[at] = acc[at] + area_ref[t] * part
        return carry

    lax.fori_loop(0, WC, work, 0)

    def summed(rel):
        at = (rel + 3) * PAD
        return jnp.sum(acc[at : at + PAD], axis=1)

    left[:PAD] = summed(-1)
    left[PAD:] = summed(-2)
    right[:PAD] = summed(1)
    right[PAD:] = summed(2)
    own[:PAD] = summed(0)
    own[PAD : 2 * PAD] = summed(-3)
    own[2 * PAD :] = summed(3)


def sums_call(idx, area, weights):
    smem = pl.BlockSpec(memory_space=pltpu.SMEM)
    vmem = pl.BlockSpec(memory_space=pltpu.VMEM)
    return pl.pallas_call(
        sums_kernel,
        in_specs=[smem, smem, pl.BlockSpec(memory_space=pltpu.HBM)],
        out_specs=[vmem] * 4,
        out_shape=[pltpu.VMEM(weights.shape, weights.dtype)]
        + [jax.ShapeDtypeStruct((n * PAD, C), jnp.float32) for n in (2, 2, 3)],
        scratch_shapes=[
            pltpu.VMEM((SECT + 1, 8, C), jnp.float32),
            pltpu.SemaphoreType.DMA((WC,)),
        ],
        compiler_params=pltpu.CompilerParams(vmem_limit_bytes=6 << 20),
        cost_estimate=pl.CostEstimate(
            flops=20_000_000, bytes_accessed=17 << 20, transcendentals=0
        ),
        name="sums",
    )(idx, area, pltpu.with_memory_space_constraint(weights, pltpu.HBM))


def split_kernel(q_hbm, qs, qm, sem):
    copies = [
        pltpu.make_async_copy(q_hbm.at[pl.ds(at, n)], ref.at[pl.ds(to, n)], sem.at[i])
        for i, (at, n, ref, to) in enumerate(
            ((0, EDGE, qs, 0), (ROWS - EDGE, EDGE, qs, EDGE), (EDGE, M, qm, 0))
        )
    ]
    for copy in copies:
        copy.start()
    for copy in copies:
        copy.wait()


def split_call(q):
    vmem = pl.BlockSpec(memory_space=pltpu.VMEM)
    return pl.pallas_call(
        split_kernel,
        in_specs=[pl.BlockSpec(memory_space=pltpu.HBM)],
        out_specs=[vmem, vmem],
        out_shape=[pltpu.VMEM((n, C, C), jnp.bfloat16) for n in (S, M)],
        scratch_shapes=[pltpu.SemaphoreType.DMA((3,))],
        compiler_params=pltpu.CompilerParams(vmem_limit_bytes=1 << 20),
        cost_estimate=pl.CostEstimate(flops=1000, bytes_accessed=2 << 20, transcendentals=0),
        name="split",
    )(pltpu.with_memory_space_constraint(q, pltpu.HBM))


def pack_kernel(qs, ls, rs, up, dn):
    for n, v in enumerate((qs, ls, rs)):
        up[pl.ds(n * R, R)] = v[S - R :]
        dn[pl.ds(n * R, R)] = v[:R]


def pack_call(parts):
    vmem = pl.BlockSpec(memory_space=pltpu.VMEM)
    return pl.pallas_call(
        pack_kernel,
        in_specs=[vmem] * 3,
        out_specs=[vmem, vmem],
        out_shape=[pltpu.VMEM((3 * R, C, C), jnp.bfloat16)] * 2,
        compiler_params=pltpu.CompilerParams(vmem_limit_bytes=6 << 20),
        cost_estimate=pl.CostEstimate(flops=1000, bytes_accessed=1000, transcendentals=0),
        name="pack",
    )(*parts)


def mass_kernel(area_ref, lost_ref, at_ref, c0, cl, cr, qs, qm, ls, lm, rs, rm, up, dn, l3, r3, out_ref, src, by):
    for n, (e, m) in enumerate(((qs, qm), (ls, lm), (rs, rm))):
        at = n * PAD + R
        src[pl.ds(at, EDGE)] = e[:EDGE]
        src[pl.ds(at + EDGE, M)] = m[...]
        src[pl.ds(at + EDGE + M, EDGE)] = e[EDGE:]
    for n in range(3):
        src[pl.ds(n * PAD, R)] = up[pl.ds(n * R, R)]
        src[pl.ds(n * PAD + R + ROWS, R)] = dn[pl.ds(n * R, R)]
    src[3 * PAD] = jnp.zeros((C, C), src.dtype)
    by[:PAD] = (c0[:PAD] + cl[:PAD]) + cr[:PAD]
    by[PAD : 2 * PAD] = cl[PAD:]
    by[2 * PAD :] = cr[PAD:]
    for r in range(ROWS):
        by[R + r : R + r + 1] = by[R + r : R + r + 1] - area_ref[r]

    def body(p, acc):
        return acc + by[pl.ds(p, 1)] * src[p].astype(jnp.float32)

    acc = lax.fori_loop(0, 3 * PAD, body, jnp.zeros((C, C), jnp.float32), unroll=8)
    at = at_ref[0]
    for i in range(E):
        acc = acc + c0[pl.ds(PAD + at + i, 1)] * l3[i].astype(jnp.float32)
        acc = acc + c0[pl.ds(2 * PAD + at + i, 1)] * r3[i].astype(jnp.float32)
    change = lax.dot_general(
        jnp.full((8, C), -1.0, jnp.float32), acc, NT,
        precision=lax.Precision.HIGHEST, preferred_element_type=jnp.float32,
    )
    row = lax.broadcasted_iota(jnp.int32, (8, C), 0)
    out_ref[...] = jnp.where(row == 0, change, lost_ref[0])


def mass_call(area, lost, at, parts):
    smem = pl.BlockSpec(memory_space=pltpu.SMEM)
    vmem = pl.BlockSpec(memory_space=pltpu.VMEM)
    return pl.pallas_call(
        mass_kernel,
        in_specs=[smem] * 3 + [vmem] * len(parts),
        out_specs=[vmem] * 2,
        out_shape=[
            jax.ShapeDtypeStruct((8, C), jnp.float32),
            pltpu.VMEM((3 * PAD + 1, C, C), jnp.bfloat16),
        ],
        scratch_shapes=[
            pltpu.VMEM((3 * PAD, C), jnp.float32),
        ],
        compiler_params=pltpu.CompilerParams(vmem_limit_bytes=6 << 20),
        cost_estimate=pl.CostEstimate(
            flops=9_000_000, bytes_accessed=3 << 20, transcendentals=0
        ),
        name="mass",
    )(area, lost, at, *parts)


def inner_kernel(first, idx_ref, wv, src, out_ref):
    def body(j, carry):
        t = first + j
        lhs = jnp.concatenate([src[idx_ref[k, t]] for k in range(KMAX)], axis=1)
        rhs = jnp.concatenate([wv[t, k] for k in range(KMAX)], axis=1)
        out_ref[j] = lax.dot_general(lhs, rhs, NT, preferred_element_type=jnp.float32)
        return carry

    lax.fori_loop(0, PER, body, 0, unroll=8)


def inner_call(chunk, idx, wv, near):
    vmem = pl.BlockSpec(memory_space=pltpu.VMEM)
    return pl.pallas_call(
        functools.partial(inner_kernel, chunk * PER),
        in_specs=[pl.BlockSpec(memory_space=pltpu.SMEM), vmem, vmem],
        out_specs=vmem,
        out_shape=pltpu.VMEM((PER, C, C), jnp.float32),
        compiler_params=pltpu.CompilerParams(vmem_limit_bytes=2 << 20),
        cost_estimate=pl.CostEstimate(
            flops=2 * PER * KMAX * C**3, bytes_accessed=1 << 20, transcendentals=0
        ),
    )(idx, wv, near)


def outer_kernel(idx_ref, wv, ls, lm, lb, rs, rm, rb, l3, r3, *refs):
    partial, (out_ref, src) = refs[:CHUNKS], refs[CHUNKS:]
    for n, (e, m, b) in enumerate(((ls, lm, lb), (rs, rm, rb))):
        at = n * SIDE
        src[pl.ds(at, S + R)] = e[...]
        src[pl.ds(at + S + R, M)] = m[...]
        src[pl.ds(at + S + R + M, B + R)] = b[...]
    src[pl.ds(FAR2, E)] = l3[...]
    src[pl.ds(FAR2 + E, E)] = r3[...]
    src[FAR2 + 2 * E] = jnp.zeros((C, C), src.dtype)
    for c in range(CHUNKS):

        def body(j, carry):
            t = c * PER + j
            lhs = jnp.concatenate([src[idx_ref[k, t]] for k in range(KMAX)], axis=1)
            rhs = jnp.concatenate([wv[t, k] for k in range(KMAX)], axis=1)
            got = lax.dot_general(lhs, rhs, NT, preferred_element_type=jnp.float32)
            out_ref[t] = got + partial[c][j]
            return carry

        lax.fori_loop(0, PER, body, 0, unroll=8)


def outer_call(idx, wv, parts, partial):
    vmem = pl.BlockSpec(memory_space=pltpu.VMEM)
    return pl.pallas_call(
        outer_kernel,
        in_specs=[pl.BlockSpec(memory_space=pltpu.SMEM)]
        + [vmem] * (1 + len(parts) + len(partial)),
        out_specs=vmem,
        out_shape=pltpu.VMEM((ROWS, C, C), jnp.float32),
        scratch_shapes=[pltpu.VMEM((FAR2 + 2 * E + 1, C, C), jnp.bfloat16)],
        compiler_params=pltpu.CompilerParams(vmem_limit_bytes=8 << 20),
        cost_estimate=pl.CostEstimate(
            flops=2 * ROWS * KMAX * C**3, bytes_accessed=1 << 20, transcendentals=0
        ),
        name="outer",
    )(idx, wv, *parts, *partial)


WRITES = 8


def write_kernel(corr_ref, in_ref, out_hbm, buf, sem):
    rows = ROWS // WRITES

    def copy(c):
        at = pl.ds(c * rows, rows)
        return pltpu.make_async_copy(buf.at[at], out_hbm.at[at], sem.at[c])

    for c in range(WRITES):
        for i in range(rows):
            t = c * rows + i
            buf[t] = in_ref[t] + corr_ref[...]
        copy(c).start()
    for c in range(WRITES):
        copy(c).wait()


def write_call(corr, advected):
    vmem = pl.BlockSpec(memory_space=pltpu.VMEM)
    return pl.pallas_call(
        write_kernel,
        in_specs=[vmem] * 2,
        out_specs=pl.BlockSpec(memory_space=pltpu.HBM),
        out_shape=jax.ShapeDtypeStruct((ROWS, C, C), jnp.float32),
        scratch_shapes=[
            pltpu.VMEM((ROWS, C, C), jnp.float32),
            pltpu.SemaphoreType.DMA((WRITES,)),
        ],
        compiler_params=pltpu.CompilerParams(vmem_limit_bytes=6 << 20),
        cost_estimate=pl.CostEstimate(
            flops=1_000_000, bytes_accessed=4 << 20, transcendentals=0
        ),
        name="write",
    )(corr, advected)


def tables(source_row, source_block, slot_count, lat, lon):
    p = source_row[:, 0, :].T - (lat * ROWS - R)
    p = jnp.clip(p, 0, PAD - 1)
    rel = (source_block[:, 0, :].T - lon + 3) % NLON_DEV - 3
    rel = jnp.clip(rel, -3, 3)
    active = jnp.arange(KMAX, dtype=jnp.int32)[:, None] < slot_count[:, 0][None, :]
    sums_idx = jnp.where(active, (rel + 3) * PAD + p, SECT)
    size = jnp.abs(rel)
    side = (rel > 0).astype(jnp.int32)
    near_idx = jnp.where(
        active & (size <= 1), jnp.where(rel == 0, 0, side + 1) * PAD + p, 3 * PAD
    )
    r = p - R
    is_polar = (lat == 0) | (lat == NLAT_DEV - 1)
    in_band = jnp.where(r < EDGE, r, jnp.where(r < EDGE + M, r - EDGE + S + R, r - M))
    below = lat == NLAT_DEV - 2
    in_next = S + R + M + jnp.where(below, r - (ROWS - B), r)
    halo = jnp.where(is_polar, S, S + R + M + B) + jnp.where(r < 0, r + R, r - ROWS)
    two = jnp.where((r < 0) | (r >= ROWS), halo, jnp.where(is_polar, in_band, in_next))
    polar_row = jnp.clip(jnp.where(lat == 0, r, r - (ROWS - E)), 0, E - 1)
    far = jnp.where(size >= 3, FAR2 + side * E + polar_row, side * SIDE + two)
    is_far = active & (size >= 2)
    held = is_polar | ((lat == 1) & (r < B)) | (below & (r >= ROWS - B))
    lost = jnp.sum((is_far & ~held).astype(jnp.float32))
    far_idx = jnp.where(is_far & held, far, FAR2 + 2 * E)
    return sums_idx, near_idx, far_idx, lost


def swap(v, axis, size, to):
    return lax.ppermute(v, axis, [(i, to(i)) for i in range(size)])


def three(v, axis, size, to):
    got = [swap(v, axis, size, functools.partial(to, by=by)) for by in (1, 2, 3)]
    return (got[0] + got[2]) + got[1]


def local(tracers, weights, source_row, source_block, slot_count):
    args = (tracers, weights, source_row, source_block, slot_count)
    lost, fixed = usual(*args)

    def redo(state):
        return jnp.zeros_like(state[0]), everywhere(*args)

    _, fixed = lax.while_loop(lambda state: state[0] > 0, redo, (lost, fixed))
    return fixed.reshape(ROWS, 32, 4, C).transpose(0, 3, 1, 2)


def usual(tracers, weights, source_row, source_block, slot_count):
    lat, lon = lax.axis_index("lat"), lax.axis_index("lon")
    both = ("lat", "lon")
    w = weights[:, 0]
    q = tracers.transpose(0, 2, 3, 1).reshape(ROWS, C, C)
    qs, qm = split_call(q)
    ls, rs = lax.ppermute(qs, "lon", ring(1)), lax.ppermute(qs, "lon", ring(-1))
    lm, rm = lax.ppermute(qm, "lon", ring(1)), lax.ppermute(qm, "lon", ring(-1))
    pole = jnp.where(lat == 0, qs[:E], qs[S - E :])
    l3 = lax.ppermute(pole, both, some(3, POLAR))
    r3 = lax.ppermute(pole, both, some(-3, POLAR))
    sums_idx, near_idx, far_idx, lost = tables(source_row, source_block, slot_count, lat, lon)
    area = latitude_area(lat * ROWS, ROWS)
    wv, to_left, to_right, own_sums = sums_call(sums_idx, area, w)
    cl = lax.ppermute(to_left, "lon", ring(-1))
    cr = lax.ppermute(to_right, "lon", ring(1))
    first, last = pack_call((qs, ls, rs))
    up1, dn1 = lax.ppermute(first, "lat", UP), lax.ppermute(last, "lat", DOWN)
    at = jnp.where(jnp.arange(NLAT_DEV, dtype=jnp.int32) == lat, R, R + ROWS - E).astype(jnp.int32)
    v, near = mass_call(
        area, lost.reshape(1), at,
        (own_sums, cl, cr, qs, qm, ls, lm, rs, rm, up1, dn1, l3, r3),
    )
    held = lambda x: pltpu.with_memory_space_constraint(x, pltpu.VMEM)
    near, wv = held(near), held(wv)
    v = v + swap(v, "lat", NLAT_DEV, lambda i: i ^ 1)
    v = v + three(v, "lat", NLAT_DEV, lambda i, by: (i + 2 * by) % NLAT_DEV)
    v = v + three(v, "lon", NLON_DEV, lambda i, by: (i + 4 * by) % NLON_DEV)
    v = v + three(v, "lon", NLON_DEV, lambda i, by: i // 4 * 4 + (i + by) % 4)
    corr = jnp.broadcast_to((v[0] * (1.0 / TOTAL_AREA))[:, None], (C, C))

    beyond = jnp.where(lat == 0, dn1[R:], jnp.where(lat == NLAT_DEV - 2, dn1[R:], up1[R:]))
    sides = ((ls, beyond[:R], 1), (rs, beyond[R:], -1))
    lls, rrs = (
        lax.ppermute(jnp.concatenate([x, h], axis=0), both, some(d, POLAR)) for x, h, d in sides
    )
    llb, rrb = (
        lax.ppermute(
            jnp.concatenate([jnp.where(lat == 1, x[:B], x[S - B :]), h], axis=0),
            both, some(d, NEXT),
        )
        for x, h, d in sides
    )
    llm, rrm = (lax.ppermute(x, both, some(d, POLAR)) for x, d in ((lm, 1), (rm, -1)))

    partial = [held(inner_call(c, near_idx, wv, near)) for c in range(CHUNKS)]
    advected = outer_call(far_idx, wv, (lls, llm, llb, rrs, rrm, rrb, l3, r3), partial)
    fixed = write_call(corr, held(advected))
    return v[1, 0], fixed


def solution(mesh):
    placed = (
        P("lat", "lon", None, None),
        P("lat", "lon", None, None, None),
        P("lat", "lon", None),
        P("lat", "lon", None),
        P("lat", "lon"),
    )
    return jax.shard_map(
        local, mesh=mesh, in_specs=placed, out_specs=P("lat", "lon", None, None), check_vma=False
    )
```
